32 devices in a mesh: island: 4 (over z), shard: 8 (over y, x, core).
Axes of the slice: x: 2, y: 2, z: 4, core: 2. Of those that a mesh axis runs over, the one named last changes fastest.
Arguments:
- weight_master: float32 [4096, 4096], P('island', 'shard'), may hold values from -6 to 6
- gain_master: float32 [4096], P(('shard', 'island')), may hold values from 0.5 to 1.5
- weight_moment: float32 [4096, 4096], P('island', 'shard'), may hold values from -0.3 to 0.3
- gain_moment: float32 [4096], P(('shard', 'island')), may hold values from -0.3 to 0.3
- attended: bfloat16 [4, 2, 768, 4096], P('island', None, 'shard'), may hold values from -6 to 6
- stream: bfloat16 [4, 2, 768, 4096], P('island', None, None, 'shard'), may hold values from -6 to 6
- targets: bfloat16 [4, 2, 768, 4096], P('island', None, None, 'shard'), may hold values from -6 to 6
Outputs:
- weight_updated: float32 [4096, 4096], P('island', 'shard')
- gain_updated: float32 [4096], P(('shard', 'island'))
- weight_velocity: float32 [4096, 4096], P('island', 'shard')
- gain_velocity: float32 [4096], P(('shard', 'island'))
The draws below stay inside these ranges and needn't reach their ends.
All inputs are finite; a program needn't handle non-finite values.
Results may differ from the reference program's by a relative error of at most 0.0066.
Values may be sent and summed in bfloat16 or wider, within the bound.
A program may use at most 192 MiB of HBM per device.

```python
import jax
import jax.numpy as jnp
from jax import lax

D = 4096
STEPS = 2
TOK = 768
ISLANDS = 4
N_ISLAND = 4


def block_scale(own_key, shape, split, smallest, largest):
    loudness, own = 1.0, jax.random.fold_in(own_key, 6)
    for position, parts in split:
        heights = jnp.exp(jax.random.uniform(jax.random.fold_in(own, position), (parts,), jnp.float32, smallest / len(split), largest / len(split)))
        loudness = loudness * jnp.repeat(heights, shape[position] // parts).reshape([-1 if axis == position else 1 for axis in range(len(shape))])
    return loudness


def normal_values(own_key, extent, width, reach, shards=(), kind=jnp.bfloat16):
    result = width * jax.random.normal(own_key, extent, jnp.float32)
    if shards:
        result = result * block_scale(own_key, extent, shards, -0.22, 0.18)
    return jnp.clip(result, -reach, reach).astype(kind)


def setup_inputs(seed: int = 0) -> dict:
    arg_keys = jax.random.split(jax.random.key(seed), 8)
    return {
        "weight_master": normal_values(arg_keys[0], (D, D), 1.0, 6.0, ((0, 4), (1, 8)), jnp.float32),
        "gain_master": jnp.clip(1.0 + 0.1 * jax.random.normal(arg_keys[1], (D,), jnp.float32), 0.5, 1.5),
        "weight_moment": normal_values(arg_keys[2], (D, D), 0.05, 0.3, ((0, 4), (1, 8)), jnp.float32),
        "gain_moment": normal_values(arg_keys[3], (D,), 0.05, 0.3, ((0, 32),), jnp.float32),
        "attended": normal_values(arg_keys[4], (ISLANDS, STEPS, TOK, D), 1.0, 6.0, ((0, 4), (2, 8))),
        "stream": normal_values(arg_keys[5], (ISLANDS, STEPS, TOK, D), 1.0, 6.0, ((0, 4), (3, 8))),
        "targets": normal_values(arg_keys[6], (ISLANDS, STEPS, TOK, D), 1.0, 6.0, ((0, 4), (3, 8))),
    }


norm_epsilon = 1e-05
inner_rate = 0.05
beta_one = 0.9
beta_two = 0.95
adam_epsilon = 0.3
decay_rate = 0.1
outer_rate = 0.7
outer_momentum = 0.9

def optimizer_update(param, gradient, first, second, number, decay):
    first = beta_one * first + (1.0 - beta_one) * gradient
    second = beta_two * second + (1.0 - beta_two) * gradient * gradient
    first_hat = first / (1.0 - beta_one ** number)
    second_hat = second / (1.0 - beta_two ** number)
    param = param - inner_rate * (first_hat / (jnp.sqrt(second_hat) + adam_epsilon) + decay * param)
    return (param, first, second)

def rounded(value):
    return lax.optimization_barrier(value.astype(jnp.bfloat16)).astype(jnp.float32)

def island_window(weight_anchor, gain_anchor, attended_all, stream_all, goals_all):
    highest = lax.Precision.HIGHEST
    width_scale = D ** (-0.5)
    weight = weight_anchor
    gain = gain_anchor
    weight_first = jnp.zeros_like(weight)
    weight_second = jnp.zeros_like(weight)
    gain_first = jnp.zeros_like(gain)
    gain_second = jnp.zeros_like(gain)
    for inner_step in range(STEPS):
        number = inner_step + 1
        weight_low = weight.astype(jnp.bfloat16).astype(jnp.float32)
        rows_wide = attended_all[inner_step].astype(jnp.float32)
        projected = jnp.dot(rows_wide, weight_low, precision=highest) * width_scale
        residual = stream_all[inner_step].astype(jnp.float32) + projected
        inverse = lax.rsqrt(lax.optimization_barrier(jnp.mean(residual * residual, axis=1, keepdims=True)) + norm_epsilon)
        normed = residual * inverse * gain
        loss_grad = rounded(normed - goals_all[inner_step].astype(jnp.float32))
        scaled = loss_grad * gain
        slope = lax.optimization_barrier(jnp.sum(scaled * residual, axis=1, keepdims=True))
        residual_grad = rounded(inverse * scaled - residual * inverse * inverse * inverse * slope / D)
        weight_grad = jnp.dot(rows_wide.T, residual_grad, precision=highest) * width_scale
        gain_grad = lax.optimization_barrier(jnp.sum(loss_grad * residual * inverse, axis=0))
        weight, weight_first, weight_second = optimizer_update(weight, weight_grad, weight_first, weight_second, number, decay_rate)
        gain, gain_first, gain_second = optimizer_update(gain, gain_grad, gain_first, gain_second, number, 0.0)
    return (weight, gain)

def reference(weight_master, gain_master, weight_moment, gain_moment, attended, stream, targets):
    weight_anchor = rounded(weight_master)
    gain_anchor = rounded(gain_master)
    weight_total = jnp.zeros_like(weight_master)
    gain_total = jnp.zeros_like(gain_master)
    for island in range(N_ISLAND):
        weight_final, gain_final = island_window(weight_anchor, gain_anchor, attended[island], stream[island], targets[island])
        weight_total = weight_total + (weight_anchor - weight_final)
        gain_total = gain_total + (gain_anchor - gain_final)
    weight_pseudo = weight_total / N_ISLAND
    gain_pseudo = gain_total / N_ISLAND
    weight_velocity = outer_momentum * weight_moment + weight_pseudo
    gain_velocity = outer_momentum * gain_moment + gain_pseudo
    weight_updated = weight_master - outer_rate * (weight_pseudo + outer_momentum * weight_velocity)
    gain_updated = gain_master - outer_rate * (gain_pseudo + outer_momentum * gain_velocity)
    return (weight_updated, gain_updated, weight_velocity, gain_velocity)
```

```python
import functools
import math

import jax
import jax.numpy as jnp
from jax import lax
from jax.experimental import pallas as pl
from jax.experimental.pallas import tpu as pltpu
from jax.sharding import PartitionSpec as P

norm_epsilon = 1e-05
inner_rate = 0.05
beta_one = 0.9
beta_two = 0.95
adam_epsilon = 0.3
decay_rate = 0.1
outer_rate = 0.7
outer_momentum = 0.9

MESH = pl.DeviceIdType.MESH
LANES = 128
keep = 1.0 - inner_rate * decay_rate


def flip(index, bit):
    size = 1 << bit
    return index + size * (1 - 2 * (lax.div(index, size) % 2))


def first_update(grad):
    return grad / (jnp.abs(grad) + adam_epsilon)


def second_update(earlier, grad):
    first = (beta_one * (1.0 - beta_one)) * earlier + (1.0 - beta_one) * grad
    second = (beta_two * (1.0 - beta_two)) * earlier * earlier + (1.0 - beta_two) * grad * grad
    first_hat = first * (1.0 / (1.0 - beta_one**2))
    second_hat = second * (1.0 / (1.0 - beta_two**2))
    return first_hat / (jnp.sqrt(second_hat) + adam_epsilon)


def general_kernel(
    n_i, n_s, low_ref, gain_ref, rows_ref, stream_ref, goals_ref, total_ref, gain_total_ref,
    rows, anchor, later, grads, res, slope_low, stream, goals, from_left, from_right,
    stats, line, gains, gain_moves,
    local_sem, z_send, z_recv, a_send, a_recv, s_send, s_recv, g_send, g_recv, r_send, r_recv,
):
    i = lax.axis_index("island")
    s = lax.axis_index("shard")
    steps, _, block, width = rows.shape
    piece, cols = low_ref.shape
    tokens = n_s * block
    tiles = tokens // LANES
    scale = width ** (-0.5)
    depth = min(512, piece)
    tall = min(256, piece)

    barrier = pltpu.get_barrier_semaphore()
    for d in range(1, n_i):
        pl.semaphore_signal(barrier, inc=1, device_id=(lax.rem(i + d, n_i), s), device_id_type=MESH)
    for d in range(1, n_s):
        pl.semaphore_signal(barrier, inc=1, device_id=(i, lax.rem(s + d, n_s)), device_id_type=MESH)

    locals_ = [pltpu.make_async_copy(low_ref, anchor.at[i], local_sem.at[0])]
    for st in range(steps):
        locals_.append(pltpu.make_async_copy(rows_ref.at[0, st], rows.at[st, s], local_sem.at[1 + st]))
    locals_.append(pltpu.make_async_copy(stream_ref.at[0], stream, local_sem.at[1 + steps]))
    locals_.append(pltpu.make_async_copy(goals_ref.at[0], goals, local_sem.at[2 + steps]))
    for copy in locals_:
        copy.start()
    pl.semaphore_wait(barrier, n_i - 1 + n_s - 1)

    def remote(src, dst, send, recv, to):
        return pltpu.make_async_remote_copy(
            src_ref=src, dst_ref=dst, send_sem=send, recv_sem=recv, device_id=to, device_id_type=MESH
        )

    right, left = (lax.rem(i + 1, n_i), s), (lax.rem(i + n_i - 1, n_i), s)

    def z_copy(way, t, at):
        return remote(
            anchor.at[at], anchor.at[at], z_send.at[way, t], z_recv.at[way, t], right if way == 0 else left
        )

    def z_start(t):
        @pl.when((i < n_i - 1) & (i - t >= 0))
        def _():
            z_copy(0, t, i - t).start()

        @pl.when((i > 0) & (i + t <= n_i - 1))
        def _():
            z_copy(1, t, i + t).start()

    def z_wait(t):
        @pl.when(i - 1 - t >= 0)
        def _():
            z_copy(0, t, i - 1 - t).wait_recv()

        @pl.when(i + 1 + t <= n_i - 1)
        def _():
            z_copy(1, t, i + 1 + t).wait_recv()

    n_bits = n_s.bit_length() - 1
    orders = [list(range(1, n_bits)) + [0], list(range(n_bits - 1, 0, -1)) + [0]]

    def a_blocks(st, phase):
        order = orders[st % 2]
        found = []
        for m in range(1 << phase):
            at = s
            for q in range(phase):
                if (m >> q) & 1:
                    at = flip(at, order[q])
            found.append(at)
        return found

    def a_copy(st, phase, m, at):
        slot = (1 << phase) - 1 + m
        return remote(
            rows.at[st, at], rows.at[st, at], a_send.at[st, slot], a_recv.at[st, slot],
            (i, flip(s, orders[st % 2][phase])),
        )

    def a_start(phase):
        for st in range(steps):
            for m, at in enumerate(a_blocks(st, phase)):
                a_copy(st, phase, m, at).start()

    def a_wait(phase):
        for st in range(steps):
            for m, at in enumerate(a_blocks(st, phase)):
                a_copy(st, phase, m, flip(at, orders[st % 2][phase])).wait_recv()

    def to_islands(buffer, which):
        return [
            remote(
                buffer.at[0], buffer.at[d], g_send.at[which, d], g_recv.at[which, d],
                (lax.rem(i + d, n_i), s),
            )
            for d in range(1, n_i)
        ]

    locals_[0].wait()
    z_start(0)
    for copy in locals_[1 : 1 + steps]:
        copy.wait()
    a_start(0)
    gains[0] = gain_ref[...]
    gain_in = to_islands(gains, 0)
    for copy in gain_in:
        copy.start()
    res[...] = jnp.zeros_like(res)
    for copy in locals_[1 + steps :]:
        copy.wait()

    def project(st, weights, at):
        def body(k, _):
            start = pl.multiple_of(k * depth, depth)
            wide = pl.multiple_of(at * piece + k * depth, depth)
            part = rows[st, :, :, pl.ds(wide, depth)].reshape(tokens, depth)
            res[...] += jnp.dot(part, weights[at, pl.ds(start, depth), :], preferred_element_type=jnp.float32)
            return 0

        lax.fori_loop(0, piece // depth, body, 0)

    def project_arrived(t):
        @pl.when(i - 1 - t >= 0)
        def _():
            project(0, anchor, i - 1 - t)

        @pl.when(i + 1 + t <= n_i - 1)
        def _():
            project(0, anchor, i + 1 + t)

    events = [(2.0 * t + 2.6, "z", t) for t in range(n_i - 1)]
    events += [(2.0 * ((2 << p) - 1), "a", p) for p in range(n_bits - 1)]
    last = events[-1][0] if n_bits > 1 else 0.0
    events.append((last + 0.1, "a", n_bits - 1))
    gathered, ready = False, []
    for _, kind, at in sorted(events):
        if kind == "a":
            a_wait(at)
            if at + 1 < n_bits:
                a_start(at + 1)
            else:
                gathered = True
                project(0, anchor, i)
                for t in ready:
                    project_arrived(t)
        else:
            z_wait(at)
            if at + 1 < n_i - 1:
                z_start(at + 1)
            if gathered:
                project_arrived(at)
            else:
                ready.append(at)

    for copy in gain_in:
        copy.wait()
    gain_anchor = gains[0]
    for d in range(1, n_i):
        gain_anchor = gain_anchor + gains[d]
    gain = gain_anchor

    def fold(value):
        total = value[:, :LANES]
        for c in range(1, cols // LANES):
            total = total + value[:, c * LANES : (c + 1) * LANES]
        return jnp.sum(total.T, axis=0, keepdims=True)

    def spread(value):
        square = jnp.broadcast_to(value, (LANES, LANES)).T
        return jnp.concatenate([square] * (cols // LANES), axis=1)

    def row_stats(st, gain):
        def body(q, _):
            at = pl.ds(pl.multiple_of(q * LANES, LANES), LANES)
            r = stream[st, at, :].astype(jnp.float32) + res[at, :] * scale
            res[at, :] = r
            weighted = r * gain
            stats[st, 0, 0:1, at] = fold(r * r)
            stats[st, 0, 1:2, at] = fold(weighted * weighted)
            stats[st, 0, 2:3, at] = fold(weighted * goals[st, at, :].astype(jnp.float32))
            stats[st, 0, 3:4, at] = jnp.zeros((1, LANES), jnp.float32)
            return 0

        lax.fori_loop(0, tiles, body, 0)
        copies = [
            remote(
                stats.at[st, 0], stats.at[st, d], s_send.at[st, d], s_recv.at[st, d],
                (i, lax.rem(s + d, n_s)),
            )
            for d in range(1, n_s)
        ]
        for copy in copies:
            copy.start()
        for copy in copies:
            copy.wait()
        total = stats[st, 0]
        for d in range(1, n_s):
            total = total + stats[st, d]
        inverse = lax.rsqrt(total[0:1] * (1.0 / width) + norm_epsilon)
        slope = inverse * total[1:2] - total[2:3]
        line[0:1, :] = inverse
        line[1:2, :] = inverse * inverse * inverse * slope * (1.0 / width)

    def row_grads(st, gain):
        def body(q, total):
            at = pl.ds(pl.multiple_of(q * LANES, LANES), LANES)
            inverse, pull = spread(line[0:1, at]), spread(line[1:2, at])
            r = res[at, :]
            unit = r * inverse
            loss = unit * gain - goals[st, at, :].astype(jnp.float32)
            loss = loss.astype(jnp.bfloat16).astype(jnp.float32)
            slope_low[at, :] = (inverse * (loss * gain) - r * pull).astype(jnp.bfloat16)
            return total + jnp.sum(loss * unit, axis=0, keepdims=True)

        return lax.fori_loop(0, tiles, body, jnp.zeros((1, cols), jnp.float32))

    def weight_grad(st, wide):
        part = rows[st, :, :, pl.ds(pl.multiple_of(wide, tall), tall)].reshape(tokens, tall)
        return (
            lax.dot_general(
                part, slope_low[...], (((0,), (0,)), ((), ())), preferred_element_type=jnp.float32
            )
            * scale
        )

    row_stats(0, gain)
    gain_first = row_grads(0, gain)
    per_piece = piece // tall

    def step_one(q, _):
        o, j = q // per_piece, q % per_piece
        at = pl.ds(pl.multiple_of(j * tall, tall), tall)
        grad = weight_grad(0, q * tall)
        grads[o, at, :] = grad
        param = keep * anchor[o, at, :].astype(jnp.float32) - inner_rate * first_update(grad)
        later[o, at, :] = param.astype(jnp.bfloat16)
        return 0

    lax.fori_loop(0, n_i * per_piece, step_one, 0)
    gain_step = first_update(gain_first)
    gain = gain_anchor - inner_rate * gain_step

    res[...] = jnp.zeros_like(res)

    def project_later(at, _):
        project(1, later, at)
        return 0

    lax.fori_loop(0, n_i, project_later, 0)
    row_stats(1, gain)
    gain_second = row_grads(1, gain)
    gain_moves[0] = inner_rate * (gain_step + second_update(gain_first, gain_second))
    gain_out = to_islands(gain_moves, 1)
    for copy in gain_out:
        copy.start()

    def to_right(k):
        at = n_i - 1 - k
        return remote(later.at[at], from_left.at[k], r_send.at[0, k], r_recv.at[0, k], right)

    def to_left(k):
        return remote(later.at[k], from_right.at[k], r_send.at[1, k], r_recv.at[1, k], left)

    early = 1 - lax.div(2 * i, n_i)

    def owner_piece(q, _):
        o = q + early * (n_i - 1 - 2 * q)

        def step_two(j, _):
            at = pl.ds(pl.multiple_of(j * tall, tall), tall)
            grad = weight_grad(1, o * piece + j * tall)
            earlier = grads[o, at, :]
            moved = (1.0 - keep * keep) * anchor[o, at, :].astype(jnp.float32) + inner_rate * (
                keep * first_update(earlier) + second_update(earlier, grad)
            )
            grads[o, at, :] = moved
            later[o, at, :] = moved.astype(jnp.bfloat16)
            return 0

        lax.fori_loop(0, per_piece, step_two, 0)

        @pl.when((i == 0) & (o > 0))
        def _():
            to_right(n_i - 1 - o).start()

        @pl.when((i == n_i - 1) & (o < n_i - 1))
        def _():
            to_left(o).start()

        return 0

    lax.fori_loop(0, n_i, owner_piece, 0)

    def add(o, arrived, k):
        def body(j, _):
            at = pl.ds(pl.multiple_of(j * tall, tall), tall)
            later[o, at, :] = (grads[o, at, :] + arrived[k, at, :].astype(jnp.float32)).astype(jnp.bfloat16)
            return 0

        lax.fori_loop(0, per_piece, body, 0)

    for t in range(n_i - 1):
        k_right = t - i
        k_left = t - (n_i - 1 - i)

        @pl.when((i > 0) & (k_right >= 0) & (k_right < n_i - 1 - i))
        def _():
            to_right(k_right).wait_recv()
            add(n_i - 1 - k_right, from_left, k_right)
            to_right(k_right).start()

        @pl.when((i < n_i - 1) & (k_left >= 0) & (k_left < i))
        def _():
            to_left(k_left).wait_recv()
            add(k_left, from_right, k_left)
            to_left(k_left).start()

    for copy in gain_out:
        copy.wait()
    gain_total = gain_moves[0]
    for d in range(1, n_i):
        gain_total = gain_total + gain_moves[d]
    gain_total_ref[...] = gain_total

    total_ref[...] = grads[i]

    @pl.when(i > 0)
    def _():
        k = n_i - 1 - i
        to_right(k).wait_recv()
        total_ref[...] += from_left[k].astype(jnp.float32)

    @pl.when(i < n_i - 1)
    def _():
        to_left(i).wait_recv()
        total_ref[...] += from_right[i].astype(jnp.float32)

    for k in range(n_i - 1):

        @pl.when(k < n_i - 1 - i)
        def _(k=k):
            to_right(k).wait_send()

        @pl.when(k < i)
        def _(k=k):
            to_left(k).wait_send()

        @pl.when((i < n_i - 1) & (i - k >= 0))
        def _(k=k):
            z_copy(0, k, i - k).wait_send()

        @pl.when((i > 0) & (i + k <= n_i - 1))
        def _(k=k):
            z_copy(1, k, i + k).wait_send()

    for phase in range(n_bits):
        for st in range(steps):
            for m, at in enumerate(a_blocks(st, phase)):
                a_copy(st, phase, m, at).wait_send()


def general_device(weight_master, gain_master, weight_moment, gain_moment, attended, stream, targets):
    n_i, n_s = lax.axis_size("island"), lax.axis_size("shard")
    _, steps, block, width = attended.shape
    _, _, tokens, cols = stream.shape
    piece = weight_master.shape[0]
    own = gain_master.shape[0]
    offset = lax.axis_index("island") * own
    low = weight_master.astype(jnp.bfloat16)
    gain_low = gain_master.astype(jnp.bfloat16).astype(jnp.float32)
    gain_row = lax.dynamic_update_slice(jnp.zeros((1, cols), jnp.float32), gain_low[None], (0, offset))
    any_space = pl.BlockSpec(memory_space=pl.ANY)
    vmem = pl.BlockSpec(memory_space=pltpu.VMEM)
    f32, bf16 = jnp.float32, jnp.bfloat16
    dma = pltpu.SemaphoreType.DMA
    weight_summed, gain_summed = pl.pallas_call(
        functools.partial(general_kernel, n_i, n_s),
        out_shape=(
            jax.ShapeDtypeStruct((piece, cols), f32),
            jax.ShapeDtypeStruct((1, cols), f32),
        ),
        in_specs=[any_space, vmem, any_space, any_space, any_space],
        out_specs=(vmem, vmem),
        scratch_shapes=[
            pltpu.VMEM((steps, n_s, block, width), bf16),
            pltpu.VMEM((n_i, piece, cols), bf16),
            pltpu.VMEM((n_i, piece, cols), bf16),
            pltpu.VMEM((n_i, piece, cols), f32),
            pltpu.VMEM((tokens, cols), f32),
            pltpu.VMEM((tokens, cols), bf16),
            pltpu.VMEM((steps, tokens, cols), bf16),
            pltpu.VMEM((steps, tokens, cols), bf16),
            pltpu.VMEM((n_i - 1, piece, cols), bf16),
            pltpu.VMEM((n_i - 1, piece, cols), bf16),
            pltpu.VMEM((steps, n_s, 4, tokens), f32),
            pltpu.VMEM((2, tokens), f32),
            pltpu.VMEM((n_i, 1, cols), f32),
            pltpu.VMEM((n_i, 1, cols), f32),
            dma((3 + steps,)),
            dma((2, n_i - 1)),
            dma((2, n_i - 1)),
            dma((steps, n_s - 1)),
            dma((steps, n_s - 1)),
            dma((steps, n_s)),
            dma((steps, n_s)),
            dma((2, n_i)),
            dma((2, n_i)),
            dma((2, n_i - 1)),
            dma((2, n_i - 1)),
        ],
        compiler_params=pltpu.CompilerParams(
            collective_id=0, has_side_effects=True, vmem_limit_bytes=67043328
        ),
    )(low, gain_row, attended, stream, targets)
    weight_pseudo = weight_summed / n_i
    gain_pseudo = lax.dynamic_slice(gain_summed, (0, offset), (1, own))[0] / n_i
    weight_velocity = outer_momentum * weight_moment + weight_pseudo
    gain_velocity = outer_momentum * gain_moment + gain_pseudo
    weight_updated = weight_master - outer_rate * (weight_pseudo + outer_momentum * weight_velocity)
    gain_updated = gain_master - outer_rate * (gain_pseudo + outer_momentum * gain_velocity)
    return (weight_updated, gain_updated, weight_velocity, gain_velocity)


def outer_sum(grad_one, grad_two):
    first = (inner_rate * beta_one * (1.0 - beta_one) / (1.0 - beta_one**2)) * grad_one + (
        inner_rate * (1.0 - beta_one) / (1.0 - beta_one**2)
    ) * grad_two
    second = (beta_two * (1.0 - beta_two) / (1.0 - beta_two**2)) * (grad_one * grad_one) + (
        (1.0 - beta_two) / (1.0 - beta_two**2)
    ) * (grad_two * grad_two)
    root = jnp.sqrt(second) + adam_epsilon
    size = jnp.abs(grad_one) + adam_epsilon
    return ((inner_rate * keep) * grad_one * root + first * size) / (root * size)


def kernel(
    n_i, n_s, master_ref, gain_ref, moment_ref, gain_moment_ref, rows_ref, stream_ref, goals_ref,
    updated_ref, gain_updated_ref, velocity_ref, gain_velocity_ref,
    master, moment, rows, rows_h, anchor, ahead, grads, res, slope, slope_h, stream, goals,
    outgo, from_mate, from_twin, stats, line, gains, gain_out, gain_in,
    local_sem, out_sem, z_send, z_recv, a_send, a_recv, h_send, h_recv, ha_send, ha_recv,
    s_send, s_recv, g_send, g_recv, r_send, r_recv, e_send, e_recv, m_send, m_recv,
):
    i = lax.axis_index("island")
    s = lax.axis_index("shard")
    steps, _, block, width = rows.shape
    _, chunks, piece, _ = anchor.shape
    cols = chunks * LANES
    own = gains.shape[2]
    tokens = n_s * block
    tiles = tokens // LANES
    scale = width ** (-0.5)
    depth = min(1024, piece)
    tall = min(256, piece)
    span = min(512, piece)
    f32, bf16 = jnp.float32, jnp.bfloat16

    is_left = i < n_i // 2
    is_end = (i == 0) | (i == n_i - 1)
    is_inner = (i > 0) & (i < n_i - 1)
    toward = jnp.where(is_left, 1, -1)
    mate = (jnp.where(is_end, i + toward, i - toward), s)
    twin = (n_i - 1 - i, s)

    def mirrored(o):
        return jnp.where(is_left, o, n_i - 1 - o)

    barrier = pltpu.get_barrier_semaphore()
    for d in range(1, n_i):
        pl.semaphore_signal(barrier, inc=1, device_id=(lax.rem(i + d, n_i), s), device_id_type=MESH)
    for d in range(1, n_s):
        pl.semaphore_signal(barrier, inc=1, device_id=(i, lax.rem(s + d, n_s)), device_id_type=MESH)

    load_master = pltpu.make_async_copy(master_ref, master, local_sem.at[0])
    load_rows = [
        pltpu.make_async_copy(rows_ref.at[0, st], rows.at[st, s], local_sem.at[1 + st]) for st in range(steps)
    ]
    load_rest = [
        pltpu.make_async_copy(stream_ref.at[0], stream, local_sem.at[1 + steps]),
        pltpu.make_async_copy(goals_ref.at[0], goals, local_sem.at[2 + steps]),
        pltpu.make_async_copy(moment_ref, moment, local_sem.at[3 + steps]),
    ]
    for copy in [load_master] + load_rows + load_rest:
        copy.start()

    def remote(src, dst, send, recv, to):
        return pltpu.make_async_remote_copy(
            src_ref=src, dst_ref=dst, send_sem=send, recv_sem=recv, device_id=to, device_id_type=MESH
        )

    right, left = (lax.rem(i + 1, n_i), s), (lax.rem(i + n_i - 1, n_i), s)

    def z_copy(way, t, c, at):
        return remote(
            anchor.at[at, c], anchor.at[at, c], z_send.at[way, t, c], z_recv.at[way, t, c],
            right if way == 0 else left,
        )

    def z_start(t, c):
        @pl.when((i < n_i - 1) & (i - t >= 0))
        def _():
            z_copy(0, t, c, i - t).start()

        @pl.when((i > 0) & (i + t <= n_i - 1))
        def _():
            z_copy(1, t, c, i + t).start()

    def z_wait(t, c):
        @pl.when(i - 1 - t >= 0)
        def _():
            z_copy(0, t, c, i - 1 - t).wait_recv()

        @pl.when(i + 1 + t <= n_i - 1)
        def _():
            z_copy(1, t, c, i + 1 + t).wait_recv()

    n_bits = n_s.bit_length() - 1
    orders = [list(range(1, n_bits)) + [0], list(range(n_bits - 1, 0, -1)) + [0]]

    def a_blocks(st, phase):
        order = orders[st % 2]
        found = []
        for m in range(1 << phase):
            at = s
            for q in range(phase):
                if (m >> q) & 1:
                    at = flip(at, order[q])
            found.append(at)
        return found

    def a_copy(buffer, send, recv, st, phase, m, at):
        slot = (1 << phase) - 1 + m
        return remote(
            buffer.at[st, at], buffer.at[st, at], send.at[st, slot], recv.at[st, slot],
            (i, flip(s, orders[st % 2][phase])),
        )

    def a_start(buffer, send, recv, phase):
        for st in range(steps):
            for m, at in enumerate(a_blocks(st, phase)):
                a_copy(buffer, send, recv, st, phase, m, at).start()

    def a_wait(buffer, send, recv, phase):
        for st in range(steps):
            for m, at in enumerate(a_blocks(st, phase)):
                a_copy(buffer, send, recv, st, phase, m, flip(at, orders[st % 2][phase])).wait_recv()

    def a_sent(buffer, send, recv):
        for phase in range(n_bits):
            for st in range(steps):
                for m, at in enumerate(a_blocks(st, phase)):
                    a_copy(buffer, send, recv, st, phase, m, at).wait_send()

    own_rows = (rows, a_send, a_recv)
    end_rows = (rows_h, h_send, h_recv)
    far = pl.multiple_of(jnp.where(is_left, width - 2 * piece, 0), LANES)

    def lend_rows(st):
        return remote(
            rows.at[st, s, :, pl.ds(far, 2 * piece)], rows_h.at[st, s], ha_send.at[st], ha_recv.at[st], mate
        )

    gains[i] = gain_ref[...].astype(bf16).astype(f32)
    gain_copies = [
        remote(gains.at[i], gains.at[i], g_send.at[0, d], g_recv.at[0, d], (lax.rem(i + d, n_i), s))
        for d in range(1, n_i)
    ]
    gain_waits = [
        remote(
            gains.at[lax.rem(i + n_i - d, n_i)], gains.at[lax.rem(i + n_i - d, n_i)],
            g_send.at[0, d], g_recv.at[0, d], (lax.rem(i + d, n_i), s),
        )
        for d in range(1, n_i)
    ]

    load_master.wait()

    def lower(j, _):
        at = pl.ds(pl.multiple_of(j * tall, tall), tall)
        for c in range(chunks):
            anchor[i, c, at, :] = master[at, c * LANES : (c + 1) * LANES].astype(bf16)
        return 0

    lax.fori_loop(0, piece // tall, lower, 0)
    for copy in load_rows:
        copy.wait()
    pl.semaphore_wait(barrier, n_i - 1 + n_s - 1)
    a_start(*own_rows, 0)
    for c in range(chunks):
        z_start(0, c)
    for copy in gain_copies:
        copy.start()
    res[...] = jnp.zeros_like(res)
    for copy in load_rest:
        copy.wait()

    def joined(buffer, at, ds):
        return jnp.concatenate([buffer[at, c, ds, :] for c in range(chunks)], axis=1)

    def project(at):
        def body(k, _):
            start = pl.multiple_of(k * depth, depth)
            wide = pl.multiple_of(at * piece + k * depth, depth)
            part = rows[0, :, :, pl.ds(wide, depth)].reshape(tokens, depth)
            res[...] += jnp.dot(part, joined(anchor, at, pl.ds(start, depth)), preferred_element_type=f32)
            return 0

        lax.fori_loop(0, piece // depth, body, 0)

    def project_arrived(t):
        @pl.when(i - 1 - t >= 0)
        def _():
            project(i - 1 - t)

        @pl.when(i + 1 + t <= n_i - 1)
        def _():
            project(i + 1 + t)

    def when_inner(f):
        pl.when(is_inner)(f)

    def when_end(f):
        pl.when(is_end)(f)

    events = [(t * chunks + c + 1 + 0.3 * (t + 1), "z", (t, c)) for t in range(n_i - 1) for c in range(chunks)]
    spent = 0.0
    for p in range(n_bits - 1):
        spent += 3.0 * (1 << p) * 1.05
        events.append((spent + 0.3, "a", p))
    events.append((spent + 1.6, "a", n_bits - 1))
    gathered, ready = False, []
    for _, kind, at in sorted(events):
        if kind == "a":
            a_wait(*own_rows, at)
            if at == 0:
                @when_end
                def _():
                    for st in range(steps):
                        lend_rows(st).start()
            if at == n_bits - 2:
                @when_inner
                def _():
                    for st in range(steps):
                        lend_rows(st).wait_recv()
                    a_start(*end_rows, 0)
            if at + 1 < n_bits:
                a_start(*own_rows, at + 1)
            else:
                gathered = True
                project(i)
                for t in ready:
                    project_arrived(t)
        else:
            t, c = at
            z_wait(t, c)
            if t + 1 < n_i - 1:
                z_start(t + 1, c)
            if c == chunks - 1:
                if gathered:
                    project_arrived(t)
                else:
                    ready.append(t)

    def lend_phase(p):
        @when_inner
        def _():
            a_wait(*end_rows, p)
            if p + 1 < n_bits:
                a_start(*end_rows, p + 1)

    for copy in gain_waits:
        copy.wait_recv()
    gain_anchor = jnp.concatenate([gains[j] for j in range(n_i)], axis=1)
    gain = gain_anchor

    def fold(value):
        total = value[:, :LANES]
        for c in range(1, chunks):
            total = total + value[:, c * LANES : (c + 1) * LANES]
        return jnp.sum(total.T, axis=0, keepdims=True)

    def spread(value):
        square = jnp.broadcast_to(value, (LANES, LANES)).T
        return jnp.concatenate([square] * chunks, axis=1)

    def row_stats(st, gain):
        def body(q, _):
            at = pl.ds(pl.multiple_of(q * LANES, LANES), LANES)
            r = stream[st, at, :].astype(f32) + res[at, :] * scale
            res[at, :] = r
            weighted = r * gain
            stats[st, 0, 0:1, at] = fold(r * r)
            stats[st, 0, 1:2, at] = fold(weighted * weighted)
            stats[st, 0, 2:3, at] = fold(weighted * goals[st, at, :].astype(f32))
            stats[st, 0, 3:4, at] = jnp.zeros((1, LANES), f32)
            return 0

        lax.fori_loop(0, tiles, body, 0)
        copies = [
            remote(
                stats.at[st, 0], stats.at[st, d], s_send.at[st, d], s_recv.at[st, d],
                (i, lax.rem(s + d, n_s)),
            )
            for d in range(1, n_s)
        ]
        for copy in copies:
            copy.start()
        for copy in copies:
            copy.wait()
        total = stats[st, 0]
        for d in range(1, n_s):
            total = total + stats[st, d]
        inverse = lax.rsqrt(total[0:1] * (1.0 / width) + norm_epsilon)
        pull = inverse * total[1:2] - total[2:3]
        line[0:1, :] = inverse
        line[1:2, :] = inverse * inverse * inverse * pull * (1.0 / width)

    def row_grads(st, gain):
        def body(q, total):
            at = pl.ds(pl.multiple_of(q * LANES, LANES), LANES)
            inverse, pull = spread(line[0:1, at]), spread(line[1:2, at])
            r = res[at, :]
            unit = r * inverse
            loss = unit * gain - goals[st, at, :].astype(f32)
            loss = loss.astype(bf16).astype(f32)
            low = (inverse * (loss * gain) - r * pull).astype(bf16)
            for c in range(chunks):
                slope[st, c, at, :] = low[:, c * LANES : (c + 1) * LANES]
            return total + jnp.sum(loss * unit, axis=0, keepdims=True)

        return lax.fori_loop(0, tiles, body, jnp.zeros((1, cols), f32))

    def product(part, against):
        return lax.dot_general(part, against, (((0,), (0,)), ((), ())), preferred_element_type=f32) * scale

    def weight_grad(st, wide, size):
        part = rows[st, :, :, pl.ds(pl.multiple_of(wide, size), size)].reshape(tokens, size)
        return product(part, joined(slope, st, slice(None)))

    row_stats(0, gain)
    gain_first = row_grads(0, gain)
    res[...] = jnp.zeros_like(res)

    def lend_slope():
        return remote(slope.at[0], slope_h.at[0], r_send.at[0], r_recv.at[0], mate)

    def lend_later(c):
        return remote(slope.at[1, c], slope_h.at[1, c], r_send.at[1 + c], r_recv.at[1 + c], mate)

    when_end(lambda: lend_slope().start())
    lend_phase(0)

    spans = width // span
    per_piece = piece // span

    def step_one(q, slot):
        o, j = q // per_piece, q % per_piece
        at = pl.ds(pl.multiple_of(j * span, span), span)
        grad = weight_grad(0, q * span, span)
        grads[o, at, :] = grad
        param = keep * joined(anchor, o, at).astype(f32) - inner_rate * first_update(grad)
        ahead[slot] = param.astype(bf16)

    def project_later(q, slot):
        part = rows[1, :, :, pl.ds(pl.multiple_of(q * span, span), span)].reshape(tokens, span)
        res[...] += jnp.dot(part, ahead[slot], preferred_element_type=f32)

    def both(q, _):
        step_one(q, 0)
        project_later(q, 0)
        return 0

    lax.fori_loop(0, spans, both, 0)
    gain_step = first_update(gain_first)
    gain = gain_anchor - inner_rate * gain_step
    lend_phase(1)

    row_stats(1, gain)
    gain_second = row_grads(1, gain)
    gain_move = inner_rate * (gain_step + second_update(gain_first, gain_second))
    for j in range(n_i):
        gain_out[j] = gain_move[:, j * own : (j + 1) * own]

    @when_end
    def _():
        for c in range(chunks):
            lend_later(c).start()

    gain_moves = [
        remote(
            gain_out.at[lax.rem(i + d, n_i)], gain_in.at[d], g_send.at[1, d], g_recv.at[1, d],
            (lax.rem(i + d, n_i), s),
        )
        for d in range(1, n_i)
    ]
    for copy in gain_moves:
        copy.start()

    def move(o):
        def body(j, _):
            at = pl.ds(pl.multiple_of(j * tall, tall), tall)
            grad = weight_grad(1, o * piece + j * tall, tall)
            grads[o, at, :] = outer_sum(grads[o, at, :], grad)
            return 0

        lax.fori_loop(0, piece // tall, body, 0)

    def give(slot, c):
        return remote(outgo.at[slot, c], from_mate.at[c], e_send.at[c], e_recv.at[c], mate)

    def cross(slot, c):
        return remote(outgo.at[slot, c], from_twin.at[slot, c], m_send.at[slot, c], m_recv.at[slot, c], twin)

    def pack(slot, c, o, *others):
        lanes = slice(c * LANES, (c + 1) * LANES)

        def body(j, _):
            at = pl.ds(pl.multiple_of(j * tall, tall), tall)
            total = grads[o, at, lanes]
            for other in others:
                total = total + other[at, :].astype(f32)
            outgo[slot, c, at, :] = total.astype(bf16)
            return 0

        lax.fori_loop(0, piece // tall, body, 0)

    store = []

    def finish(c, o, *others):
        lanes = slice(c * LANES, (c + 1) * LANES)

        def body(j, _):
            at = pl.ds(pl.multiple_of(j * tall, tall), tall)
            total = grads[o, at, lanes]
            for other in others:
                total = total + other[at, :].astype(f32)
            outer = master[at, lanes]
            pseudo = total * (1.0 / n_i) + (1.0 - keep * keep) * outer.astype(bf16).astype(f32)
            velocity = outer_momentum * moment[at, lanes] + pseudo
            moment[at, lanes] = velocity
            master[at, lanes] = outer - outer_rate * (pseudo + outer_momentum * velocity)
            return 0

        lax.fori_loop(0, piece // tall, body, 0)
        stores(c)[0].start()
        stores(c)[1].start()

    def stores(c):
        lanes = slice(c * LANES, (c + 1) * LANES)
        return (
            pltpu.make_async_copy(master.at[:, lanes], updated_ref.at[:, lanes], out_sem.at[0, c]),
            pltpu.make_async_copy(moment.at[:, lanes], velocity_ref.at[:, lanes], out_sem.at[1, c]),
        )

    @when_end
    def _():
        o = mirrored(1)
        move(o)
        for c in range(chunks):
            pack(0, c, o)
        for c in range(chunks):
            give(0, c).start()
        o = mirrored(0)
        move(o)
        for c in range(chunks):
            give(0, c).wait_recv()
            finish(c, o, from_mate.at[c])

    def help_end(slot, c, o):
        base = (o - jnp.where(is_left, n_i - 2, 0)) * piece
        lanes = slice(c * LANES, (c + 1) * LANES)

        def body(j, _):
            at = pl.ds(pl.multiple_of(j * tall, tall), tall)
            wide = pl.ds(pl.multiple_of(base + j * tall, tall), tall)
            pair = [
                product(rows_h[st, :, :, wide].reshape(tokens, tall), slope_h[st, c]) for st in range(steps)
            ]
            outgo[slot, c, at, :] = (grads[o, at, lanes] + outer_sum(*pair)).astype(bf16)
            return 0

        lax.fori_loop(0, piece // tall, body, 0)

    @when_inner
    def _():
        for o in (3, 2, 0, 1):
            move(mirrored(o))
        a_wait(*end_rows, n_bits - 1)
        lend_slope().wait_recv()
        for c in range(chunks):
            lend_later(c).wait_recv()
            help_end(0, c, mirrored(3))
            cross(0, c).start()
        for c in range(chunks):
            help_end(1, c, mirrored(2))
            cross(1, c).start()
        o = mirrored(0)
        for c in range(chunks):
            cross(0, c).wait_recv()
            pack(2, c, o, from_twin.at[0, c])
            give(2, c).start()
        o = mirrored(1)
        for c in range(chunks):
            give(2, c).wait_recv()
            cross(1, c).wait_recv()
            finish(c, o, from_mate.at[c], from_twin.at[1, c])

    for copy in gain_moves:
        copy.wait()
    gain_total = gain_out[i]
    for d in range(1, n_i):
        gain_total = gain_total + gain_in[d]
    gain_pseudo = gain_total * (1.0 / n_i)
    gain_velocity = outer_momentum * gain_moment_ref[...] + gain_pseudo
    gain_velocity_ref[...] = gain_velocity
    gain_updated_ref[...] = gain_ref[...] - outer_rate * (gain_pseudo + outer_momentum * gain_velocity)

    @when_end
    def _():
        for st in range(steps):
            lend_rows(st).wait_send()
        lend_slope().wait_send()
        for c in range(chunks):
            lend_later(c).wait_send()
            give(0, c).wait_send()

    @when_inner
    def _():
        for c in range(chunks):
            cross(0, c).wait_send()
            cross(1, c).wait_send()
            give(2, c).wait_send()
        a_sent(*end_rows)

    for copy in gain_copies:
        copy.wait_send()
    for t in range(n_i - 1):
        for c in range(chunks):

            @pl.when((i < n_i - 1) & (i - t >= 0))
            def _():
                z_copy(0, t, c, i - t).wait_send()

            @pl.when((i > 0) & (i + t <= n_i - 1))
            def _():
                z_copy(1, t, c, i + t).wait_send()

    a_sent(*own_rows)
    for c in range(chunks):
        for copy in stores(c):
            copy.wait()


def per_device(weight_master, gain_master, weight_moment, gain_moment, attended, stream, targets):
    n_i, n_s = lax.axis_size("island"), lax.axis_size("shard")
    _, steps, block, width = attended.shape
    _, _, tokens, cols = stream.shape
    piece = weight_master.shape[0]
    own = gain_master.shape[0]
    f32, bf16 = jnp.float32, jnp.bfloat16
    chunks = cols // LANES
    arrays = [
        ((piece, cols), f32),
        ((piece, cols), f32),
        ((steps, n_s, block, width), bf16),
        ((steps, n_s, block, 2 * piece), bf16),
        ((n_i, chunks, piece, LANES), bf16),
        ((1, min(512, piece), cols), bf16),
        ((n_i, piece, cols), f32),
        ((tokens, cols), f32),
        ((steps, chunks, tokens, LANES), bf16),
        ((steps, chunks, tokens, LANES), bf16),
        ((steps, tokens, cols), bf16),
        ((steps, tokens, cols), bf16),
        ((3, chunks, piece, LANES), bf16),
        ((chunks, piece, LANES), bf16),
        ((2, chunks, piece, LANES), bf16),
        ((steps, n_s, 4, tokens), f32),
        ((2, tokens), f32),
        ((n_i, 1, own), f32),
        ((n_i, 1, own), f32),
        ((n_i, 1, own), f32),
    ]
    held = sum(math.prod(shape) * jnp.dtype(kind).itemsize for shape, kind in arrays)
    if n_i != 4 or steps != 2 or own % LANES or held > 60e6:
        return general_device(weight_master, gain_master, weight_moment, gain_moment, attended, stream, targets)
    any_space = pl.BlockSpec(memory_space=pl.ANY)
    vmem = pl.BlockSpec(memory_space=pltpu.VMEM)
    dma = pltpu.SemaphoreType.DMA
    updated, gain_updated, velocity, gain_velocity = pl.pallas_call(
        functools.partial(kernel, n_i, n_s),
        out_shape=(
            jax.ShapeDtypeStruct((piece, cols), f32),
            jax.ShapeDtypeStruct((1, own), f32),
            jax.ShapeDtypeStruct((piece, cols), f32),
            jax.ShapeDtypeStruct((1, own), f32),
        ),
        in_specs=[any_space, vmem, any_space, vmem, any_space, any_space, any_space],
        out_specs=(any_space, vmem, any_space, vmem),
        scratch_shapes=[pltpu.VMEM(shape, kind) for shape, kind in arrays]
        + [
            dma((4 + steps,)),
            dma((2, chunks)),
            dma((2, n_i - 1, chunks)),
            dma((2, n_i - 1, chunks)),
            dma((steps, n_s - 1)),
            dma((steps, n_s - 1)),
            dma((steps, n_s - 1)),
            dma((steps, n_s - 1)),
            dma((steps,)),
            dma((steps,)),
            dma((steps, n_s)),
            dma((steps, n_s)),
            dma((2, n_i)),
            dma((2, n_i)),
            dma((1 + chunks,)),
            dma((1 + chunks,)),
            dma((chunks,)),
            dma((chunks,)),
            dma((2, chunks)),
            dma((2, chunks)),
        ],
        compiler_params=pltpu.CompilerParams(
            collective_id=0, has_side_effects=True, vmem_limit_bytes=67043328
        ),
    )(weight_master, gain_master[None], weight_moment, gain_moment[None], attended, stream, targets)
    return (updated, gain_updated[0], velocity, gain_velocity[0])


def solution(mesh):
    placed = (
        P("island", "shard"),
        P(("shard", "island")),
        P("island", "shard"),
        P(("shard", "island")),
        P("island", None, "shard", None),
        P("island", None, None, "shard"),
        P("island", None, None, "shard"),
    )
    return jax.shard_map(
        per_device,
        mesh=mesh,
        in_specs=placed,
        out_specs=(
            P("island", "shard"),
            P(("shard", "island")),
            P("island", "shard"),
            P(("shard", "island")),
        ),
        check_vma=False,
    )
```

```python
import functools
import math

import jax
import jax.numpy as jnp
from jax import lax
from jax.experimental import pallas as pl
from jax.experimental.pallas import tpu as pltpu
from jax.sharding import PartitionSpec as P

norm_epsilon = 1e-05
inner_rate = 0.05
beta_one = 0.9
beta_two = 0.95
adam_epsilon = 0.3
decay_rate = 0.1
outer_rate = 0.7
outer_momentum = 0.9

MESH = pl.DeviceIdType.MESH
LANES = 128
keep = 1.0 - inner_rate * decay_rate


def flip(index, bit):
    size = 1 << bit
    return index + size * (1 - 2 * (lax.div(index, size) % 2))


def first_update(grad):
    return grad / (jnp.abs(grad) + adam_epsilon)


def second_update(earlier, grad):
    first = (beta_one * (1.0 - beta_one)) * earlier + (1.0 - beta_one) * grad
    second = (beta_two * (1.0 - beta_two)) * earlier * earlier + (1.0 - beta_two) * grad * grad
    first_hat = first * (1.0 / (1.0 - beta_one**2))
    second_hat = second * (1.0 / (1.0 - beta_two**2))
    return first_hat / (jnp.sqrt(second_hat) + adam_epsilon)


def general_kernel(
    n_i, n_s, low_ref, gain_ref, rows_ref, stream_ref, goals_ref, total_ref, gain_total_ref,
    rows, anchor, later, grads, res, slope_low, stream, goals, from_left, from_right,
    stats, line, gains, gain_moves,
    local_sem, z_send, z_recv, a_send, a_recv, s_send, s_recv, g_send, g_recv, r_send, r_recv,
):
    i = lax.axis_index("island")
    s = lax.axis_index("shard")
    steps, _, block, width = rows.shape
    piece, cols = low_ref.shape
    tokens = n_s * block
    tiles = tokens // LANES
    scale = width ** (-0.5)
    depth = min(512, piece)
    tall = min(256, piece)

    barrier = pltpu.get_barrier_semaphore()
    for d in range(1, n_i):
        pl.semaphore_signal(barrier, inc=1, device_id=(lax.rem(i + d, n_i), s), device_id_type=MESH)
    for d in range(1, n_s):
        pl.semaphore_signal(barrier, inc=1, device_id=(i, lax.rem(s + d, n_s)), device_id_type=MESH)

    locals_ = [pltpu.make_async_copy(low_ref, anchor.at[i], local_sem.at[0])]
    for st in range(steps):
        locals_.append(pltpu.make_async_copy(rows_ref.at[0, st], rows.at[st, s], local_sem.at[1 + st]))
    locals_.append(pltpu.make_async_copy(stream_ref.at[0], stream, local_sem.at[1 + steps]))
    locals_.append(pltpu.make_async_copy(goals_ref.at[0], goals, local_sem.at[2 + steps]))
    for copy in locals_:
        copy.start()
    pl.semaphore_wait(barrier, n_i - 1 + n_s - 1)

    def remote(src, dst, send, recv, to):
        return pltpu.make_async_remote_copy(
            src_ref=src, dst_ref=dst, send_sem=send, recv_sem=recv, device_id=to, device_id_type=MESH
        )

    right, left = (lax.rem(i + 1, n_i), s), (lax.rem(i + n_i - 1, n_i), s)

    def z_copy(way, t, at):
        return remote(
            anchor.at[at], anchor.at[at], z_send.at[way, t], z_recv.at[way, t], right if way == 0 else left
        )

    def z_start(t):
        @pl.when((i < n_i - 1) & (i - t >= 0))
        def _():
            z_copy(0, t, i - t).start()

        @pl.when((i > 0) & (i + t <= n_i - 1))
        def _():
            z_copy(1, t, i + t).start()

    def z_wait(t):
        @pl.when(i - 1 - t >= 0)
        def _():
            z_copy(0, t, i - 1 - t).wait_recv()

        @pl.when(i + 1 + t <= n_i - 1)
        def _():
            z_copy(1, t, i + 1 + t).wait_recv()

    n_bits = n_s.bit_length() - 1
    orders = [list(range(1, n_bits)) + [0], list(range(n_bits - 1, 0, -1)) + [0]]

    def a_blocks(st, phase):
        order = orders[st % 2]
        found = []
        for m in range(1 << phase):
            at = s
            for q in range(phase):
                if (m >> q) & 1:
                    at = flip(at, order[q])
            found.append(at)
        return found

    def a_copy(st, phase, m, at):
        slot = (1 << phase) - 1 + m
        return remote(
            rows.at[st, at], rows.at[st, at], a_send.at[st, slot], a_recv.at[st, slot],
            (i, flip(s, orders[st % 2][phase])),
        )

    def a_start(phase):
        for st in range(steps):
            for m, at in enumerate(a_blocks(st, phase)):
                a_copy(st, phase, m, at).start()

    def a_wait(phase):
        for st in range(steps):
            for m, at in enumerate(a_blocks(st, phase)):
                a_copy(st, phase, m, flip(at, orders[st % 2][phase])).wait_recv()

    def to_islands(buffer, which):
        return [
            remote(
                buffer.at[0], buffer.at[d], g_send.at[which, d], g_recv.at[which, d],
                (lax.rem(i + d, n_i), s),
            )
            for d in range(1, n_i)
        ]

    locals_[0].wait()
    z_start(0)
    for copy in locals_[1 : 1 + steps]:
        copy.wait()
    a_start(0)
    gains[0] = gain_ref[...]
    gain_in = to_islands(gains, 0)
    for copy in gain_in:
        copy.start()
    res[...] = jnp.zeros_like(res)
    for copy in locals_[1 + steps :]:
        copy.wait()

    def project(st, weights, at):
        def body(k, _):
            start = pl.multiple_of(k * depth, depth)
            wide = pl.multiple_of(at * piece + k * depth, depth)
            part = rows[st, :, :, pl.ds(wide, depth)].reshape(tokens, depth)
            res[...] += jnp.dot(part, weights[at, pl.ds(start, depth), :], preferred_element_type=jnp.float32)
            return 0

        lax.fori_loop(0, piece // depth, body, 0)

    def project_arrived(t):
        @pl.when(i - 1 - t >= 0)
        def _():
            project(0, anchor, i - 1 - t)

        @pl.when(i + 1 + t <= n_i - 1)
        def _():
            project(0, anchor, i + 1 + t)

    events = [(2.0 * t + 2.6, "z", t) for t in range(n_i - 1)]
    events += [(2.0 * ((2 << p) - 1), "a", p) for p in range(n_bits - 1)]
    last = events[-1][0] if n_bits > 1 else 0.0
    events.append((last + 0.1, "a", n_bits - 1))
    gathered, ready = False, []
    for _, kind, at in sorted(events):
        if kind == "a":
            a_wait(at)
            if at + 1 < n_bits:
                a_start(at + 1)
            else:
                gathered = True
                project(0, anchor, i)
                for t in ready:
                    project_arrived(t)
        else:
            z_wait(at)
            if at + 1 < n_i - 1:
                z_start(at + 1)
            if gathered:
                project_arrived(at)
            else:
                ready.append(at)

    for copy in gain_in:
        copy.wait()
    gain_anchor = gains[0]
    for d in range(1, n_i):
        gain_anchor = gain_anchor + gains[d]
    gain = gain_anchor

    def fold(value):
        total = value[:, :LANES]
        for c in range(1, cols // LANES):
            total = total + value[:, c * LANES : (c + 1) * LANES]
        return jnp.sum(total.T, axis=0, keepdims=True)

    def spread(value):
        square = jnp.broadcast_to(value, (LANES, LANES)).T
        return jnp.concatenate([square] * (cols // LANES), axis=1)

    def row_stats(st, gain):
        def body(q, _):
            at = pl.ds(pl.multiple_of(q * LANES, LANES), LANES)
            r = stream[st, at, :].astype(jnp.float32) + res[at, :] * scale
            res[at, :] = r
            weighted = r * gain
            stats[st, 0, 0:1, at] = fold(r * r)
            stats[st, 0, 1:2, at] = fold(weighted * weighted)
            stats[st, 0, 2:3, at] = fold(weighted * goals[st, at, :].astype(jnp.float32))
            stats[st, 0, 3:4, at] = jnp.zeros((1, LANES), jnp.float32)
            return 0

        lax.fori_loop(0, tiles, body, 0)
        copies = [
            remote(
                stats.at[st, 0], stats.at[st, d], s_send.at[st, d], s_recv.at[st, d],
                (i, lax.rem(s + d, n_s)),
            )
            for d in range(1, n_s)
        ]
        for copy in copies:
            copy.start()
        for copy in copies:
            copy.wait()
        total = stats[st, 0]
        for d in range(1, n_s):
            total = total + stats[st, d]
        inverse = lax.rsqrt(total[0:1] * (1.0 / width) + norm_epsilon)
        slope = inverse * total[1:2] - total[2:3]
        line[0:1, :] = inverse
        line[1:2, :] = inverse * inverse * inverse * slope * (1.0 / width)

    def row_grads(st, gain):
        def body(q, total):
            at = pl.ds(pl.multiple_of(q * LANES, LANES), LANES)
            inverse, pull = spread(line[0:1, at]), spread(line[1:2, at])
            r = res[at, :]
            unit = r * inverse
            loss = unit * gain - goals[st, at, :].astype(jnp.float32)
            loss = loss.astype(jnp.bfloat16).astype(jnp.float32)
            slope_low[at, :] = (inverse * (loss * gain) - r * pull).astype(jnp.bfloat16)
            return total + jnp.sum(loss * unit, axis=0, keepdims=True)

        return lax.fori_loop(0, tiles, body, jnp.zeros((1, cols), jnp.float32))

    def weight_grad(st, wide):
        part = rows[st, :, :, pl.ds(pl.multiple_of(wide, tall), tall)].reshape(tokens, tall)
        return (
            lax.dot_general(
                part, slope_low[...], (((0,), (0,)), ((), ())), preferred_element_type=jnp.float32
            )
            * scale
        )

    row_stats(0, gain)
    gain_first = row_grads(0, gain)
    per_piece = piece // tall

    def step_one(q, _):
        o, j = q // per_piece, q % per_piece
        at = pl.ds(pl.multiple_of(j * tall, tall), tall)
        grad = weight_grad(0, q * tall)
        grads[o, at, :] = grad
        param = keep * anchor[o, at, :].astype(jnp.float32) - inner_rate * first_update(grad)
        later[o, at, :] = param.astype(jnp.bfloat16)
        return 0

    lax.fori_loop(0, n_i * per_piece, step_one, 0)
    gain_step = first_update(gain_first)
    gain = gain_anchor - inner_rate * gain_step

    res[...] = jnp.zeros_like(res)

    def project_later(at, _):
        project(1, later, at)
        return 0

    lax.fori_loop(0, n_i, project_later, 0)
    row_stats(1, gain)
    gain_second = row_grads(1, gain)
    gain_moves[0] = inner_rate * (gain_step + second_update(gain_first, gain_second))
    gain_out = to_islands(gain_moves, 1)
    for copy in gain_out:
        copy.start()

    def to_right(k):
        at = n_i - 1 - k
        return remote(later.at[at], from_left.at[k], r_send.at[0, k], r_recv.at[0, k], right)

    def to_left(k):
        return remote(later.at[k], from_right.at[k], r_send.at[1, k], r_recv.at[1, k], left)

    early = 1 - lax.div(2 * i, n_i)

    def owner_piece(q, _):
        o = q + early * (n_i - 1 - 2 * q)

        def step_two(j, _):
            at = pl.ds(pl.multiple_of(j * tall, tall), tall)
            grad = weight_grad(1, o * piece + j * tall)
            earlier = grads[o, at, :]
            moved = (1.0 - keep * keep) * anchor[o, at, :].astype(jnp.float32) + inner_rate * (
                keep * first_update(earlier) + second_update(earlier, grad)
            )
            grads[o, at, :] = moved
            later[o, at, :] = moved.astype(jnp.bfloat16)
            return 0

        lax.fori_loop(0, per_piece, step_two, 0)

        @pl.when((i == 0) & (o > 0))
        def _():
            to_right(n_i - 1 - o).start()

        @pl.when((i == n_i - 1) & (o < n_i - 1))
        def _():
            to_left(o).start()

        return 0

    lax.fori_loop(0, n_i, owner_piece, 0)

    def add(o, arrived, k):
        def body(j, _):
            at = pl.ds(pl.multiple_of(j * tall, tall), tall)
            later[o, at, :] = (grads[o, at, :] + arrived[k, at, :].astype(jnp.float32)).astype(jnp.bfloat16)
            return 0

        lax.fori_loop(0, per_piece, body, 0)

    for t in range(n_i - 1):
        k_right = t - i
        k_left = t - (n_i - 1 - i)

        @pl.when((i > 0) & (k_right >= 0) & (k_right < n_i - 1 - i))
        def _():
            to_right(k_right).wait_recv()
            add(n_i - 1 - k_right, from_left, k_right)
            to_right(k_right).start()

        @pl.when((i < n_i - 1) & (k_left >= 0) & (k_left < i))
        def _():
            to_left(k_left).wait_recv()
            add(k_left, from_right, k_left)
            to_left(k_left).start()

    for copy in gain_out:
        copy.wait()
    gain_total = gain_moves[0]
    for d in range(1, n_i):
        gain_total = gain_total + gain_moves[d]
    gain_total_ref[...] = gain_total

    total_ref[...] = grads[i]

    @pl.when(i > 0)
    def _():
        k = n_i - 1 - i
        to_right(k).wait_recv()
        total_ref[...] += from_left[k].astype(jnp.float32)

    @pl.when(i < n_i - 1)
    def _():
        to_left(i).wait_recv()
        total_ref[...] += from_right[i].astype(jnp.float32)

    for k in range(n_i - 1):

        @pl.when(k < n_i - 1 - i)
        def _(k=k):
            to_right(k).wait_send()

        @pl.when(k < i)
        def _(k=k):
            to_left(k).wait_send()

        @pl.when((i < n_i - 1) & (i - k >= 0))
        def _(k=k):
            z_copy(0, k, i - k).wait_send()

        @pl.when((i > 0) & (i + k <= n_i - 1))
        def _(k=k):
            z_copy(1, k, i + k).wait_send()

    for phase in range(n_bits):
        for st in range(steps):
            for m, at in enumerate(a_blocks(st, phase)):
                a_copy(st, phase, m, at).wait_send()


def general_device(weight_master, gain_master, weight_moment, gain_moment, attended, stream, targets):
    n_i, n_s = lax.axis_size("island"), lax.axis_size("shard")
    _, steps, block, width = attended.shape
    _, _, tokens, cols = stream.shape
    piece = weight_master.shape[0]
    own = gain_master.shape[0]
    offset = lax.axis_index("island") * own
    low = weight_master.astype(jnp.bfloat16)
    gain_low = gain_master.astype(jnp.bfloat16).astype(jnp.float32)
    gain_row = lax.dynamic_update_slice(jnp.zeros((1, cols), jnp.float32), gain_low[None], (0, offset))
    any_space = pl.BlockSpec(memory_space=pl.ANY)
    vmem = pl.BlockSpec(memory_space=pltpu.VMEM)
    f32, bf16 = jnp.float32, jnp.bfloat16
    dma = pltpu.SemaphoreType.DMA
    weight_summed, gain_summed = pl.pallas_call(
        functools.partial(general_kernel, n_i, n_s),
        out_shape=(
            jax.ShapeDtypeStruct((piece, cols), f32),
            jax.ShapeDtypeStruct((1, cols), f32),
        ),
        in_specs=[any_space, vmem, any_space, any_space, any_space],
        out_specs=(vmem, vmem),
        scratch_shapes=[
            pltpu.VMEM((steps, n_s, block, width), bf16),
            pltpu.VMEM((n_i, piece, cols), bf16),
            pltpu.VMEM((n_i, piece, cols), bf16),
            pltpu.VMEM((n_i, piece, cols), f32),
            pltpu.VMEM((tokens, cols), f32),
            pltpu.VMEM((tokens, cols), bf16),
            pltpu.VMEM((steps, tokens, cols), bf16),
            pltpu.VMEM((steps, tokens, cols), bf16),
            pltpu.VMEM((n_i - 1, piece, cols), bf16),
            pltpu.VMEM((n_i - 1, piece, cols), bf16),
            pltpu.VMEM((steps, n_s, 4, tokens), f32),
            pltpu.VMEM((2, tokens), f32),
            pltpu.VMEM((n_i, 1, cols), f32),
            pltpu.VMEM((n_i, 1, cols), f32),
            dma((3 + steps,)),
            dma((2, n_i - 1)),
            dma((2, n_i - 1)),
            dma((steps, n_s - 1)),
            dma((steps, n_s - 1)),
            dma((steps, n_s)),
            dma((steps, n_s)),
            dma((2, n_i)),
            dma((2, n_i)),
            dma((2, n_i - 1)),
            dma((2, n_i - 1)),
        ],
        compiler_params=pltpu.CompilerParams(
            collective_id=0, has_side_effects=True, vmem_limit_bytes=67043328
        ),
    )(low, gain_row, attended, stream, targets)
    weight_pseudo = weight_summed / n_i
    gain_pseudo = lax.dynamic_slice(gain_summed, (0, offset), (1, own))[0] / n_i
    weight_velocity = outer_momentum * weight_moment + weight_pseudo
    gain_velocity = outer_momentum * gain_moment + gain_pseudo
    weight_updated = weight_master - outer_rate * (weight_pseudo + outer_momentum * weight_velocity)
    gain_updated = gain_master - outer_rate * (gain_pseudo + outer_momentum * gain_velocity)
    return (weight_updated, gain_updated, weight_velocity, gain_velocity)


def outer_sum(grad_one, grad_two):
    first = (inner_rate * beta_one * (1.0 - beta_one) / (1.0 - beta_one**2)) * grad_one + (
        inner_rate * (1.0 - beta_one) / (1.0 - beta_one**2)
    ) * grad_two
    second = (beta_two * (1.0 - beta_two) / (1.0 - beta_two**2)) * (grad_one * grad_one) + (
        (1.0 - beta_two) / (1.0 - beta_two**2)
    ) * (grad_two * grad_two)
    root = jnp.sqrt(second) + adam_epsilon
    size = jnp.abs(grad_one) + adam_epsilon
    return ((inner_rate * keep) * grad_one * root + first * size) / (root * size)


def kernel(
    n_i, n_s, master_ref, gain_ref, moment_ref, gain_moment_ref, rows_ref, stream_ref, goals_ref,
    updated_ref, gain_updated_ref, velocity_ref, gain_velocity_ref,
    master, moment, rows, rows_h, anchor, ahead_a, ahead_b, grads, res, slope, slope_h, stream, goals,
    outgo, from_mate, from_twin, part_out, part_in, stats, line, gains, gain_out, gain_in,
    local_sem, z_send, z_recv, a_send, a_recv, p_send, p_recv, ha_send, ha_recv,
    s_send, s_recv, g_send, g_recv, r_send, r_recv, e_send, e_recv, m_send, m_recv,
):
    i = lax.axis_index("island")
    s = lax.axis_index("shard")
    steps, _, block, width = rows.shape
    _, chunks, piece, _ = anchor.shape
    cols = chunks * LANES
    own = gains.shape[2]
    tokens = n_s * block
    tiles = tokens // LANES
    scale = width ** (-0.5)
    depth = min(1024, piece)
    tall = min(256, piece)
    span = min(512, piece)
    f32, bf16 = jnp.float32, jnp.bfloat16

    is_left = i < n_i // 2
    is_end = (i == 0) | (i == n_i - 1)
    is_inner = (i > 0) & (i < n_i - 1)
    toward = jnp.where(is_left, 1, -1)
    mate = (jnp.where(is_end, i + toward, i - toward), s)
    twin = (n_i - 1 - i, s)

    def when_inner(f):
        pl.when(is_inner)(f)

    def when_end(f):
        pl.when(is_end)(f)

    def mirrored(o):
        return jnp.where(is_left, o, n_i - 1 - o)

    barrier = pltpu.get_barrier_semaphore()
    for d in range(1, n_i):
        pl.semaphore_signal(barrier, inc=1, device_id=(lax.rem(i + d, n_i), s), device_id_type=MESH)
    for d in range(1, n_s):
        pl.semaphore_signal(barrier, inc=1, device_id=(i, lax.rem(s + d, n_s)), device_id_type=MESH)

    load_master = pltpu.make_async_copy(master_ref, master, local_sem.at[0])
    load_rows = [
        pltpu.make_async_copy(rows_ref.at[0, st], rows.at[st, s], local_sem.at[1 + st]) for st in range(steps)
    ]
    load_rest = [
        pltpu.make_async_copy(stream_ref.at[0], stream, local_sem.at[1 + steps]),
        pltpu.make_async_copy(goals_ref.at[0], goals, local_sem.at[2 + steps]),
        pltpu.make_async_copy(moment_ref, moment, local_sem.at[3 + steps]),
    ]
    for copy in [load_master] + load_rows + load_rest:
        copy.start()

    def remote(src, dst, send, recv, to):
        return pltpu.make_async_remote_copy(
            src_ref=src, dst_ref=dst, send_sem=send, recv_sem=recv, device_id=to, device_id_type=MESH
        )

    def z_mate(o, c):
        return remote(anchor.at[o, c], anchor.at[o, c], z_send.at[0, o, c], z_recv.at[o, c], mate)

    def z_twin(o, c):
        return remote(anchor.at[o, c], anchor.at[o, c], z_send.at[1, o, c], z_recv.at[o, c], twin)

    n_bits = n_s.bit_length() - 1
    orders = [list(range(1, n_bits)) + [0], list(range(n_bits - 1, 0, -1)) + [0]]
    half = block // 2

    def a_blocks(h, phase):
        found = []
        for m in range(1 << phase):
            at = s
            for q in range(phase):
                if (m >> q) & 1:
                    at = flip(at, orders[h][q])
            found.append(at)
        return found

    def a_copy(which, h, phase, m, at):
        slot = (1 << phase) - 1 + m
        buffer = rows if which < steps else rows_h
        part = buffer.at[which % steps, at, pl.ds(h * half, half)]
        return remote(
            part, part, a_send.at[which, h, slot], a_recv.at[which, h, slot], (i, flip(s, orders[h][phase]))
        )

    def a_start(which, phase):
        for m in range(1 << phase):
            for h in range(2):
                a_copy(which, h, phase, m, a_blocks(h, phase)[m]).start()

    def a_wait(which, phase):
        for h in range(2):
            for m, at in enumerate(a_blocks(h, phase)):
                a_copy(which, h, phase, m, flip(at, orders[h][phase])).wait_recv()

    def a_sent(which):
        for phase in range(n_bits):
            for h in range(2):
                for m, at in enumerate(a_blocks(h, phase)):
                    a_copy(which, h, phase, m, at).wait_send()

    far = pl.multiple_of(jnp.where(is_left, width - 2 * piece, 0), LANES)

    def lend_rows(st):
        return remote(
            rows.at[st, s, :, pl.ds(far, 2 * piece)], rows_h.at[st, s], ha_send.at[st], ha_recv.at[st], mate
        )

    gains[i] = gain_ref[...].astype(bf16).astype(f32)
    gain_copies = [
        remote(gains.at[i], gains.at[i], g_send.at[0, d], g_recv.at[0, d], (lax.rem(i + d, n_i), s))
        for d in range(1, n_i)
    ]
    gain_waits = [
        remote(
            gains.at[lax.rem(i + n_i - d, n_i)], gains.at[lax.rem(i + n_i - d, n_i)],
            g_send.at[0, d], g_recv.at[0, d], (lax.rem(i + d, n_i), s),
        )
        for d in range(1, n_i)
    ]

    load_master.wait()

    def lower(j, _):
        at = pl.ds(pl.multiple_of(j * tall, tall), tall)
        for c in range(chunks):
            anchor[i, c, at, :] = master[at, c * LANES : (c + 1) * LANES].astype(bf16)
        return 0

    lax.fori_loop(0, piece // tall, lower, 0)
    for copy in load_rows:
        copy.wait()
    pl.semaphore_wait(barrier, n_i - 1 + n_s - 1)
    a_start(0, 0)

    @when_end
    def _():
        for c in range(chunks):
            z_mate(i, c).start()
            if c == 1:
                lend_rows(0).start()
        lend_rows(1).start()

    @when_inner
    def _():
        for c in range(chunks):
            z_mate(i, c).start()
            z_twin(i, c).start()

    for copy in gain_copies:
        copy.start()
    res[...] = jnp.zeros_like(res)
    for copy in load_rest:
        copy.wait()

    def joined(buffer, at, ds):
        return jnp.concatenate([buffer[at, c, ds, :] for c in range(chunks)], axis=1)

    def project(o, count=chunks):
        def body(k, _):
            start = pl.multiple_of(k * depth, depth)
            wide = pl.multiple_of(o * piece + k * depth, depth)
            part = rows[0, :, :, pl.ds(wide, depth)].reshape(tokens, depth)
            weights = [anchor[o, c, pl.ds(start, depth), :] for c in range(count)]
            res[:, : count * LANES] += jnp.dot(part, jnp.concatenate(weights, axis=1), preferred_element_type=f32)
            return 0

        lax.fori_loop(0, piece // depth, body, 0)

    def arrived(o, c):
        z_mate(o, c).wait_recv()

    held = chunks - 1
    near_far = jnp.where(is_left, n_i - 2, 0)
    groups = 2

    def part_copy():
        return remote(part_out, part_in, p_send, p_recv, mate)

    def project_for_end():
        weights = jnp.concatenate([anchor[near_far + k, held] for k in range(2)], axis=0)
        count = n_s // groups
        for g in range(groups):
            part = rows_h[0, g * count : (g + 1) * count].reshape(count * block, 2 * piece)
            part_out[g * count * block : (g + 1) * count * block, :] = jnp.dot(
                part, weights, preferred_element_type=f32
            ).astype(bf16)

    @when_end
    def _():
        one, two, three = mirrored(1), mirrored(2), mirrored(3)
        a_wait(0, 0)
        for p in range(1, n_bits):
            a_start(0, p)
            if p == 1:
                a_start(1, 0)
            a_wait(0, p)
        project(i)
        for c in range(chunks):
            arrived(one, c)
        project(one)
        a_wait(1, 0)
        a_start(1, 1)
        for c in range(held):
            arrived(two, c)
        project(two, held)
        for p in range(1, n_bits - 1):
            a_wait(1, p)
            a_start(1, p + 1)
        for c in range(held):
            arrived(three, c)
        project(three, held)
        part_copy().wait_recv()
        res[:, held * LANES :] += part_in[...].astype(f32)

    @when_inner
    def _():
        zero, two, three = mirrored(0), mirrored(2), mirrored(3)

        def from_end(c):
            arrived(zero, c)
            z_twin(zero, c).start()

        def from_far(o, c):
            arrived(o, c)
            if c < held:
                z_mate(o, c).start()

        from_end(0)
        from_far(two, 0)
        a_wait(0, 0)
        a_start(0, 1)
        from_end(1)
        from_far(two, 1)
        from_far(two, 2)
        from_far(two, 3)
        from_end(2)
        for p in range(1, n_bits - 1):
            a_wait(0, p)
            a_start(0, p + 1)
        lend_rows(0).wait_recv()
        a_start(2, 0)
        from_far(three, 0)
        a_wait(2, 0)
        a_start(2, 1)
        a_start(1, 0)
        from_end(3)
        a_wait(0, n_bits - 1)
        project(i)
        from_far(three, 1)
        project(zero)
        for p in range(1, n_bits - 1):
            a_wait(2, p)
            a_start(2, p + 1)
        from_far(three, 2)
        project(two)
        from_far(three, 3)
        a_wait(2, n_bits - 1)
        project_for_end()
        part_copy().start()
        z_mate(two, held).start()
        z_mate(three, held).start()
        project(three)

    for copy in gain_waits:
        copy.wait_recv()
    gain_anchor = jnp.concatenate([gains[j] for j in range(n_i)], axis=1)
    gain = gain_anchor

    def fold(value):
        total = value[:, :LANES]
        for c in range(1, chunks):
            total = total + value[:, c * LANES : (c + 1) * LANES]
        return jnp.sum(total.T, axis=0, keepdims=True)

    def spread(value):
        square = jnp.broadcast_to(value, (LANES, LANES)).T
        return jnp.concatenate([square] * chunks, axis=1)

    def row_stats(st, gain, between=None):
        def body(q, _):
            at = pl.ds(pl.multiple_of(q * LANES, LANES), LANES)
            r = stream[st, at, :].astype(f32) + res[at, :] * scale
            res[at, :] = r
            weighted = r * gain
            stats[st, 0, 0:1, at] = fold(r * r)
            stats[st, 0, 1:2, at] = fold(weighted * weighted)
            stats[st, 0, 2:3, at] = fold(weighted * goals[st, at, :].astype(f32))
            stats[st, 0, 3:4, at] = jnp.zeros((1, LANES), f32)
            return 0

        lax.fori_loop(0, tiles, body, 0)
        copies = [
            remote(
                stats.at[st, 0], stats.at[st, d], s_send.at[st, d], s_recv.at[st, d],
                (i, lax.rem(s + d, n_s)),
            )
            for d in range(1, n_s)
        ]
        for copy in copies:
            copy.start()
        if between is not None:
            between()
        for copy in copies:
            copy.wait()
        total = stats[st, 0]
        for d in range(1, n_s):
            total = total + stats[st, d]
        inverse = lax.rsqrt(total[0:1] * (1.0 / width) + norm_epsilon)
        pull = inverse * total[1:2] - total[2:3]
        line[0:1, :] = inverse
        line[1:2, :] = inverse * inverse * inverse * pull * (1.0 / width)

    def row_grads(st, gain):
        def body(q, total):
            at = pl.ds(pl.multiple_of(q * LANES, LANES), LANES)
            inverse, pull = spread(line[0:1, at]), spread(line[1:2, at])
            r = res[at, :]
            unit = r * inverse
            loss = unit * gain - goals[st, at, :].astype(f32)
            loss = loss.astype(bf16).astype(f32)
            low = (inverse * (loss * gain) - r * pull).astype(bf16)
            for c in range(chunks):
                slope[st, c, at, :] = low[:, c * LANES : (c + 1) * LANES]
            return total + jnp.sum(loss * unit, axis=0, keepdims=True)

        return lax.fori_loop(0, tiles, body, jnp.zeros((1, cols), f32))

    def product(part, against):
        return lax.dot_general(part, against, (((0,), (0,)), ((), ())), preferred_element_type=f32) * scale

    def weight_grad(st, wide, size):
        part = rows[st, :, :, pl.ds(pl.multiple_of(wide, size), size)].reshape(tokens, size)
        return product(part, joined(slope, st, slice(None)))

    @when_inner
    def _():
        a_wait(1, 0)

    def more_rows():
        @when_inner
        def _():
            a_start(1, 1)
            lend_rows(1).wait_recv()
            a_start(3, 0)

    row_stats(0, gain, more_rows)
    gain_first = row_grads(0, gain)
    res[...] = jnp.zeros_like(res)

    def lend_slope():
        return remote(slope.at[0], slope_h.at[0], r_send.at[0], r_recv.at[0], mate)

    def lend_later(c):
        return remote(slope.at[1, c], slope_h.at[1, c], r_send.at[1 + c], r_recv.at[1 + c], mate)

    when_end(lambda: lend_slope().start())

    @when_inner
    def _():
        for p in range(1, n_bits - 1):
            a_wait(1, p)
            a_start(1, p + 1)
        a_wait(3, 0)
        a_start(3, 1)

    a_wait(1, n_bits - 1)

    spans = width // span
    per_piece = piece // span

    def place(q):
        return mirrored(q // per_piece), q % per_piece

    def step_one(q, ahead):
        o, j = place(q)
        at = pl.ds(pl.multiple_of(j * span, span), span)
        grad = weight_grad(0, o * piece + j * span, span)
        grads[o, at, :] = grad
        param = keep * joined(anchor, o, at).astype(f32) - inner_rate * first_update(grad)
        ahead[...] = param.astype(bf16)

    def project_later(q, ahead):
        o, j = place(q)
        wide = pl.multiple_of(o * piece + j * span, span)
        part = rows[1, :, :, pl.ds(wide, span)].reshape(tokens, span)
        res[...] += jnp.dot(part, ahead[...], preferred_element_type=f32)

    def both(t, _):
        for k in (2, 3):

            @pl.when(is_end & (2 * t == k * per_piece))
            def _():
                arrived(mirrored(k), held)

        project_later(jnp.maximum(2 * t - 1, 0), ahead_b)
        step_one(2 * t, ahead_a)
        project_later(2 * t, ahead_a)
        step_one(2 * t + 1, ahead_b)
        return 0

    ahead_b[...] = jnp.zeros_like(ahead_b)
    lax.fori_loop(0, spans // 2, both, 0)
    project_later(spans - 1, ahead_b)
    gain_step = first_update(gain_first)
    gain = gain_anchor - inner_rate * gain_step

    @when_inner
    def _():
        for p in range(1, n_bits - 1):
            a_wait(3, p)
            a_start(3, p + 1)

    row_stats(1, gain)
    gain_second = row_grads(1, gain)
    gain_move = inner_rate * (gain_step + second_update(gain_first, gain_second))
    for j in range(n_i):
        gain_out[j] = gain_move[:, j * own : (j + 1) * own]

    @when_end
    def _():
        for c in range(chunks):
            lend_later(c).start()

    gain_moves = [
        remote(
            gain_out.at[lax.rem(i + d, n_i)], gain_in.at[d], g_send.at[1, d], g_recv.at[1, d],
            (lax.rem(i + d, n_i), s),
        )
        for d in range(1, n_i)
    ]
    for copy in gain_moves:
        copy.start()

    def move(o):
        def body(j, _):
            at = pl.ds(pl.multiple_of(j * tall, tall), tall)
            grad = weight_grad(1, o * piece + j * tall, tall)
            grads[o, at, :] = outer_sum(grads[o, at, :], grad)
            return 0

        lax.fori_loop(0, piece // tall, body, 0)

    def give(slot, c):
        return remote(outgo.at[slot, c], from_mate.at[c], e_send.at[c], e_recv.at[c], mate)

    def cross(slot, c):
        return remote(outgo.at[slot, c], from_twin.at[slot, c], m_send.at[slot, c], m_recv.at[slot, c], twin)

    def pack(slot, c, o, *others):
        lanes = slice(c * LANES, (c + 1) * LANES)

        def body(j, _):
            at = pl.ds(pl.multiple_of(j * tall, tall), tall)
            total = grads[o, at, lanes]
            for other in others:
                total = total + other[at, :].astype(f32)
            outgo[slot, c, at, :] = total.astype(bf16)
            return 0

        lax.fori_loop(0, piece // tall, body, 0)

    def finish(c, o, *others):
        lanes = slice(c * LANES, (c + 1) * LANES)

        def body(j, _):
            at = pl.ds(pl.multiple_of(j * tall, tall), tall)
            total = grads[o, at, lanes]
            for other in others:
                total = total + other[at, :].astype(f32)
            outer = master[at, lanes]
            pseudo = total * (1.0 / n_i) + (1.0 - keep * keep) * outer.astype(bf16).astype(f32)
            velocity = outer_momentum * moment[at, lanes] + pseudo
            velocity_ref[at, lanes] = velocity
            updated_ref[at, lanes] = outer - outer_rate * (pseudo + outer_momentum * velocity)
            return 0

        lax.fori_loop(0, piece // tall, body, 0)
    @when_end
    def _():
        o = mirrored(1)
        move(o)
        for c in range(chunks):
            pack(0, c, o)
        for c in range(chunks):
            give(0, c).start()
        o = mirrored(0)
        move(o)
        for c in range(chunks):
            give(0, c).wait_recv()
            finish(c, o, from_mate.at[c])

    def help_end(slot, c, o):
        base = (o - near_far) * piece
        lanes = slice(c * LANES, (c + 1) * LANES)

        def body(j, _):
            at = pl.ds(pl.multiple_of(j * tall, tall), tall)
            wide = pl.ds(pl.multiple_of(base + j * tall, tall), tall)
            pair = [
                product(rows_h[st, :, :, wide].reshape(tokens, tall), slope_h[st, c]) for st in range(steps)
            ]
            outgo[slot, c, at, :] = (grads[o, at, lanes] + outer_sum(*pair)).astype(bf16)
            return 0

        lax.fori_loop(0, piece // tall, body, 0)

    @when_inner
    def _():
        def help_and_cross(slot, c):
            help_end(slot, c, mirrored(3 - slot))
            cross(slot, c).start()

        def forward(c):
            cross(0, c).wait_recv()
            pack(2, c, mirrored(0), from_twin.at[0, c])
            give(2, c).start()

        move(mirrored(3))
        move(mirrored(0))
        a_wait(3, n_bits - 1)
        lend_slope().wait_recv()
        for c in range(chunks):
            lend_later(c).wait_recv()
            help_and_cross(0, c)
            if c == 0:
                move(mirrored(2))
            if c == chunks - 2:
                move(mirrored(1))
        for c in range(chunks):
            help_and_cross(1, c)
            forward(c)
        for c in range(chunks):
            give(2, c).wait_recv()
            cross(1, c).wait_recv()
            finish(c, mirrored(1), from_mate.at[c], from_twin.at[1, c])

    for copy in gain_moves:
        copy.wait()
    gain_total = gain_out[i]
    for d in range(1, n_i):
        gain_total = gain_total + gain_in[d]
    gain_pseudo = gain_total * (1.0 / n_i)
    gain_velocity = outer_momentum * gain_moment_ref[...] + gain_pseudo
    gain_velocity_ref[...] = gain_velocity
    gain_updated_ref[...] = gain_ref[...] - outer_rate * (gain_pseudo + outer_momentum * gain_velocity)

    @when_end
    def _():
        for st in range(steps):
            lend_rows(st).wait_send()
        lend_slope().wait_send()
        for c in range(chunks):
            z_mate(i, c).wait_send()
        for c in range(chunks):
            lend_later(c).wait_send()
            give(0, c).wait_send()

    @when_inner
    def _():
        for c in range(chunks):
            cross(0, c).wait_send()
            cross(1, c).wait_send()
            give(2, c).wait_send()
        part_copy().wait_send()
        a_sent(2)
        a_sent(3)
        for c in range(chunks):
            z_mate(i, c).wait_send()
            z_twin(i, c).wait_send()
            z_twin(mirrored(0), c).wait_send()
            z_mate(mirrored(2), c).wait_send()
            z_mate(mirrored(3), c).wait_send()

    for copy in gain_copies:
        copy.wait_send()
    a_sent(0)
    a_sent(1)


def per_device(weight_master, gain_master, weight_moment, gain_moment, attended, stream, targets):
    n_i, n_s = lax.axis_size("island"), lax.axis_size("shard")
    _, steps, block, width = attended.shape
    _, _, tokens, cols = stream.shape
    piece = weight_master.shape[0]
    own = gain_master.shape[0]
    f32, bf16 = jnp.float32, jnp.bfloat16
    chunks = cols // LANES
    arrays = [
        ((piece, cols), f32),
        ((piece, cols), f32),
        ((steps, n_s, block, width), bf16),
        ((steps, n_s, block, 2 * piece), bf16),
        ((n_i, chunks, piece, LANES), bf16),
        ((min(512, piece), cols), bf16),
        ((min(512, piece), cols), bf16),
        ((n_i, piece, cols), f32),
        ((tokens, cols), f32),
        ((steps, chunks, tokens, LANES), bf16),
        ((steps, chunks, tokens, LANES), bf16),
        ((steps, tokens, cols), bf16),
        ((steps, tokens, cols), bf16),
        ((3, chunks, piece, LANES), bf16),
        ((chunks, piece, LANES), bf16),
        ((2, chunks, piece, LANES), bf16),
        ((tokens, LANES), bf16),
        ((tokens, LANES), bf16),
        ((steps, n_s, 4, tokens), f32),
        ((2, tokens), f32),
        ((n_i, 1, own), f32),
        ((n_i, 1, own), f32),
        ((n_i, 1, own), f32),
    ]
    held = sum(math.prod(shape) * jnp.dtype(kind).itemsize for shape, kind in arrays)
    if n_i != 4 or steps != 2 or own % LANES or chunks < 2 or block % 32 or n_s < 4 or held > 60e6:
        return general_device(weight_master, gain_master, weight_moment, gain_moment, attended, stream, targets)
    any_space = pl.BlockSpec(memory_space=pl.ANY)
    vmem = pl.BlockSpec(memory_space=pltpu.VMEM)
    dma = pltpu.SemaphoreType.DMA
    updated, gain_updated, velocity, gain_velocity = pl.pallas_call(
        functools.partial(kernel, n_i, n_s),
        out_shape=(
            jax.ShapeDtypeStruct((piece, cols), f32),
            jax.ShapeDtypeStruct((1, own), f32),
            jax.ShapeDtypeStruct((piece, cols), f32),
            jax.ShapeDtypeStruct((1, own), f32),
        ),
        in_specs=[any_space, vmem, any_space, vmem, any_space, any_space, any_space],
        out_specs=(vmem, vmem, vmem, vmem),
        scratch_shapes=[pltpu.VMEM(shape, kind) for shape, kind in arrays]
        + [
            dma((4 + steps,)),
            dma((2, n_i, chunks)),
            dma((n_i, chunks)),
            dma((2 * steps, 2, n_s - 1)),
            dma((2 * steps, 2, n_s - 1)),
            dma(()),
            dma(()),
            dma((steps,)),
            dma((steps,)),
            dma((steps, n_s)),
            dma((steps, n_s)),
            dma((2, n_i)),
            dma((2, n_i)),
            dma((1 + chunks,)),
            dma((1 + chunks,)),
            dma((chunks,)),
            dma((chunks,)),
            dma((2, chunks)),
            dma((2, chunks)),
        ],
        compiler_params=pltpu.CompilerParams(
            collective_id=0, has_side_effects=True, vmem_limit_bytes=67043328
        ),
    )(weight_master, gain_master[None], weight_moment, gain_moment[None], attended, stream, targets)
    return (updated, gain_updated[0], velocity, gain_velocity[0])


def solution(mesh):
    placed = (
        P("island", "shard"),
        P(("shard", "island")),
        P("island", "shard"),
        P(("shard", "island")),
        P("island", None, "shard", None),
        P("island", None, None, "shard"),
        P("island", None, None, "shard"),
    )
    return jax.shard_map(
        per_device,
        mesh=mesh,
        in_specs=placed,
        out_specs=(
            P("island", "shard"),
            P(("shard", "island")),
            P("island", "shard"),
            P(("shard", "island")),
        ),
        check_vma=False,
    )
```

```python
import functools
import math

import jax
import jax.numpy as jnp
from jax import lax
from jax.experimental import pallas as pl
from jax.experimental.pallas import tpu as pltpu
from jax.sharding import PartitionSpec as P

norm_epsilon = 1e-05
inner_rate = 0.05
beta_one = 0.9
beta_two = 0.95
adam_epsilon = 0.3
decay_rate = 0.1
outer_rate = 0.7
outer_momentum = 0.9

MESH = pl.DeviceIdType.MESH
LANES = 128
keep = 1.0 - inner_rate * decay_rate


def flip(index, bit):
    size = 1 << bit
    return index + size * (1 - 2 * (lax.div(index, size) % 2))


def first_update(grad):
    return grad / (jnp.abs(grad) + adam_epsilon)


def second_update(earlier, grad):
    first = (beta_one * (1.0 - beta_one)) * earlier + (1.0 - beta_one) * grad
    second = (beta_two * (1.0 - beta_two)) * earlier * earlier + (1.0 - beta_two) * grad * grad
    first_hat = first * (1.0 / (1.0 - beta_one**2))
    second_hat = second * (1.0 / (1.0 - beta_two**2))
    return first_hat / (jnp.sqrt(second_hat) + adam_epsilon)


def general_kernel(
    n_i, n_s, low_ref, gain_ref, rows_ref, stream_ref, goals_ref, total_ref, gain_total_ref,
    rows, anchor, later, grads, res, slope_low, stream, goals, from_left, from_right,
    stats, line, gains, gain_moves,
    local_sem, z_send, z_recv, a_send, a_recv, s_send, s_recv, g_send, g_recv, r_send, r_recv,
):
    i = lax.axis_index("island")
    s = lax.axis_index("shard")
    steps, _, block, width = rows.shape
    piece, cols = low_ref.shape
    tokens = n_s * block
    tiles = tokens // LANES
    scale = width ** (-0.5)
    depth = min(512, piece)
    tall = min(256, piece)

    barrier = pltpu.get_barrier_semaphore()
    for d in range(1, n_i):
        pl.semaphore_signal(barrier, inc=1, device_id=(lax.rem(i + d, n_i), s), device_id_type=MESH)
    for d in range(1, n_s):
        pl.semaphore_signal(barrier, inc=1, device_id=(i, lax.rem(s + d, n_s)), device_id_type=MESH)

    locals_ = [pltpu.make_async_copy(low_ref, anchor.at[i], local_sem.at[0])]
    for st in range(steps):
        locals_.append(pltpu.make_async_copy(rows_ref.at[0, st], rows.at[st, s], local_sem.at[1 + st]))
    locals_.append(pltpu.make_async_copy(stream_ref.at[0], stream, local_sem.at[1 + steps]))
    locals_.append(pltpu.make_async_copy(goals_ref.at[0], goals, local_sem.at[2 + steps]))
    for copy in locals_:
        copy.start()
    pl.semaphore_wait(barrier, n_i - 1 + n_s - 1)

    def remote(src, dst, send, recv, to):
        return pltpu.make_async_remote_copy(
            src_ref=src, dst_ref=dst, send_sem=send, recv_sem=recv, device_id=to, device_id_type=MESH
        )

    right, left = (lax.rem(i + 1, n_i), s), (lax.rem(i + n_i - 1, n_i), s)

    def z_copy(way, t, at):
        return remote(
            anchor.at[at], anchor.at[at], z_send.at[way, t], z_recv.at[way, t], right if way == 0 else left
        )

    def z_start(t):
        @pl.when((i < n_i - 1) & (i - t >= 0))
        def _():
            z_copy(0, t, i - t).start()

        @pl.when((i > 0) & (i + t <= n_i - 1))
        def _():
            z_copy(1, t, i + t).start()

    def z_wait(t):
        @pl.when(i - 1 - t >= 0)
        def _():
            z_copy(0, t, i - 1 - t).wait_recv()

        @pl.when(i + 1 + t <= n_i - 1)
        def _():
            z_copy(1, t, i + 1 + t).wait_recv()

    n_bits = n_s.bit_length() - 1
    orders = [list(range(1, n_bits)) + [0], list(range(n_bits - 1, 0, -1)) + [0]]

    def a_blocks(st, phase):
        order = orders[st % 2]
        found = []
        for m in range(1 << phase):
            at = s
            for q in range(phase):
                if (m >> q) & 1:
                    at = flip(at, order[q])
            found.append(at)
        return found

    def a_copy(st, phase, m, at):
        slot = (1 << phase) - 1 + m
        return remote(
            rows.at[st, at], rows.at[st, at], a_send.at[st, slot], a_recv.at[st, slot],
            (i, flip(s, orders[st % 2][phase])),
        )

    def a_start(phase):
        for st in range(steps):
            for m, at in enumerate(a_blocks(st, phase)):
                a_copy(st, phase, m, at).start()

    def a_wait(phase):
        for st in range(steps):
            for m, at in enumerate(a_blocks(st, phase)):
                a_copy(st, phase, m, flip(at, orders[st % 2][phase])).wait_recv()

    def to_islands(buffer, which):
        return [
            remote(
                buffer.at[0], buffer.at[d], g_send.at[which, d], g_recv.at[which, d],
                (lax.rem(i + d, n_i), s),
            )
            for d in range(1, n_i)
        ]

    locals_[0].wait()
    z_start(0)
    for copy in locals_[1 : 1 + steps]:
        copy.wait()
    a_start(0)
    gains[0] = gain_ref[...]
    gain_in = to_islands(gains, 0)
    for copy in gain_in:
        copy.start()
    res[...] = jnp.zeros_like(res)
    for copy in locals_[1 + steps :]:
        copy.wait()

    def project(st, weights, at):
        def body(k, _):
            start = pl.multiple_of(k * depth, depth)
            wide = pl.multiple_of(at * piece + k * depth, depth)
            part = rows[st, :, :, pl.ds(wide, depth)].reshape(tokens, depth)
            res[...] += jnp.dot(part, weights[at, pl.ds(start, depth), :], preferred_element_type=jnp.float32)
            return 0

        lax.fori_loop(0, piece // depth, body, 0)

    def project_arrived(t):
        @pl.when(i - 1 - t >= 0)
        def _():
            project(0, anchor, i - 1 - t)

        @pl.when(i + 1 + t <= n_i - 1)
        def _():
            project(0, anchor, i + 1 + t)

    events = [(2.0 * t + 2.6, "z", t) for t in range(n_i - 1)]
    events += [(2.0 * ((2 << p) - 1), "a", p) for p in range(n_bits - 1)]
    last = events[-1][0] if n_bits > 1 else 0.0
    events.append((last + 0.1, "a", n_bits - 1))
    gathered, ready = False, []
    for _, kind, at in sorted(events):
        if kind == "a":
            a_wait(at)
            if at + 1 < n_bits:
                a_start(at + 1)
            else:
                gathered = True
                project(0, anchor, i)
                for t in ready:
                    project_arrived(t)
        else:
            z_wait(at)
            if at + 1 < n_i - 1:
                z_start(at + 1)
            if gathered:
                project_arrived(at)
            else:
                ready.append(at)

    for copy in gain_in:
        copy.wait()
    gain_anchor = gains[0]
    for d in range(1, n_i):
        gain_anchor = gain_anchor + gains[d]
    gain = gain_anchor

    def fold(value):
        total = value[:, :LANES]
        for c in range(1, cols // LANES):
            total = total + value[:, c * LANES : (c + 1) * LANES]
        return jnp.sum(total.T, axis=0, keepdims=True)

    def spread(value):
        square = jnp.broadcast_to(value, (LANES, LANES)).T
        return jnp.concatenate([square] * (cols // LANES), axis=1)

    def row_stats(st, gain):
        def body(q, _):
            at = pl.ds(pl.multiple_of(q * LANES, LANES), LANES)
            r = stream[st, at, :].astype(jnp.float32) + res[at, :] * scale
            res[at, :] = r
            weighted = r * gain
            stats[st, 0, 0:1, at] = fold(r * r)
            stats[st, 0, 1:2, at] = fold(weighted * weighted)
            stats[st, 0, 2:3, at] = fold(weighted * goals[st, at, :].astype(jnp.float32))
            stats[st, 0, 3:4, at] = jnp.zeros((1, LANES), jnp.float32)
            return 0

        lax.fori_loop(0, tiles, body, 0)
        copies = [
            remote(
                stats.at[st, 0], stats.at[st, d], s_send.at[st, d], s_recv.at[st, d],
                (i, lax.rem(s + d, n_s)),
            )
            for d in range(1, n_s)
        ]
        for copy in copies:
            copy.start()
        for copy in copies:
            copy.wait()
        total = stats[st, 0]
        for d in range(1, n_s):
            total = total + stats[st, d]
        inverse = lax.rsqrt(total[0:1] * (1.0 / width) + norm_epsilon)
        slope = inverse * total[1:2] - total[2:3]
        line[0:1, :] = inverse
        line[1:2, :] = inverse * inverse * inverse * slope * (1.0 / width)

    def row_grads(st, gain):
        def body(q, total):
            at = pl.ds(pl.multiple_of(q * LANES, LANES), LANES)
            inverse, pull = spread(line[0:1, at]), spread(line[1:2, at])
            r = res[at, :]
            unit = r * inverse
            loss = unit * gain - goals[st, at, :].astype(jnp.float32)
            loss = loss.astype(jnp.bfloat16).astype(jnp.float32)
            slope_low[at, :] = (inverse * (loss * gain) - r * pull).astype(jnp.bfloat16)
            return total + jnp.sum(loss * unit, axis=0, keepdims=True)

        return lax.fori_loop(0, tiles, body, jnp.zeros((1, cols), jnp.float32))

    def weight_grad(st, wide):
        part = rows[st, :, :, pl.ds(pl.multiple_of(wide, tall), tall)].reshape(tokens, tall)
        return (
            lax.dot_general(
                part, slope_low[...], (((0,), (0,)), ((), ())), preferred_element_type=jnp.float32
            )
            * scale
        )

    row_stats(0, gain)
    gain_first = row_grads(0, gain)
    per_piece = piece // tall

    def step_one(q, _):
        o, j = q // per_piece, q % per_piece
        at = pl.ds(pl.multiple_of(j * tall, tall), tall)
        grad = weight_grad(0, q * tall)
        grads[o, at, :] = grad
        param = keep * anchor[o, at, :].astype(jnp.float32) - inner_rate * first_update(grad)
        later[o, at, :] = param.astype(jnp.bfloat16)
        return 0

    lax.fori_loop(0, n_i * per_piece, step_one, 0)
    gain_step = first_update(gain_first)
    gain = gain_anchor - inner_rate * gain_step

    res[...] = jnp.zeros_like(res)

    def project_later(at, _):
        project(1, later, at)
        return 0

    lax.fori_loop(0, n_i, project_later, 0)
    row_stats(1, gain)
    gain_second = row_grads(1, gain)
    gain_moves[0] = inner_rate * (gain_step + second_update(gain_first, gain_second))
    gain_out = to_islands(gain_moves, 1)
    for copy in gain_out:
        copy.start()

    def to_right(k):
        at = n_i - 1 - k
        return remote(later.at[at], from_left.at[k], r_send.at[0, k], r_recv.at[0, k], right)

    def to_left(k):
        return remote(later.at[k], from_right.at[k], r_send.at[1, k], r_recv.at[1, k], left)

    early = 1 - lax.div(2 * i, n_i)

    def owner_piece(q, _):
        o = q + early * (n_i - 1 - 2 * q)

        def step_two(j, _):
            at = pl.ds(pl.multiple_of(j * tall, tall), tall)
            grad = weight_grad(1, o * piece + j * tall)
            earlier = grads[o, at, :]
            moved = (1.0 - keep * keep) * anchor[o, at, :].astype(jnp.float32) + inner_rate * (
                keep * first_update(earlier) + second_update(earlier, grad)
            )
            grads[o, at, :] = moved
            later[o, at, :] = moved.astype(jnp.bfloat16)
            return 0

        lax.fori_loop(0, per_piece, step_two, 0)

        @pl.when((i == 0) & (o > 0))
        def _():
            to_right(n_i - 1 - o).start()

        @pl.when((i == n_i - 1) & (o < n_i - 1))
        def _():
            to_left(o).start()

        return 0

    lax.fori_loop(0, n_i, owner_piece, 0)

    def add(o, arrived, k):
        def body(j, _):
            at = pl.ds(pl.multiple_of(j * tall, tall), tall)
            later[o, at, :] = (grads[o, at, :] + arrived[k, at, :].astype(jnp.float32)).astype(jnp.bfloat16)
            return 0

        lax.fori_loop(0, per_piece, body, 0)

    for t in range(n_i - 1):
        k_right = t - i
        k_left = t - (n_i - 1 - i)

        @pl.when((i > 0) & (k_right >= 0) & (k_right < n_i - 1 - i))
        def _():
            to_right(k_right).wait_recv()
            add(n_i - 1 - k_right, from_left, k_right)
            to_right(k_right).start()

        @pl.when((i < n_i - 1) & (k_left >= 0) & (k_left < i))
        def _():
            to_left(k_left).wait_recv()
            add(k_left, from_right, k_left)
            to_left(k_left).start()

    for copy in gain_out:
        copy.wait()
    gain_total = gain_moves[0]
    for d in range(1, n_i):
        gain_total = gain_total + gain_moves[d]
    gain_total_ref[...] = gain_total

    total_ref[...] = grads[i]

    @pl.when(i > 0)
    def _():
        k = n_i - 1 - i
        to_right(k).wait_recv()
        total_ref[...] += from_left[k].astype(jnp.float32)

    @pl.when(i < n_i - 1)
    def _():
        to_left(i).wait_recv()
        total_ref[...] += from_right[i].astype(jnp.float32)

    for k in range(n_i - 1):

        @pl.when(k < n_i - 1 - i)
        def _(k=k):
            to_right(k).wait_send()

        @pl.when(k < i)
        def _(k=k):
            to_left(k).wait_send()

        @pl.when((i < n_i - 1) & (i - k >= 0))
        def _(k=k):
            z_copy(0, k, i - k).wait_send()

        @pl.when((i > 0) & (i + k <= n_i - 1))
        def _(k=k):
            z_copy(1, k, i + k).wait_send()

    for phase in range(n_bits):
        for st in range(steps):
            for m, at in enumerate(a_blocks(st, phase)):
                a_copy(st, phase, m, at).wait_send()


def general_device(weight_master, gain_master, weight_moment, gain_moment, attended, stream, targets):
    n_i, n_s = lax.axis_size("island"), lax.axis_size("shard")
    _, steps, block, width = attended.shape
    _, _, tokens, cols = stream.shape
    piece = weight_master.shape[0]
    own = gain_master.shape[0]
    offset = lax.axis_index("island") * own
    low = weight_master.astype(jnp.bfloat16)
    gain_low = gain_master.astype(jnp.bfloat16).astype(jnp.float32)
    gain_row = lax.dynamic_update_slice(jnp.zeros((1, cols), jnp.float32), gain_low[None], (0, offset))
    any_space = pl.BlockSpec(memory_space=pl.ANY)
    vmem = pl.BlockSpec(memory_space=pltpu.VMEM)
    f32, bf16 = jnp.float32, jnp.bfloat16
    dma = pltpu.SemaphoreType.DMA
    weight_summed, gain_summed = pl.pallas_call(
        functools.partial(general_kernel, n_i, n_s),
        out_shape=(
            jax.ShapeDtypeStruct((piece, cols), f32),
            jax.ShapeDtypeStruct((1, cols), f32),
        ),
        in_specs=[any_space, vmem, any_space, any_space, any_space],
        out_specs=(vmem, vmem),
        scratch_shapes=[
            pltpu.VMEM((steps, n_s, block, width), bf16),
            pltpu.VMEM((n_i, piece, cols), bf16),
            pltpu.VMEM((n_i, piece, cols), bf16),
            pltpu.VMEM((n_i, piece, cols), f32),
            pltpu.VMEM((tokens, cols), f32),
            pltpu.VMEM((tokens, cols), bf16),
            pltpu.VMEM((steps, tokens, cols), bf16),
            pltpu.VMEM((steps, tokens, cols), bf16),
            pltpu.VMEM((n_i - 1, piece, cols), bf16),
            pltpu.VMEM((n_i - 1, piece, cols), bf16),
            pltpu.VMEM((steps, n_s, 4, tokens), f32),
            pltpu.VMEM((2, tokens), f32),
            pltpu.VMEM((n_i, 1, cols), f32),
            pltpu.VMEM((n_i, 1, cols), f32),
            dma((3 + steps,)),
            dma((2, n_i - 1)),
            dma((2, n_i - 1)),
            dma((steps, n_s - 1)),
            dma((steps, n_s - 1)),
            dma((steps, n_s)),
            dma((steps, n_s)),
            dma((2, n_i)),
            dma((2, n_i)),
            dma((2, n_i - 1)),
            dma((2, n_i - 1)),
        ],
        compiler_params=pltpu.CompilerParams(
            collective_id=0, has_side_effects=True, vmem_limit_bytes=67043328
        ),
    )(low, gain_row, attended, stream, targets)
    weight_pseudo = weight_summed / n_i
    gain_pseudo = lax.dynamic_slice(gain_summed, (0, offset), (1, own))[0] / n_i
    weight_velocity = outer_momentum * weight_moment + weight_pseudo
    gain_velocity = outer_momentum * gain_moment + gain_pseudo
    weight_updated = weight_master - outer_rate * (weight_pseudo + outer_momentum * weight_velocity)
    gain_updated = gain_master - outer_rate * (gain_pseudo + outer_momentum * gain_velocity)
    return (weight_updated, gain_updated, weight_velocity, gain_velocity)


def outer_sum(grad_one, grad_two):
    first = (inner_rate * beta_one * (1.0 - beta_one) / (1.0 - beta_one**2)) * grad_one + (
        inner_rate * (1.0 - beta_one) / (1.0 - beta_one**2)
    ) * grad_two
    second = (beta_two * (1.0 - beta_two) / (1.0 - beta_two**2)) * (grad_one * grad_one) + (
        (1.0 - beta_two) / (1.0 - beta_two**2)
    ) * (grad_two * grad_two)
    root = jnp.sqrt(second) + adam_epsilon
    size = jnp.abs(grad_one) + adam_epsilon
    return ((inner_rate * keep) * grad_one * root + first * size) / (root * size)


def kernel(
    n_i, n_s, master_ref, gain_ref, moment_ref, gain_moment_ref, rows_ref, stream_ref, goals_ref,
    updated_ref, gain_updated_ref, velocity_ref, gain_velocity_ref,
    master, moment, rows, rows_h, anchor, ahead_a, ahead_b, later, grads, res, slope, slope_h, stream, goals,
    outgo, from_mate, from_twin, part_out, part_in, stats, line, gains, gain_out, gain_in,
    local_sem, z_send, z_recv, a_send, a_recv, p_send, p_recv, ha_send, ha_recv,
    s_send, s_recv, g_send, g_recv, r_send, r_recv, e_send, e_recv, m_send, m_recv,
):
    i = lax.axis_index("island")
    s = lax.axis_index("shard")
    steps, _, block, width = rows.shape
    _, chunks, piece, _ = anchor.shape
    cols = chunks * LANES
    own = gains.shape[2]
    tokens = n_s * block
    tiles = tokens // LANES
    scale = width ** (-0.5)
    depth = min(1024, piece)
    tall = min(256, piece)
    span = min(512, piece)
    f32, bf16 = jnp.float32, jnp.bfloat16

    is_left = i < n_i // 2
    is_end = (i == 0) | (i == n_i - 1)
    is_inner = (i > 0) & (i < n_i - 1)
    toward = jnp.where(is_left, 1, -1)
    mate = (jnp.where(is_end, i + toward, i - toward), s)
    twin = (n_i - 1 - i, s)

    def when_inner(f):
        pl.when(is_inner)(f)

    def when_end(f):
        pl.when(is_end)(f)

    def mirrored(o):
        return jnp.where(is_left, o, n_i - 1 - o)

    barrier = pltpu.get_barrier_semaphore()
    for d in range(1, n_i):
        pl.semaphore_signal(barrier, inc=1, device_id=(lax.rem(i + d, n_i), s), device_id_type=MESH)
    for d in range(1, n_s):
        pl.semaphore_signal(barrier, inc=1, device_id=(i, lax.rem(s + d, n_s)), device_id_type=MESH)

    load_master = pltpu.make_async_copy(master_ref, master, local_sem.at[0])
    load_rows = [
        pltpu.make_async_copy(rows_ref.at[0, st], rows.at[st, s], local_sem.at[1 + st]) for st in range(steps)
    ]
    load_rest = [
        pltpu.make_async_copy(stream_ref.at[0], stream, local_sem.at[1 + steps]),
        pltpu.make_async_copy(goals_ref.at[0], goals, local_sem.at[2 + steps]),
        pltpu.make_async_copy(moment_ref, moment, local_sem.at[3 + steps]),
    ]
    for copy in [load_master] + load_rows + load_rest:
        copy.start()

    def remote(src, dst, send, recv, to):
        return pltpu.make_async_remote_copy(
            src_ref=src, dst_ref=dst, send_sem=send, recv_sem=recv, device_id=to, device_id_type=MESH
        )

    def z_mate(o, c):
        return remote(anchor.at[o, c], anchor.at[o, c], z_send.at[0, o, c], z_recv.at[o, c], mate)

    def z_twin(o, c):
        return remote(anchor.at[o, c], anchor.at[o, c], z_send.at[1, o, c], z_recv.at[o, c], twin)

    n_bits = n_s.bit_length() - 1
    orders = [list(range(1, n_bits)) + [0], list(range(n_bits - 1, 0, -1)) + [0]]
    half = block // 2

    def a_blocks(h, phase):
        found = []
        for m in range(1 << phase):
            at = s
            for q in range(phase):
                if (m >> q) & 1:
                    at = flip(at, orders[h][q])
            found.append(at)
        return found

    def a_copy(which, h, phase, m, at):
        slot = (1 << phase) - 1 + m
        buffer = rows if which < steps else rows_h
        part = buffer.at[which % steps, at, pl.ds(h * half, half)]
        return remote(
            part, part, a_send.at[which, h, slot], a_recv.at[which, h, slot], (i, flip(s, orders[h][phase]))
        )

    def a_start(which, phase, among=None):
        for m in among or range(1 << phase):
            for h in range(2):
                a_copy(which, h, phase, m, a_blocks(h, phase)[m]).start()

    def a_wait(which, phase):
        for h in range(2):
            for m, at in enumerate(a_blocks(h, phase)):
                a_copy(which, h, phase, m, flip(at, orders[h][phase])).wait_recv()

    def a_sent(which):
        for phase in range(n_bits):
            for h in range(2):
                for m, at in enumerate(a_blocks(h, phase)):
                    a_copy(which, h, phase, m, at).wait_send()

    far = pl.multiple_of(jnp.where(is_left, width - 2 * piece, 0), LANES)

    def lend_rows(st):
        return remote(
            rows.at[st, s, :, pl.ds(far, 2 * piece)], rows_h.at[st, s], ha_send.at[st], ha_recv.at[st], mate
        )

    gains[i] = gain_ref[...].astype(bf16).astype(f32)
    gain_copies = [
        remote(gains.at[i], gains.at[i], g_send.at[0, d], g_recv.at[0, d], (lax.rem(i + d, n_i), s))
        for d in range(1, n_i)
    ]
    gain_waits = [
        remote(
            gains.at[lax.rem(i + n_i - d, n_i)], gains.at[lax.rem(i + n_i - d, n_i)],
            g_send.at[0, d], g_recv.at[0, d], (lax.rem(i + d, n_i), s),
        )
        for d in range(1, n_i)
    ]

    load_master.wait()

    def lower(j, _):
        at = pl.ds(pl.multiple_of(j * tall, tall), tall)
        for c in range(chunks):
            anchor[i, c, at, :] = master[at, c * LANES : (c + 1) * LANES].astype(bf16)
        return 0

    lax.fori_loop(0, piece // tall, lower, 0)
    for copy in load_rows:
        copy.wait()
    pl.semaphore_wait(barrier, n_i - 1 + n_s - 1)
    a_start(0, 0)

    @when_end
    def _():
        for c in range(chunks):
            z_mate(i, c).start()
            if c == 1:
                lend_rows(0).start()
        lend_rows(1).start()

    @when_inner
    def _():
        for c in range(chunks):
            z_mate(i, c).start()
            z_twin(i, c).start()

    for copy in gain_copies:
        copy.start()
    res[...] = jnp.zeros_like(res)
    for copy in load_rest:
        copy.wait()

    def joined(buffer, at, ds):
        return jnp.concatenate([buffer[at, c, ds, :] for c in range(chunks)], axis=1)

    def project(o, count=chunks):
        def body(k, _):
            start = pl.multiple_of(k * depth, depth)
            wide = pl.multiple_of(o * piece + k * depth, depth)
            part = rows[0, :, :, pl.ds(wide, depth)].reshape(tokens, depth)
            weights = [anchor[o, c, pl.ds(start, depth), :] for c in range(count)]
            res[:, : count * LANES] += jnp.dot(part, jnp.concatenate(weights, axis=1), preferred_element_type=f32)
            return 0

        lax.fori_loop(0, piece // depth, body, 0)

    def arrived(o, c):
        z_mate(o, c).wait_recv()

    held = chunks - 1
    near_far = jnp.where(is_left, n_i - 2, 0)
    groups = 2

    def part_copy():
        return remote(part_out, part_in, p_send, p_recv, mate)

    def project_for_end():
        weights = jnp.concatenate([anchor[near_far + k, held] for k in range(2)], axis=0)
        count = n_s // groups
        for g in range(groups):
            part = rows_h[0, g * count : (g + 1) * count].reshape(count * block, 2 * piece)
            part_out[g * count * block : (g + 1) * count * block, :] = jnp.dot(
                part, weights, preferred_element_type=f32
            ).astype(bf16)

    @when_end
    def _():
        one, two, three = mirrored(1), mirrored(2), mirrored(3)
        a_wait(0, 0)
        for p in range(1, n_bits):
            a_start(0, p)
            if p == 1:
                a_start(1, 0)
            a_wait(0, p)
        project(i)
        for c in range(chunks):
            arrived(one, c)
        project(one)
        a_wait(1, 0)
        a_start(1, 1)
        for c in range(held):
            arrived(two, c)
        project(two, held)
        for p in range(1, n_bits - 1):
            a_wait(1, p)
            a_start(1, p + 1)
        for c in range(held):
            arrived(three, c)
        project(three, held)
        part_copy().wait_recv()
        res[:, held * LANES :] += part_in[...].astype(f32)

    @when_inner
    def _():
        zero, two, three = mirrored(0), mirrored(2), mirrored(3)

        def from_end(c):
            arrived(zero, c)
            z_twin(zero, c).start()

        def from_far(o, c):
            arrived(o, c)
            if c < held:
                z_mate(o, c).start()

        from_end(0)
        from_far(two, 0)
        a_wait(0, 0)
        a_start(0, 1)
        from_end(1)
        from_far(two, 1)
        from_far(two, 2)
        from_far(two, 3)
        from_end(2)
        for p in range(1, n_bits - 1):
            a_wait(0, p)
            a_start(0, p + 1)
        lend_rows(0).wait_recv()
        a_start(2, 0)
        from_far(three, 0)
        a_wait(2, 0)
        a_start(2, 1)
        a_start(1, 0)
        from_end(3)
        a_wait(0, n_bits - 1)
        project(i)
        from_far(three, 1)
        project(zero)
        for p in range(1, n_bits - 1):
            a_wait(2, p)
            a_start(2, p + 1)
        from_far(three, 2)
        project(two)
        from_far(three, 3)
        a_wait(2, n_bits - 1)
        project_for_end()
        part_copy().start()
        z_mate(two, held).start()
        z_mate(three, held).start()
        project(three)

    for copy in gain_waits:
        copy.wait_recv()
    gain_anchor = jnp.concatenate([gains[j] for j in range(n_i)], axis=1)
    gain = gain_anchor

    def fold(value):
        total = value[:, :LANES]
        for c in range(1, chunks):
            total = total + value[:, c * LANES : (c + 1) * LANES]
        return jnp.sum(total.T, axis=0, keepdims=True)

    def spread(value):
        square = jnp.broadcast_to(value, (LANES, LANES)).T
        return jnp.concatenate([square] * chunks, axis=1)

    def row_stats(st, gain, between=None):
        def body(q, _):
            at = pl.ds(pl.multiple_of(q * LANES, LANES), LANES)
            r = stream[st, at, :].astype(f32) + res[at, :] * scale
            res[at, :] = r
            weighted = r * gain
            stats[st, 0, 0:1, at] = fold(r * r)
            stats[st, 0, 1:2, at] = fold(weighted * weighted)
            stats[st, 0, 2:3, at] = fold(weighted * goals[st, at, :].astype(f32))
            stats[st, 0, 3:4, at] = jnp.zeros((1, LANES), f32)
            return 0

        lax.fori_loop(0, tiles, body, 0)
        copies = [
            remote(
                stats.at[st, 0], stats.at[st, d], s_send.at[st, d], s_recv.at[st, d],
                (i, lax.rem(s + d, n_s)),
            )
            for d in range(1, n_s)
        ]
        for copy in copies:
            copy.start()
        if between is not None:
            between()
        for copy in copies:
            copy.wait()
        total = stats[st, 0]
        for d in range(1, n_s):
            total = total + stats[st, d]
        inverse = lax.rsqrt(total[0:1] * (1.0 / width) + norm_epsilon)
        pull = inverse * total[1:2] - total[2:3]
        line[0:1, :] = inverse
        line[1:2, :] = inverse * inverse * inverse * pull * (1.0 / width)

    def row_grads(st, gain):
        def body(q, total):
            at = pl.ds(pl.multiple_of(q * LANES, LANES), LANES)
            inverse, pull = spread(line[0:1, at]), spread(line[1:2, at])
            r = res[at, :]
            unit = r * inverse
            loss = unit * gain - goals[st, at, :].astype(f32)
            loss = loss.astype(bf16).astype(f32)
            low = (inverse * (loss * gain) - r * pull).astype(bf16)
            for c in range(chunks):
                slope[st, c, at, :] = low[:, c * LANES : (c + 1) * LANES]
            return total + jnp.sum(loss * unit, axis=0, keepdims=True)

        return lax.fori_loop(0, tiles, body, jnp.zeros((1, cols), f32))

    def product(part, against):
        return lax.dot_general(part, against, (((0,), (0,)), ((), ())), preferred_element_type=f32) * scale

    def weight_grad(st, wide, size):
        part = rows[st, :, :, pl.ds(pl.multiple_of(wide, size), size)].reshape(tokens, size)
        return product(part, joined(slope, st, slice(None)))

    @when_inner
    def _():
        a_wait(1, 0)

    def more_rows():
        @when_inner
        def _():
            a_start(1, 1)
            lend_rows(1).wait_recv()
            a_start(3, 0)

    row_stats(0, gain, more_rows)
    gain_first = row_grads(0, gain)
    res[...] = jnp.zeros_like(res)

    def lend_slope():
        return remote(slope.at[0], slope_h.at[0], r_send.at[0], r_recv.at[0], mate)

    def lend_later(c):
        return remote(slope.at[1, c], slope_h.at[1, c], r_send.at[1 + c], r_recv.at[1 + c], mate)

    when_end(lambda: lend_slope().start())

    spans = width // span
    per_piece = piece // span

    def place(q):
        return mirrored(q // per_piece), q % per_piece

    def step_one(q, ahead):
        o, j = place(q)
        at = pl.ds(pl.multiple_of(j * span, span), span)
        grad = weight_grad(0, o * piece + j * span, span)
        grads[o, at, :] = grad
        param = keep * joined(anchor, o, at).astype(f32) - inner_rate * first_update(grad)
        ahead[...] = param.astype(bf16)

    def project_later(q, ahead):
        o, j = place(q)
        wide = pl.multiple_of(o * piece + j * span, span)
        part = rows[1, :, :, pl.ds(wide, span)].reshape(tokens, span)
        res[...] += jnp.dot(part, ahead[...], preferred_element_type=f32)

    def both(t, _):
        for k in (2, 3):

            @pl.when(2 * t == k * per_piece)
            def _():
                arrived(mirrored(k), held)

        project_later(jnp.maximum(2 * t - 1, 0), ahead_b)
        step_one(2 * t, ahead_a)
        project_later(2 * t, ahead_a)
        step_one(2 * t + 1, ahead_b)
        return 0

    def one_alone(q, _):
        step_one(q, later.at[q])
        return 0

    def later_alone(q, _):
        project_later(q, later.at[q])
        return 0

    @when_end
    def _():
        a_wait(1, n_bits - 1)
        ahead_b[...] = jnp.zeros_like(ahead_b)
        lax.fori_loop(0, spans // 2, both, 0)
        project_later(spans - 1, ahead_b)

    @when_inner
    def _():
        lax.fori_loop(0, spans, one_alone, 0)
        for p in range(1, n_bits - 1):
            a_wait(1, p)
            a_start(1, p + 1)
        a_wait(3, 0)
        a_start(3, 1, (0,))
        a_wait(1, n_bits - 1)
        lax.fori_loop(0, spans, later_alone, 0)

    gain_step = first_update(gain_first)
    gain = gain_anchor - inner_rate * gain_step

    def more_end_rows():
        @when_inner
        def _():
            a_start(3, 1, (1,))

    row_stats(1, gain, more_end_rows)
    gain_second = row_grads(1, gain)
    gain_move = inner_rate * (gain_step + second_update(gain_first, gain_second))
    for j in range(n_i):
        gain_out[j] = gain_move[:, j * own : (j + 1) * own]

    @when_end
    def _():
        for c in range(chunks):
            lend_later(c).start()

    gain_moves = [
        remote(
            gain_out.at[lax.rem(i + d, n_i)], gain_in.at[d], g_send.at[1, d], g_recv.at[1, d],
            (lax.rem(i + d, n_i), s),
        )
        for d in range(1, n_i)
    ]
    for copy in gain_moves:
        copy.start()

    def move(o):
        def body(j, _):
            at = pl.ds(pl.multiple_of(j * tall, tall), tall)
            grad = weight_grad(1, o * piece + j * tall, tall)
            grads[o, at, :] = outer_sum(grads[o, at, :], grad)
            return 0

        lax.fori_loop(0, piece // tall, body, 0)

    def give(slot, c):
        return remote(outgo.at[slot, c], from_mate.at[c], e_send.at[c], e_recv.at[c], mate)

    def cross(slot, c):
        return remote(outgo.at[slot, c], from_twin.at[slot, c], m_send.at[slot, c], m_recv.at[slot, c], twin)

    def pack(slot, c, o, *others):
        lanes = slice(c * LANES, (c + 1) * LANES)

        def body(j, _):
            at = pl.ds(pl.multiple_of(j * tall, tall), tall)
            total = grads[o, at, lanes]
            for other in others:
                total = total + other[at, :].astype(f32)
            outgo[slot, c, at, :] = total.astype(bf16)
            return 0

        lax.fori_loop(0, piece // tall, body, 0)

    def finish(c, o, *others):
        lanes = slice(c * LANES, (c + 1) * LANES)

        def body(j, _):
            at = pl.ds(pl.multiple_of(j * tall, tall), tall)
            total = grads[o, at, lanes]
            for other in others:
                total = total + other[at, :].astype(f32)
            outer = master[at, lanes]
            pseudo = total * (1.0 / n_i) + (1.0 - keep * keep) * outer.astype(bf16).astype(f32)
            velocity = outer_momentum * moment[at, lanes] + pseudo
            velocity_ref[at, lanes] = velocity
            updated_ref[at, lanes] = outer - outer_rate * (pseudo + outer_momentum * velocity)
            return 0

        lax.fori_loop(0, piece // tall, body, 0)
    @when_end
    def _():
        o = mirrored(1)
        move(o)
        for c in range(chunks):
            pack(0, c, o)
        for c in range(chunks):
            give(0, c).start()
        o = mirrored(0)
        move(o)
        for c in range(chunks):
            give(0, c).wait_recv()
            finish(c, o, from_mate.at[c])

    def help_end(slot, c, o):
        base = (o - near_far) * piece
        lanes = slice(c * LANES, (c + 1) * LANES)

        def body(j, _):
            at = pl.ds(pl.multiple_of(j * tall, tall), tall)
            wide = pl.ds(pl.multiple_of(base + j * tall, tall), tall)
            pair = [
                product(rows_h[st, :, :, wide].reshape(tokens, tall), slope_h[st, c]) for st in range(steps)
            ]
            outgo[slot, c, at, :] = (grads[o, at, lanes] + outer_sum(*pair)).astype(bf16)
            return 0

        lax.fori_loop(0, piece // tall, body, 0)

    @when_inner
    def _():
        def help_and_cross(slot, c):
            help_end(slot, c, mirrored(3 - slot))
            cross(slot, c).start()

        def forward(c):
            cross(0, c).wait_recv()
            pack(2, c, mirrored(0), from_twin.at[0, c])
            give(2, c).start()

        for p in range(1, n_bits - 1):
            a_wait(3, p)
            a_start(3, p + 1)
        move(mirrored(3))
        a_wait(3, n_bits - 1)
        lend_slope().wait_recv()
        for c in range(chunks):
            lend_later(c).wait_recv()
            help_and_cross(0, c)
            if c == 0:
                move(mirrored(0))
            if c == 1:
                move(mirrored(2))
        for c in range(chunks):
            help_and_cross(1, c)
            if c == 0:
                move(mirrored(1))
            forward(c)
        for c in range(chunks):
            give(2, c).wait_recv()
            cross(1, c).wait_recv()
            finish(c, mirrored(1), from_mate.at[c], from_twin.at[1, c])

    for copy in gain_moves:
        copy.wait()
    gain_total = gain_out[i]
    for d in range(1, n_i):
        gain_total = gain_total + gain_in[d]
    gain_pseudo = gain_total * (1.0 / n_i)
    gain_velocity = outer_momentum * gain_moment_ref[...] + gain_pseudo
    gain_velocity_ref[...] = gain_velocity
    gain_updated_ref[...] = gain_ref[...] - outer_rate * (gain_pseudo + outer_momentum * gain_velocity)

    @when_end
    def _():
        for st in range(steps):
            lend_rows(st).wait_send()
        lend_slope().wait_send()
        for c in range(chunks):
            z_mate(i, c).wait_send()
        for c in range(chunks):
            lend_later(c).wait_send()
            give(0, c).wait_send()

    @when_inner
    def _():
        for c in range(chunks):
            cross(0, c).wait_send()
            cross(1, c).wait_send()
            give(2, c).wait_send()
        part_copy().wait_send()
        a_sent(2)
        a_sent(3)
        for c in range(chunks):
            z_mate(i, c).wait_send()
            z_twin(i, c).wait_send()
            z_twin(mirrored(0), c).wait_send()
            z_mate(mirrored(2), c).wait_send()
            z_mate(mirrored(3), c).wait_send()

    for copy in gain_copies:
        copy.wait_send()
    a_sent(0)
    a_sent(1)


def write_out(*refs):
    count = len(refs) // 2
    sem = refs[-1]
    copies = [pltpu.make_async_copy(refs[k], refs[count + k], sem.at[k]) for k in range(count)]
    for copy in copies:
        copy.start()
    for copy in copies:
        copy.wait()


def per_device(weight_master, gain_master, weight_moment, gain_moment, attended, stream, targets):
    n_i, n_s = lax.axis_size("island"), lax.axis_size("shard")
    _, steps, block, width = attended.shape
    _, _, tokens, cols = stream.shape
    piece = weight_master.shape[0]
    own = gain_master.shape[0]
    f32, bf16 = jnp.float32, jnp.bfloat16
    chunks = cols // LANES
    arrays = [
        ((piece, cols), f32),
        ((piece, cols), f32),
        ((steps, n_s, block, width), bf16),
        ((steps, n_s, block, 2 * piece), bf16),
        ((n_i, chunks, piece, LANES), bf16),
        ((min(512, piece), cols), bf16),
        ((min(512, piece), cols), bf16),
        ((width // min(512, piece), min(512, piece), cols), bf16),
        ((n_i, piece, cols), f32),
        ((tokens, cols), f32),
        ((steps, chunks, tokens, LANES), bf16),
        ((steps, chunks, tokens, LANES), bf16),
        ((steps, tokens, cols), bf16),
        ((steps, tokens, cols), bf16),
        ((3, chunks, piece, LANES), bf16),
        ((chunks, piece, LANES), bf16),
        ((2, chunks, piece, LANES), bf16),
        ((tokens, LANES), bf16),
        ((tokens, LANES), bf16),
        ((steps, n_s, 4, tokens), f32),
        ((2, tokens), f32),
        ((n_i, 1, own), f32),
        ((n_i, 1, own), f32),
        ((n_i, 1, own), f32),
    ]
    held = sum(math.prod(shape) * jnp.dtype(kind).itemsize for shape, kind in arrays)
    if n_i != 4 or steps != 2 or own % LANES or chunks < 2 or block % 32 or n_s < 4 or held > 60e6:
        return general_device(weight_master, gain_master, weight_moment, gain_moment, attended, stream, targets)
    any_space = pl.BlockSpec(memory_space=pl.ANY)
    vmem = pl.BlockSpec(memory_space=pltpu.VMEM)
    dma = pltpu.SemaphoreType.DMA
    outs = ((piece, cols), (1, own), (piece, cols), (1, own))
    results = pl.pallas_call(
        functools.partial(kernel, n_i, n_s),
        out_shape=tuple(pltpu.VMEM(shape, f32) for shape in outs),
        in_specs=[any_space, vmem, any_space, vmem, any_space, any_space, any_space],
        out_specs=(vmem, vmem, vmem, vmem),
        scratch_shapes=[pltpu.VMEM(shape, kind) for shape, kind in arrays]
        + [
            dma((4 + steps,)),
            dma((2, n_i, chunks)),
            dma((n_i, chunks)),
            dma((2 * steps, 2, n_s - 1)),
            dma((2 * steps, 2, n_s - 1)),
            dma(()),
            dma(()),
            dma((steps,)),
            dma((steps,)),
            dma((steps, n_s)),
            dma((steps, n_s)),
            dma((2, n_i)),
            dma((2, n_i)),
            dma((1 + chunks,)),
            dma((1 + chunks,)),
            dma((chunks,)),
            dma((chunks,)),
            dma((2, chunks)),
            dma((2, chunks)),
        ],
        compiler_params=pltpu.CompilerParams(
            collective_id=0, has_side_effects=True, vmem_limit_bytes=58 << 20
        ),
    )(weight_master, gain_master[None], weight_moment, gain_moment[None], attended, stream, targets)
    results = [pltpu.with_memory_space_constraint(x, pltpu.VMEM) for x in results]
    updated, gain_updated, velocity, gain_velocity = pl.pallas_call(
        write_out,
        out_shape=tuple(jax.ShapeDtypeStruct(shape, f32) for shape in outs),
        in_specs=[vmem] * 4,
        out_specs=(any_space,) * 4,
        scratch_shapes=[dma((4,))],
        compiler_params=pltpu.CompilerParams(vmem_limit_bytes=1 << 20),
    )(*results)
    return (updated, gain_updated[0], velocity, gain_velocity[0])


def solution(mesh):
    placed = (
        P("island", "shard"),
        P(("shard", "island")),
        P("island", "shard"),
        P(("shard", "island")),
        P("island", None, "shard", None),
        P("island", None, None, "shard"),
        P("island", None, None, "shard"),
    )
    return jax.shard_map(
        per_device,
        mesh=mesh,
        in_specs=placed,
        out_specs=(
            P("island", "shard"),
            P(("shard", "island")),
            P("island", "shard"),
            P(("shard", "island")),
        ),
        check_vma=False,
    )
```

```python
import functools
import math

import jax
import jax.numpy as jnp
from jax import lax
from jax.experimental import pallas as pl
from jax.experimental.pallas import tpu as pltpu
from jax.sharding import PartitionSpec as P

norm_epsilon = 1e-05
inner_rate = 0.05
beta_one = 0.9
beta_two = 0.95
adam_epsilon = 0.3
decay_rate = 0.1
outer_rate = 0.7
outer_momentum = 0.9

MESH = pl.DeviceIdType.MESH
LANES = 128
keep = 1.0 - inner_rate * decay_rate


def flip(index, bit):
    size = 1 << bit
    return index + size * (1 - 2 * (lax.div(index, size) % 2))


def first_update(grad):
    return grad / (jnp.abs(grad) + adam_epsilon)


def second_update(earlier, grad):
    first = (beta_one * (1.0 - beta_one)) * earlier + (1.0 - beta_one) * grad
    second = (beta_two * (1.0 - beta_two)) * earlier * earlier + (1.0 - beta_two) * grad * grad
    first_hat = first * (1.0 / (1.0 - beta_one**2))
    second_hat = second * (1.0 / (1.0 - beta_two**2))
    return first_hat / (jnp.sqrt(second_hat) + adam_epsilon)


def general_kernel(
    n_i, n_s, low_ref, gain_ref, rows_ref, stream_ref, goals_ref, total_ref, gain_total_ref,
    rows, anchor, later, grads, res, slope_low, stream, goals, from_left, from_right,
    stats, line, gains, gain_moves,
    local_sem, z_send, z_recv, a_send, a_recv, s_send, s_recv, g_send, g_recv, r_send, r_recv,
):
    i = lax.axis_index("island")
    s = lax.axis_index("shard")
    steps, _, block, width = rows.shape
    piece, cols = low_ref.shape
    tokens = n_s * block
    tiles = tokens // LANES
    scale = width ** (-0.5)
    depth = min(512, piece)
    tall = min(256, piece)

    barrier = pltpu.get_barrier_semaphore()
    for d in range(1, n_i):
        pl.semaphore_signal(barrier, inc=1, device_id=(lax.rem(i + d, n_i), s), device_id_type=MESH)
    for d in range(1, n_s):
        pl.semaphore_signal(barrier, inc=1, device_id=(i, lax.rem(s + d, n_s)), device_id_type=MESH)

    locals_ = [pltpu.make_async_copy(low_ref, anchor.at[i], local_sem.at[0])]
    for st in range(steps):
        locals_.append(pltpu.make_async_copy(rows_ref.at[0, st], rows.at[st, s], local_sem.at[1 + st]))
    locals_.append(pltpu.make_async_copy(stream_ref.at[0], stream, local_sem.at[1 + steps]))
    locals_.append(pltpu.make_async_copy(goals_ref.at[0], goals, local_sem.at[2 + steps]))
    for copy in locals_:
        copy.start()
    pl.semaphore_wait(barrier, n_i - 1 + n_s - 1)

    def remote(src, dst, send, recv, to):
        return pltpu.make_async_remote_copy(
            src_ref=src, dst_ref=dst, send_sem=send, recv_sem=recv, device_id=to, device_id_type=MESH
        )

    right, left = (lax.rem(i + 1, n_i), s), (lax.rem(i + n_i - 1, n_i), s)

    def z_copy(way, t, at):
        return remote(
            anchor.at[at], anchor.at[at], z_send.at[way, t], z_recv.at[way, t], right if way == 0 else left
        )

    def z_start(t):
        @pl.when((i < n_i - 1) & (i - t >= 0))
        def _():
            z_copy(0, t, i - t).start()

        @pl.when((i > 0) & (i + t <= n_i - 1))
        def _():
            z_copy(1, t, i + t).start()

    def z_wait(t):
        @pl.when(i - 1 - t >= 0)
        def _():
            z_copy(0, t, i - 1 - t).wait_recv()

        @pl.when(i + 1 + t <= n_i - 1)
        def _():
            z_copy(1, t, i + 1 + t).wait_recv()

    n_bits = n_s.bit_length() - 1
    orders = [list(range(1, n_bits)) + [0], list(range(n_bits - 1, 0, -1)) + [0]]

    def a_blocks(st, phase):
        order = orders[st % 2]
        found = []
        for m in range(1 << phase):
            at = s
            for q in range(phase):
                if (m >> q) & 1:
                    at = flip(at, order[q])
            found.append(at)
        return found

    def a_copy(st, phase, m, at):
        slot = (1 << phase) - 1 + m
        return remote(
            rows.at[st, at], rows.at[st, at], a_send.at[st, slot], a_recv.at[st, slot],
            (i, flip(s, orders[st % 2][phase])),
        )

    def a_start(phase):
        for st in range(steps):
            for m, at in enumerate(a_blocks(st, phase)):
                a_copy(st, phase, m, at).start()

    def a_wait(phase):
        for st in range(steps):
            for m, at in enumerate(a_blocks(st, phase)):
                a_copy(st, phase, m, flip(at, orders[st % 2][phase])).wait_recv()

    def to_islands(buffer, which):
        return [
            remote(
                buffer.at[0], buffer.at[d], g_send.at[which, d], g_recv.at[which, d],
                (lax.rem(i + d, n_i), s),
            )
            for d in range(1, n_i)
        ]

    locals_[0].wait()
    z_start(0)
    for copy in locals_[1 : 1 + steps]:
        copy.wait()
    a_start(0)
    gains[0] = gain_ref[...]
    gain_in = to_islands(gains, 0)
    for copy in gain_in:
        copy.start()
    res[...] = jnp.zeros_like(res)
    for copy in locals_[1 + steps :]:
        copy.wait()

    def project(st, weights, at):
        def body(k, _):
            start = pl.multiple_of(k * depth, depth)
            wide = pl.multiple_of(at * piece + k * depth, depth)
            part = rows[st, :, :, pl.ds(wide, depth)].reshape(tokens, depth)
            res[...] += jnp.dot(part, weights[at, pl.ds(start, depth), :], preferred_element_type=jnp.float32)
            return 0

        lax.fori_loop(0, piece // depth, body, 0)

    def project_arrived(t):
        @pl.when(i - 1 - t >= 0)
        def _():
            project(0, anchor, i - 1 - t)

        @pl.when(i + 1 + t <= n_i - 1)
        def _():
            project(0, anchor, i + 1 + t)

    events = [(2.0 * t + 2.6, "z", t) for t in range(n_i - 1)]
    events += [(2.0 * ((2 << p) - 1), "a", p) for p in range(n_bits - 1)]
    last = events[-1][0] if n_bits > 1 else 0.0
    events.append((last + 0.1, "a", n_bits - 1))
    gathered, ready = False, []
    for _, kind, at in sorted(events):
        if kind == "a":
            a_wait(at)
            if at + 1 < n_bits:
                a_start(at + 1)
            else:
                gathered = True
                project(0, anchor, i)
                for t in ready:
                    project_arrived(t)
        else:
            z_wait(at)
            if at + 1 < n_i - 1:
                z_start(at + 1)
            if gathered:
                project_arrived(at)
            else:
                ready.append(at)

    for copy in gain_in:
        copy.wait()
    gain_anchor = gains[0]
    for d in range(1, n_i):
        gain_anchor = gain_anchor + gains[d]
    gain = gain_anchor

    def fold(value):
        total = value[:, :LANES]
        for c in range(1, cols // LANES):
            total = total + value[:, c * LANES : (c + 1) * LANES]
        return jnp.sum(total.T, axis=0, keepdims=True)

    def spread(value):
        square = jnp.broadcast_to(value, (LANES, LANES)).T
        return jnp.concatenate([square] * (cols // LANES), axis=1)

    def row_stats(st, gain):
        def body(q, _):
            at = pl.ds(pl.multiple_of(q * LANES, LANES), LANES)
            r = stream[st, at, :].astype(jnp.float32) + res[at, :] * scale
            res[at, :] = r
            weighted = r * gain
            stats[st, 0, 0:1, at] = fold(r * r)
            stats[st, 0, 1:2, at] = fold(weighted * weighted)
            stats[st, 0, 2:3, at] = fold(weighted * goals[st, at, :].astype(jnp.float32))
            stats[st, 0, 3:4, at] = jnp.zeros((1, LANES), jnp.float32)
            return 0

        lax.fori_loop(0, tiles, body, 0)
        copies = [
            remote(
                stats.at[st, 0], stats.at[st, d], s_send.at[st, d], s_recv.at[st, d],
                (i, lax.rem(s + d, n_s)),
            )
            for d in range(1, n_s)
        ]
        for copy in copies:
            copy.start()
        for copy in copies:
            copy.wait()
        total = stats[st, 0]
        for d in range(1, n_s):
            total = total + stats[st, d]
        inverse = lax.rsqrt(total[0:1] * (1.0 / width) + norm_epsilon)
        slope = inverse * total[1:2] - total[2:3]
        line[0:1, :] = inverse
        line[1:2, :] = inverse * inverse * inverse * slope * (1.0 / width)

    def row_grads(st, gain):
        def body(q, total):
            at = pl.ds(pl.multiple_of(q * LANES, LANES), LANES)
            inverse, pull = spread(line[0:1, at]), spread(line[1:2, at])
            r = res[at, :]
            unit = r * inverse
            loss = unit * gain - goals[st, at, :].astype(jnp.float32)
            loss = loss.astype(jnp.bfloat16).astype(jnp.float32)
            slope_low[at, :] = (inverse * (loss * gain) - r * pull).astype(jnp.bfloat16)
            return total + jnp.sum(loss * unit, axis=0, keepdims=True)

        return lax.fori_loop(0, tiles, body, jnp.zeros((1, cols), jnp.float32))

    def weight_grad(st, wide):
        part = rows[st, :, :, pl.ds(pl.multiple_of(wide, tall), tall)].reshape(tokens, tall)
        return (
            lax.dot_general(
                part, slope_low[...], (((0,), (0,)), ((), ())), preferred_element_type=jnp.float32
            )
            * scale
        )

    row_stats(0, gain)
    gain_first = row_grads(0, gain)
    per_piece = piece // tall

    def step_one(q, _):
        o, j = q // per_piece, q % per_piece
        at = pl.ds(pl.multiple_of(j * tall, tall), tall)
        grad = weight_grad(0, q * tall)
        grads[o, at, :] = grad
        param = keep * anchor[o, at, :].astype(jnp.float32) - inner_rate * first_update(grad)
        later[o, at, :] = param.astype(jnp.bfloat16)
        return 0

    lax.fori_loop(0, n_i * per_piece, step_one, 0)
    gain_step = first_update(gain_first)
    gain = gain_anchor - inner_rate * gain_step

    res[...] = jnp.zeros_like(res)

    def project_later(at, _):
        project(1, later, at)
        return 0

    lax.fori_loop(0, n_i, project_later, 0)
    row_stats(1, gain)
    gain_second = row_grads(1, gain)
    gain_moves[0] = inner_rate * (gain_step + second_update(gain_first, gain_second))
    gain_out = to_islands(gain_moves, 1)
    for copy in gain_out:
        copy.start()

    def to_right(k):
        at = n_i - 1 - k
        return remote(later.at[at], from_left.at[k], r_send.at[0, k], r_recv.at[0, k], right)

    def to_left(k):
        return remote(later.at[k], from_right.at[k], r_send.at[1, k], r_recv.at[1, k], left)

    early = 1 - lax.div(2 * i, n_i)

    def owner_piece(q, _):
        o = q + early * (n_i - 1 - 2 * q)

        def step_two(j, _):
            at = pl.ds(pl.multiple_of(j * tall, tall), tall)
            grad = weight_grad(1, o * piece + j * tall)
            earlier = grads[o, at, :]
            moved = (1.0 - keep * keep) * anchor[o, at, :].astype(jnp.float32) + inner_rate * (
                keep * first_update(earlier) + second_update(earlier, grad)
            )
            grads[o, at, :] = moved
            later[o, at, :] = moved.astype(jnp.bfloat16)
            return 0

        lax.fori_loop(0, per_piece, step_two, 0)

        @pl.when((i == 0) & (o > 0))
        def _():
            to_right(n_i - 1 - o).start()

        @pl.when((i == n_i - 1) & (o < n_i - 1))
        def _():
            to_left(o).start()

        return 0

    lax.fori_loop(0, n_i, owner_piece, 0)

    def add(o, arrived, k):
        def body(j, _):
            at = pl.ds(pl.multiple_of(j * tall, tall), tall)
            later[o, at, :] = (grads[o, at, :] + arrived[k, at, :].astype(jnp.float32)).astype(jnp.bfloat16)
            return 0

        lax.fori_loop(0, per_piece, body, 0)

    for t in range(n_i - 1):
        k_right = t - i
        k_left = t - (n_i - 1 - i)

        @pl.when((i > 0) & (k_right >= 0) & (k_right < n_i - 1 - i))
        def _():
            to_right(k_right).wait_recv()
            add(n_i - 1 - k_right, from_left, k_right)
            to_right(k_right).start()

        @pl.when((i < n_i - 1) & (k_left >= 0) & (k_left < i))
        def _():
            to_left(k_left).wait_recv()
            add(k_left, from_right, k_left)
            to_left(k_left).start()

    for copy in gain_out:
        copy.wait()
    gain_total = gain_moves[0]
    for d in range(1, n_i):
        gain_total = gain_total + gain_moves[d]
    gain_total_ref[...] = gain_total

    total_ref[...] = grads[i]

    @pl.when(i > 0)
    def _():
        k = n_i - 1 - i
        to_right(k).wait_recv()
        total_ref[...] += from_left[k].astype(jnp.float32)

    @pl.when(i < n_i - 1)
    def _():
        to_left(i).wait_recv()
        total_ref[...] += from_right[i].astype(jnp.float32)

    for k in range(n_i - 1):

        @pl.when(k < n_i - 1 - i)
        def _(k=k):
            to_right(k).wait_send()

        @pl.when(k < i)
        def _(k=k):
            to_left(k).wait_send()

        @pl.when((i < n_i - 1) & (i - k >= 0))
        def _(k=k):
            z_copy(0, k, i - k).wait_send()

        @pl.when((i > 0) & (i + k <= n_i - 1))
        def _(k=k):
            z_copy(1, k, i + k).wait_send()

    for phase in range(n_bits):
        for st in range(steps):
            for m, at in enumerate(a_blocks(st, phase)):
                a_copy(st, phase, m, at).wait_send()


def general_device(weight_master, gain_master, weight_moment, gain_moment, attended, stream, targets):
    n_i, n_s = lax.axis_size("island"), lax.axis_size("shard")
    _, steps, block, width = attended.shape
    _, _, tokens, cols = stream.shape
    piece = weight_master.shape[0]
    own = gain_master.shape[0]
    offset = lax.axis_index("island") * own
    low = weight_master.astype(jnp.bfloat16)
    gain_low = gain_master.astype(jnp.bfloat16).astype(jnp.float32)
    gain_row = lax.dynamic_update_slice(jnp.zeros((1, cols), jnp.float32), gain_low[None], (0, offset))
    any_space = pl.BlockSpec(memory_space=pl.ANY)
    vmem = pl.BlockSpec(memory_space=pltpu.VMEM)
    f32, bf16 = jnp.float32, jnp.bfloat16
    dma = pltpu.SemaphoreType.DMA
    weight_summed, gain_summed = pl.pallas_call(
        functools.partial(general_kernel, n_i, n_s),
        out_shape=(
            jax.ShapeDtypeStruct((piece, cols), f32),
            jax.ShapeDtypeStruct((1, cols), f32),
        ),
        in_specs=[any_space, vmem, any_space, any_space, any_space],
        out_specs=(vmem, vmem),
        scratch_shapes=[
            pltpu.VMEM((steps, n_s, block, width), bf16),
            pltpu.VMEM((n_i, piece, cols), bf16),
            pltpu.VMEM((n_i, piece, cols), bf16),
            pltpu.VMEM((n_i, piece, cols), f32),
            pltpu.VMEM((tokens, cols), f32),
            pltpu.VMEM((tokens, cols), bf16),
            pltpu.VMEM((steps, tokens, cols), bf16),
            pltpu.VMEM((steps, tokens, cols), bf16),
            pltpu.VMEM((n_i - 1, piece, cols), bf16),
            pltpu.VMEM((n_i - 1, piece, cols), bf16),
            pltpu.VMEM((steps, n_s, 4, tokens), f32),
            pltpu.VMEM((2, tokens), f32),
            pltpu.VMEM((n_i, 1, cols), f32),
            pltpu.VMEM((n_i, 1, cols), f32),
            dma((3 + steps,)),
            dma((2, n_i - 1)),
            dma((2, n_i - 1)),
            dma((steps, n_s - 1)),
            dma((steps, n_s - 1)),
            dma((steps, n_s)),
            dma((steps, n_s)),
            dma((2, n_i)),
            dma((2, n_i)),
            dma((2, n_i - 1)),
            dma((2, n_i - 1)),
        ],
        compiler_params=pltpu.CompilerParams(
            collective_id=0, has_side_effects=True, vmem_limit_bytes=67043328
        ),
    )(low, gain_row, attended, stream, targets)
    weight_pseudo = weight_summed / n_i
    gain_pseudo = lax.dynamic_slice(gain_summed, (0, offset), (1, own))[0] / n_i
    weight_velocity = outer_momentum * weight_moment + weight_pseudo
    gain_velocity = outer_momentum * gain_moment + gain_pseudo
    weight_updated = weight_master - outer_rate * (weight_pseudo + outer_momentum * weight_velocity)
    gain_updated = gain_master - outer_rate * (gain_pseudo + outer_momentum * gain_velocity)
    return (weight_updated, gain_updated, weight_velocity, gain_velocity)


def outer_sum(grad_one, grad_two):
    first = (inner_rate * beta_one * (1.0 - beta_one) / (1.0 - beta_one**2)) * grad_one + (
        inner_rate * (1.0 - beta_one) / (1.0 - beta_one**2)
    ) * grad_two
    second = (beta_two * (1.0 - beta_two) / (1.0 - beta_two**2)) * (grad_one * grad_one) + (
        (1.0 - beta_two) / (1.0 - beta_two**2)
    ) * (grad_two * grad_two)
    root = second * lax.rsqrt(jnp.maximum(second, 1e-30)) + adam_epsilon
    size = jnp.abs(grad_one) + adam_epsilon
    return ((inner_rate * keep) * grad_one * root + first * size) * pl.reciprocal(root * size)


def kernel(
    n_i, n_s, master_ref, gain_ref, moment_ref, gain_moment_ref, rows_ref, stream_ref, goals_ref,
    updated_ref, gain_updated_ref, velocity_ref, gain_velocity_ref,
    master, moment, rows, rows_h, anchor, ahead_a, ahead_b, later, grads, res, slope, slope_h, stream, goals,
    outgo, from_mate, from_twin, part_out, part_in, stats, line, gains, gain_out, gain_in,
    local_sem, z_send, z_recv, a_send, a_recv, p_send, p_recv, ha_send, ha_recv,
    s_send, s_recv, g_send, g_recv, r_send, r_recv, e_send, e_recv, m_send, m_recv,
):
    i = lax.axis_index("island")
    s = lax.axis_index("shard")
    steps, _, block, width = rows.shape
    _, chunks, piece, _ = anchor.shape
    cols = chunks * LANES
    own = gains.shape[2]
    tokens = n_s * block
    tiles = tokens // LANES
    scale = width ** (-0.5)
    depth = min(1024, piece)
    tall = min(256, piece)
    span = min(512, piece)
    f32, bf16 = jnp.float32, jnp.bfloat16

    is_left = i < n_i // 2
    is_end = (i == 0) | (i == n_i - 1)
    is_inner = (i > 0) & (i < n_i - 1)
    toward = jnp.where(is_left, 1, -1)
    mate = (jnp.where(is_end, i + toward, i - toward), s)
    twin = (n_i - 1 - i, s)

    def when_inner(f):
        pl.when(is_inner)(f)

    def when_end(f):
        pl.when(is_end)(f)

    def mirrored(o):
        return jnp.where(is_left, o, n_i - 1 - o)

    near_far = jnp.where(is_left, n_i - 2, 0)
    barrier = pltpu.get_barrier_semaphore()
    for d in range(1, n_i):
        pl.semaphore_signal(barrier, inc=1, device_id=(lax.rem(i + d, n_i), s), device_id_type=MESH)
    for d in range(1, n_s):
        pl.semaphore_signal(barrier, inc=1, device_id=(i, lax.rem(s + d, n_s)), device_id_type=MESH)

    load_master = pltpu.make_async_copy(master_ref, master, local_sem.at[0])
    load_rows = [
        pltpu.make_async_copy(rows_ref.at[0, st], rows.at[st, s], local_sem.at[1 + st]) for st in range(steps)
    ]
    load_rest = [
        pltpu.make_async_copy(stream_ref.at[0], stream, local_sem.at[1 + steps]),
        pltpu.make_async_copy(goals_ref.at[0], goals, local_sem.at[2 + steps]),
        pltpu.make_async_copy(moment_ref, moment, local_sem.at[3 + steps]),
    ]
    for copy in [load_master] + load_rows + load_rest:
        copy.start()

    def remote(src, dst, send, recv, to):
        return pltpu.make_async_remote_copy(
            src_ref=src, dst_ref=dst, send_sem=send, recv_sem=recv, device_id=to, device_id_type=MESH
        )

    def z_mate(o, c):
        return remote(anchor.at[o, c], anchor.at[o, c], z_send.at[0], z_recv.at[o, c], mate)

    def z_twin(o, c):
        return remote(anchor.at[o, c], anchor.at[o, c], z_send.at[1], z_recv.at[o, c], twin)

    n_bits = n_s.bit_length() - 1
    orders = [list(range(1, n_bits)) + [0], list(range(n_bits - 1, 0, -1)) + [0]]
    half = block // 2

    def a_blocks(h, phase):
        found = []
        for m in range(1 << phase):
            at = s
            for q in range(phase):
                if (m >> q) & 1:
                    at = flip(at, orders[h][q])
            found.append(at)
        return found

    def rows_of(which, blocks, band=slice(None)):
        if which < 2:
            return rows.at[which, blocks, band]
        if which == 2:
            return rows_h.at[0, blocks, band]
        wide = pl.multiple_of((mirrored(6 - which) - near_far) * piece, LANES)
        return rows_h.at[1, blocks, band, pl.ds(wide, piece)]

    last = n_bits - 1

    def a_start(which, stage):
        phase = min(stage, last)
        count = 1 << phase
        part = range(count) if stage < last else range((stage - last) * count // 2, (stage - last + 1) * count // 2)
        for m in part:
            for h in range(2):
                block_part = rows_of(which, a_blocks(h, phase)[m], pl.ds(h * half, half))
                remote(
                    block_part, block_part, a_send.at[which], a_recv.at[which, stage],
                    (i, flip(s, orders[h][phase])),
                ).start()

    def a_wait(which, stage):
        count = (1 << stage) if stage < last else (1 << last) // 2
        blocks = rows_of(which, pl.ds(0, count))
        remote(blocks, blocks, a_send.at[which], a_recv.at[which, stage], mate).wait_recv()

    def a_sent(which):
        blocks = rows_of(which, pl.ds(0, n_s - 1))
        remote(blocks, blocks, a_send.at[which], a_recv.at[which, 0], mate).wait_send()

    def a_next(which, phase):
        a_wait(which, phase)
        if phase + 1 < last:
            a_start(which, phase + 1)
        if phase == last - 2:
            a_start(which, last)
        if phase == last - 1:
            a_start(which, last + 1)

    def a_done(which):
        a_wait(which, last)
        a_wait(which, last + 1)

    far = pl.multiple_of(jnp.where(is_left, width - 2 * piece, 0), LANES)

    def lend_rows(st):
        return remote(
            rows.at[st, s, :, pl.ds(far, 2 * piece)], rows_h.at[st, s], ha_send.at[0], ha_recv.at[st], mate
        )

    gains[i] = gain_ref[...].astype(bf16).astype(f32)
    gain_copies = [
        remote(gains.at[i], gains.at[i], g_send.at[0], g_recv.at[0], (lax.rem(i + d, n_i), s))
        for d in range(1, n_i)
    ]
    gain_wait = remote(
        gains.at[pl.ds(0, n_i - 1)], gains.at[pl.ds(0, n_i - 1)], g_send.at[0], g_recv.at[0], mate
    )

    load_master.wait()

    def lower(j, _):
        at = pl.ds(pl.multiple_of(j * tall, tall), tall)
        for c in range(chunks):
            anchor[i, c, at, :] = master[at, c * LANES : (c + 1) * LANES].astype(bf16)
        return 0

    lax.fori_loop(0, piece // tall, lower, 0)
    for copy in load_rows:
        copy.wait()
    pl.semaphore_wait(barrier, n_i - 1 + n_s - 1)
    a_start(0, 0)

    @when_end
    def _():
        for c in range(chunks):
            z_mate(i, c).start()
            if c == 1:
                lend_rows(0).start()
        lend_rows(1).start()

    @when_inner
    def _():
        for c in range(chunks):
            z_mate(i, c).start()
            z_twin(i, c).start()

    for copy in gain_copies:
        copy.start()
    res[...] = jnp.zeros_like(res)
    for copy in load_rest:
        copy.wait()

    def joined(buffer, at, ds):
        return jnp.concatenate([buffer[at, c, ds, :] for c in range(chunks)], axis=1)

    def project(o, count=chunks):
        def body(k, _):
            start = pl.multiple_of(k * depth, depth)
            wide = pl.multiple_of(o * piece + k * depth, depth)
            part = rows[0, :, :, pl.ds(wide, depth)].reshape(tokens, depth)
            weights = [anchor[o, c, pl.ds(start, depth), :] for c in range(count)]
            res[:, : count * LANES] += jnp.dot(part, jnp.concatenate(weights, axis=1), preferred_element_type=f32)
            return 0

        lax.fori_loop(0, piece // depth, body, 0)

    def arrived(o, c):
        z_mate(o, c).wait_recv()

    held = chunks - 1
    groups = 2

    def part_copy():
        return remote(part_out, part_in, p_send, p_recv, mate)

    def project_for_end():
        weights = jnp.concatenate([anchor[near_far + k, held] for k in range(2)], axis=0)
        count = n_s // groups
        for g in range(groups):
            part = rows_h[0, g * count : (g + 1) * count].reshape(count * block, 2 * piece)
            part_out[g * count * block : (g + 1) * count * block, :] = jnp.dot(
                part, weights, preferred_element_type=f32
            ).astype(bf16)

    @when_end
    def _():
        one, two, three = mirrored(1), mirrored(2), mirrored(3)
        a_next(0, 0)
        a_start(1, 0)
        for p in range(1, last):
            a_next(0, p)
        a_done(0)
        project(i)
        for c in range(chunks):
            arrived(one, c)
        project(one)
        a_next(1, 0)
        for c in range(held):
            arrived(two, c)
        project(two, held)
        for p in range(1, last):
            a_next(1, p)
        for c in range(held):
            arrived(three, c)
        project(three, held)
        part_copy().wait_recv()
        res[:, held * LANES :] += part_in[...].astype(f32)

    @when_inner
    def _():
        zero, two, three = mirrored(0), mirrored(2), mirrored(3)

        def from_end(c):
            arrived(zero, c)
            z_twin(zero, c).start()

        def from_far(o, c):
            arrived(o, c)
            if c < held:
                z_mate(o, c).start()

        from_end(0)
        from_far(two, 0)
        a_next(0, 0)
        from_end(1)
        for c in range(1, chunks):
            from_far(two, c)
        from_end(2)
        for p in range(1, last):
            a_next(0, p)
        lend_rows(0).wait_recv()
        a_start(2, 0)
        from_far(three, 0)
        a_next(2, 0)
        a_start(1, 0)
        for c in range(3, chunks):
            from_end(c)
        a_done(0)
        project(i)
        from_far(three, 1)
        project(zero)
        for p in range(1, last):
            a_next(2, p)
        for c in range(2, held):
            from_far(three, c)
        project(two)
        from_far(three, held)
        a_done(2)
        project_for_end()
        part_copy().start()
        z_mate(two, held).start()
        z_mate(three, held).start()
        project(three)

    gain_wait.wait_recv()
    gain_anchor = jnp.concatenate([gains[j] for j in range(n_i)], axis=1)
    gain = gain_anchor

    def fold(value):
        total = value[:, :LANES]
        for c in range(1, chunks):
            total = total + value[:, c * LANES : (c + 1) * LANES]
        return jnp.sum(total.T, axis=0, keepdims=True)

    def spread(value):
        square = jnp.broadcast_to(value, (LANES, LANES)).T
        return jnp.concatenate([square] * chunks, axis=1)

    def row_stats(st, gain, between=None):
        def body(q, _):
            at = pl.ds(pl.multiple_of(q * LANES, LANES), LANES)
            r = stream[st, at, :].astype(f32) + res[at, :] * scale
            res[at, :] = r
            weighted = r * gain
            stats[st, 0, 0:1, at] = fold(r * r)
            stats[st, 0, 1:2, at] = fold(weighted * weighted)
            stats[st, 0, 2:3, at] = fold(weighted * goals[st, at, :].astype(f32))
            stats[st, 0, 3:4, at] = jnp.zeros((1, LANES), f32)
            return 0

        lax.fori_loop(0, tiles, body, 0)
        copies = [
            remote(
                stats.at[st, 0], stats.at[st, d], s_send.at[st], s_recv.at[st],
                (i, lax.rem(s + d, n_s)),
            )
            for d in range(1, n_s)
        ]
        for copy in copies:
            copy.start()
        if between is not None:
            between()
        others = stats.at[st, pl.ds(1, n_s - 1)]
        remote(others, others, s_send.at[st], s_recv.at[st], mate).wait()
        total = stats[st, 0]
        for d in range(1, n_s):
            total = total + stats[st, d]
        inverse = lax.rsqrt(total[0:1] * (1.0 / width) + norm_epsilon)
        pull = inverse * total[1:2] - total[2:3]
        line[0:1, :] = inverse
        line[1:2, :] = inverse * inverse * inverse * pull * (1.0 / width)

    def row_grads(st, gain):
        def body(q, total):
            at = pl.ds(pl.multiple_of(q * LANES, LANES), LANES)
            inverse, pull = spread(line[0:1, at]), spread(line[1:2, at])
            r = res[at, :]
            unit = r * inverse
            loss = unit * gain - goals[st, at, :].astype(f32)
            loss = loss.astype(bf16).astype(f32)
            low = (inverse * (loss * gain) - r * pull).astype(bf16)
            for c in range(chunks):
                slope[st, c, at, :] = low[:, c * LANES : (c + 1) * LANES]
            return total + jnp.sum(loss * unit, axis=0, keepdims=True)

        return lax.fori_loop(0, tiles, body, jnp.zeros((1, cols), f32))

    def product(part, against):
        return lax.dot_general(part, against, (((0,), (0,)), ((), ())), preferred_element_type=f32) * scale

    def weight_grad(st, wide, size):
        part = rows[st, :, :, pl.ds(pl.multiple_of(wide, size), size)].reshape(tokens, size)
        return product(part, joined(slope, st, slice(None)))

    def more_rows():
        @when_inner
        def _():
            a_next(1, 0)
            lend_rows(1).wait_recv()
            a_start(3, 0)

    row_stats(0, gain, more_rows)
    gain_first = row_grads(0, gain)
    res[...] = jnp.zeros_like(res)

    def lend_slope(st, c):
        return remote(slope.at[st, c], slope_h.at[st, c], r_send.at[0], r_recv.at[st, c], mate)

    @when_end
    def _():
        for c in range(held):
            lend_slope(0, c).start()

    spans = width // span
    per_piece = piece // span

    def place(q):
        return mirrored(q // per_piece), q % per_piece

    def step_one(q, ahead):
        o, j = place(q)
        at = pl.ds(pl.multiple_of(j * span, span), span)
        grad = weight_grad(0, o * piece + j * span, span)
        grads[o, at, :] = grad
        step = (inner_rate * grad) * pl.reciprocal(jnp.abs(grad) + adam_epsilon)
        param = keep * joined(anchor, o, at).astype(f32) - step
        ahead[...] = param.astype(bf16)

    def project_later(q, ahead):
        o, j = place(q)
        wide = pl.multiple_of(o * piece + j * span, span)
        part = rows[1, :, :, pl.ds(wide, span)].reshape(tokens, span)
        res[...] += jnp.dot(part, ahead[...], preferred_element_type=f32)

    def both(t, _):
        for k in (2, 3):

            @pl.when(2 * t == k * per_piece)
            def _():
                arrived(mirrored(k), held)

        project_later(jnp.maximum(2 * t - 1, 0), ahead_b)
        step_one(2 * t, ahead_a)
        project_later(2 * t, ahead_a)
        step_one(2 * t + 1, ahead_b)
        return 0

    def one_alone(q, _):
        step_one(q, later.at[q])
        return 0

    def later_alone(q, _):
        project_later(q, later.at[q])
        return 0

    @when_end
    def _():
        a_done(1)
        ahead_b[...] = jnp.zeros_like(ahead_b)
        lax.fori_loop(0, spans // 2, both, 0)
        project_later(spans - 1, ahead_b)

    @when_inner
    def _():
        lax.fori_loop(0, spans, one_alone, 0)
        for p in range(1, last):
            a_next(1, p)
        a_next(3, 0)
        a_done(1)
        lax.fori_loop(0, spans, later_alone, 0)
        for p in range(1, last):
            a_next(3, p)

    gain_step = first_update(gain_first)
    gain = gain_anchor - inner_rate * gain_step

    row_stats(1, gain)
    gain_second = row_grads(1, gain)
    when_inner(lambda: a_start(4, 0))
    gain_move = inner_rate * (gain_step + second_update(gain_first, gain_second))
    for j in range(n_i):
        gain_out[j] = gain_move[:, j * own : (j + 1) * own]

    @when_end
    def _():
        for c in range(chunks):
            lend_slope(1, c).start()
            if c == held - 1:
                lend_slope(0, held).start()

    gain_moves = [
        remote(
            gain_out.at[lax.rem(i + d, n_i)], gain_in.at[d], g_send.at[1], g_recv.at[1],
            (lax.rem(i + d, n_i), s),
        )
        for d in range(1, n_i)
    ]
    for copy in gain_moves:
        copy.start()

    def move(o):
        def body(j, _):
            at = pl.ds(pl.multiple_of(j * tall, tall), tall)
            grad = weight_grad(1, o * piece + j * tall, tall)
            grads[o, at, :] = outer_sum(grads[o, at, :], grad)
            return 0

        lax.fori_loop(0, piece // tall, body, 0)

    def give(slot, c):
        return remote(outgo.at[slot, c], from_mate.at[c], e_send.at[0], e_recv.at[c], mate)

    def cross(slot, c, at=slice(None)):
        return remote(
            outgo.at[slot, c, at], from_twin.at[slot, c, at], m_send.at[0], m_recv.at[slot, c], twin
        )

    def pack(slot, c, o, *others):
        lanes = slice(c * LANES, (c + 1) * LANES)

        def body(j, _):
            at = pl.ds(pl.multiple_of(j * tall, tall), tall)
            total = grads[o, at, lanes]
            for other in others:
                total = total + other[at, :].astype(f32)
            outgo[slot, c, at, :] = total.astype(bf16)
            return 0

        lax.fori_loop(0, piece // tall, body, 0)

    def finish(c, o, *others):
        lanes = slice(c * LANES, (c + 1) * LANES)

        def body(j, _):
            at = pl.ds(pl.multiple_of(j * tall, tall), tall)
            total = grads[o, at, lanes]
            for other in others:
                total = total + other[at, :].astype(f32)
            outer = master[at, lanes]
            pseudo = total * (1.0 / n_i) + (1.0 - keep * keep) * outer.astype(bf16).astype(f32)
            velocity = outer_momentum * moment[at, lanes] + pseudo
            velocity_ref[at, lanes] = velocity
            updated_ref[at, lanes] = outer - outer_rate * (pseudo + outer_momentum * velocity)
            return 0

        lax.fori_loop(0, piece // tall, body, 0)
    @when_end
    def _():
        o = mirrored(1)
        move(o)
        for c in range(chunks):
            pack(0, c, o)
        for c in range(chunks):
            give(0, c).start()
        o = mirrored(0)
        move(o)
        for c in range(chunks):
            give(0, c).wait_recv()
            finish(c, o, from_mate.at[c])

    def help_end(slot, c, o):
        base = (o - near_far) * piece
        lanes = slice(c * LANES, (c + 1) * LANES)

        def body(j, _):
            at = pl.ds(pl.multiple_of(j * tall, tall), tall)
            wide = pl.ds(pl.multiple_of(base + j * tall, tall), tall)
            pair = [
                product(rows_h[st, :, :, wide].reshape(tokens, tall), slope_h[st, c]) for st in range(steps)
            ]
            outgo[slot, c, at, :] = (grads[o, at, lanes] + outer_sum(*pair)).astype(bf16)
            cross(slot, c, at).start()
            return 0

        lax.fori_loop(0, piece // tall, body, 0)

    @when_inner
    def _():
        def help_and_cross(slot, c):
            help_end(slot, c, mirrored(3 - slot))

        def forward(c):
            cross(0, c).wait_recv()
            pack(2, c, mirrored(0), from_twin.at[0, c])
            give(2, c).start()

        move(mirrored(3))
        a_done(3)
        phases = list(range(last))
        for c in range(chunks):
            lend_slope(0, c).wait_recv()
            lend_slope(1, c).wait_recv()
            help_and_cross(0, c)
            if c == 0:
                a_next(4, phases.pop(0))
                move(mirrored(0))
            if c == 1:
                for p in phases:
                    a_next(4, p)
                move(mirrored(2))
            if c == chunks - 2:
                forward(0)
        a_done(4)
        for c in range(chunks):
            help_and_cross(1, c)
            if c + 1 < chunks:
                forward(c + 1)
            if c == 1:
                move(mirrored(1))
        for c in range(chunks):
            give(2, c).wait_recv()
            cross(1, c).wait_recv()
            finish(c, mirrored(1), from_mate.at[c], from_twin.at[1, c])

    moved_gains = gain_in.at[pl.ds(1, n_i - 1)]
    remote(moved_gains, moved_gains, g_send.at[1], g_recv.at[1], mate).wait()
    gain_total = gain_out[i]
    for d in range(1, n_i):
        gain_total = gain_total + gain_in[d]
    gain_pseudo = gain_total * (1.0 / n_i)
    gain_velocity = outer_momentum * gain_moment_ref[...] + gain_pseudo
    gain_velocity_ref[...] = gain_velocity
    gain_updated_ref[...] = gain_ref[...] - outer_rate * (gain_pseudo + outer_momentum * gain_velocity)

    def sent_pieces(way, count):
        pieces = anchor.at[pl.ds(0, count)]
        remote(pieces, pieces, z_send.at[way], z_recv.at[0, 0], mate).wait_send()

    @when_end
    def _():
        lent = rows_h.at[pl.ds(0, steps), 0]
        remote(lent, lent, ha_send.at[0], ha_recv.at[0], mate).wait_send()
        sent_pieces(0, 1)
        remote(slope, slope, r_send.at[0], r_recv.at[0, 0], mate).wait_send()
        remote(from_mate, from_mate, e_send.at[0], e_recv.at[0], mate).wait_send()

    @when_inner
    def _():
        remote(from_twin, from_twin, m_send.at[0], m_recv.at[0, 0], twin).wait_send()
        remote(from_mate, from_mate, e_send.at[0], e_recv.at[0], mate).wait_send()
        part_copy().wait_send()
        for which in (2, 3, 4):
            a_sent(which)
        sent_pieces(0, 3)
        sent_pieces(1, 2)

    gain_wait.wait_send()
    a_sent(0)
    a_sent(1)


def write_out(*refs):
    count = len(refs) // 2
    sem = refs[-1]
    copies = [pltpu.make_async_copy(refs[k], refs[count + k], sem.at[k]) for k in range(count)]
    for copy in copies:
        copy.start()
    for copy in copies:
        copy.wait()


def per_device(weight_master, gain_master, weight_moment, gain_moment, attended, stream, targets):
    n_i, n_s = lax.axis_size("island"), lax.axis_size("shard")
    _, steps, block, width = attended.shape
    _, _, tokens, cols = stream.shape
    piece = weight_master.shape[0]
    own = gain_master.shape[0]
    f32, bf16 = jnp.float32, jnp.bfloat16
    chunks = cols // LANES
    arrays = [
        ((piece, cols), f32),
        ((piece, cols), f32),
        ((steps, n_s, block, width), bf16),
        ((steps, n_s, block, 2 * piece), bf16),
        ((n_i, chunks, piece, LANES), bf16),
        ((min(512, piece), cols), bf16),
        ((min(512, piece), cols), bf16),
        ((width // min(512, piece), min(512, piece), cols), bf16),
        ((n_i, piece, cols), f32),
        ((tokens, cols), f32),
        ((steps, chunks, tokens, LANES), bf16),
        ((steps, chunks, tokens, LANES), bf16),
        ((steps, tokens, cols), bf16),
        ((steps, tokens, cols), bf16),
        ((3, chunks, piece, LANES), bf16),
        ((chunks, piece, LANES), bf16),
        ((2, chunks, piece, LANES), bf16),
        ((tokens, LANES), bf16),
        ((tokens, LANES), bf16),
        ((steps, n_s, 4, tokens), f32),
        ((2, tokens), f32),
        ((n_i, 1, own), f32),
        ((n_i, 1, own), f32),
        ((n_i, 1, own), f32),
    ]
    held = sum(math.prod(shape) * jnp.dtype(kind).itemsize for shape, kind in arrays)
    if n_i != 4 or steps != 2 or own % LANES or chunks < 2 or block % 32 or n_s < 8 or held > 60e6:
        return general_device(weight_master, gain_master, weight_moment, gain_moment, attended, stream, targets)
    any_space = pl.BlockSpec(memory_space=pl.ANY)
    vmem = pl.BlockSpec(memory_space=pltpu.VMEM)
    dma = pltpu.SemaphoreType.DMA
    outs = ((piece, cols), (1, own), (piece, cols), (1, own))
    results = pl.pallas_call(
        functools.partial(kernel, n_i, n_s),
        out_shape=tuple(pltpu.VMEM(shape, f32) for shape in outs),
        in_specs=[any_space, vmem, any_space, vmem, any_space, any_space, any_space],
        out_specs=(vmem, vmem, vmem, vmem),
        scratch_shapes=[pltpu.VMEM(shape, kind) for shape, kind in arrays]
        + [
            dma((4 + steps,)),
            dma((2,)),
            dma((n_i, chunks)),
            dma((5,)),
            dma((5, n_s.bit_length())),
            dma(()),
            dma(()),
            dma((1,)),
            dma((steps,)),
            dma((steps,)),
            dma((steps,)),
            dma((2,)),
            dma((2,)),
            dma((1,)),
            dma((steps, chunks)),
            dma((1,)),
            dma((chunks,)),
            dma((1,)),
            dma((2, chunks)),
        ],
        compiler_params=pltpu.CompilerParams(
            collective_id=0, has_side_effects=True, vmem_limit_bytes=58 << 20
        ),
    )(weight_master, gain_master[None], weight_moment, gain_moment[None], attended, stream, targets)
    results = [pltpu.with_memory_space_constraint(x, pltpu.VMEM) for x in results]
    updated, gain_updated, velocity, gain_velocity = pl.pallas_call(
        write_out,
        out_shape=tuple(jax.ShapeDtypeStruct(shape, f32) for shape in outs),
        in_specs=[vmem] * 4,
        out_specs=(any_space,) * 4,
        scratch_shapes=[dma((4,))],
        compiler_params=pltpu.CompilerParams(vmem_limit_bytes=1 << 20),
    )(*results)
    return (updated, gain_updated[0], velocity, gain_velocity[0])


def solution(mesh):
    placed = (
        P("island", "shard"),
        P(("shard", "island")),
        P("island", "shard"),
        P(("shard", "island")),
        P("island", None, "shard", None),
        P("island", None, None, "shard"),
        P("island", None, None, "shard"),
    )
    return jax.shard_map(
        per_device,
        mesh=mesh,
        in_specs=placed,
        out_specs=(
            P("island", "shard"),
            P(("shard", "island")),
            P("island", "shard"),
            P(("shard", "island")),
        ),
        check_vma=False,
    )
```

```python
import functools
import math

import jax
import jax.numpy as jnp
from jax import lax
from jax.experimental import pallas as pl
from jax.experimental.pallas import tpu as pltpu
from jax.sharding import PartitionSpec as P

norm_epsilon = 1e-05
inner_rate = 0.05
beta_one = 0.9
beta_two = 0.95
adam_epsilon = 0.3
decay_rate = 0.1
outer_rate = 0.7
outer_momentum = 0.9

MESH = pl.DeviceIdType.MESH
LANES = 128
keep = 1.0 - inner_rate * decay_rate


def flip(index, bit):
    size = 1 << bit
    return index + size * (1 - 2 * (lax.div(index, size) % 2))


def first_update(grad):
    return grad / (jnp.abs(grad) + adam_epsilon)


def second_update(earlier, grad):
    first = (beta_one * (1.0 - beta_one)) * earlier + (1.0 - beta_one) * grad
    second = (beta_two * (1.0 - beta_two)) * earlier * earlier + (1.0 - beta_two) * grad * grad
    first_hat = first * (1.0 / (1.0 - beta_one**2))
    second_hat = second * (1.0 / (1.0 - beta_two**2))
    return first_hat / (jnp.sqrt(second_hat) + adam_epsilon)


def general_kernel(
    n_i, n_s, low_ref, gain_ref, rows_ref, stream_ref, goals_ref, total_ref, gain_total_ref,
    rows, anchor, later, grads, res, slope_low, stream, goals, from_left, from_right,
    stats, line, gains, gain_moves,
    local_sem, z_send, z_recv, a_send, a_recv, s_send, s_recv, g_send, g_recv, r_send, r_recv,
):
    i = lax.axis_index("island")
    s = lax.axis_index("shard")
    steps, _, block, width = rows.shape
    piece, cols = low_ref.shape
    tokens = n_s * block
    tiles = tokens // LANES
    scale = width ** (-0.5)
    depth = min(512, piece)
    tall = min(256, piece)

    barrier = pltpu.get_barrier_semaphore()
    for d in range(1, n_i):
        pl.semaphore_signal(barrier, inc=1, device_id=(lax.rem(i + d, n_i), s), device_id_type=MESH)
    for d in range(1, n_s):
        pl.semaphore_signal(barrier, inc=1, device_id=(i, lax.rem(s + d, n_s)), device_id_type=MESH)

    locals_ = [pltpu.make_async_copy(low_ref, anchor.at[i], local_sem.at[0])]
    for st in range(steps):
        locals_.append(pltpu.make_async_copy(rows_ref.at[0, st], rows.at[st, s], local_sem.at[1 + st]))
    locals_.append(pltpu.make_async_copy(stream_ref.at[0], stream, local_sem.at[1 + steps]))
    locals_.append(pltpu.make_async_copy(goals_ref.at[0], goals, local_sem.at[2 + steps]))
    for copy in locals_:
        copy.start()
    pl.semaphore_wait(barrier, n_i - 1 + n_s - 1)

    def remote(src, dst, send, recv, to):
        return pltpu.make_async_remote_copy(
            src_ref=src, dst_ref=dst, send_sem=send, recv_sem=recv, device_id=to, device_id_type=MESH
        )

    right, left = (lax.rem(i + 1, n_i), s), (lax.rem(i + n_i - 1, n_i), s)

    def z_copy(way, t, at):
        return remote(
            anchor.at[at], anchor.at[at], z_send.at[way, t], z_recv.at[way, t], right if way == 0 else left
        )

    def z_start(t):
        @pl.when((i < n_i - 1) & (i - t >= 0))
        def _():
            z_copy(0, t, i - t).start()

        @pl.when((i > 0) & (i + t <= n_i - 1))
        def _():
            z_copy(1, t, i + t).start()

    def z_wait(t):
        @pl.when(i - 1 - t >= 0)
        def _():
            z_copy(0, t, i - 1 - t).wait_recv()

        @pl.when(i + 1 + t <= n_i - 1)
        def _():
            z_copy(1, t, i + 1 + t).wait_recv()

    n_bits = n_s.bit_length() - 1
    orders = [list(range(1, n_bits)) + [0], list(range(n_bits - 1, 0, -1)) + [0]]

    def a_blocks(st, phase):
        order = orders[st % 2]
        found = []
        for m in range(1 << phase):
            at = s
            for q in range(phase):
                if (m >> q) & 1:
                    at = flip(at, order[q])
            found.append(at)
        return found

    def a_copy(st, phase, m, at):
        slot = (1 << phase) - 1 + m
        return remote(
            rows.at[st, at], rows.at[st, at], a_send.at[st, slot], a_recv.at[st, slot],
            (i, flip(s, orders[st % 2][phase])),
        )

    def a_start(phase):
        for st in range(steps):
            for m, at in enumerate(a_blocks(st, phase)):
                a_copy(st, phase, m, at).start()

    def a_wait(phase):
        for st in range(steps):
            for m, at in enumerate(a_blocks(st, phase)):
                a_copy(st, phase, m, flip(at, orders[st % 2][phase])).wait_recv()

    def to_islands(buffer, which):
        return [
            remote(
                buffer.at[0], buffer.at[d], g_send.at[which, d], g_recv.at[which, d],
                (lax.rem(i + d, n_i), s),
            )
            for d in range(1, n_i)
        ]

    locals_[0].wait()
    z_start(0)
    for copy in locals_[1 : 1 + steps]:
        copy.wait()
    a_start(0)
    gains[0] = gain_ref[...]
    gain_in = to_islands(gains, 0)
    for copy in gain_in:
        copy.start()
    res[...] = jnp.zeros_like(res)
    for copy in locals_[1 + steps :]:
        copy.wait()

    def project(st, weights, at):
        def body(k, _):
            start = pl.multiple_of(k * depth, depth)
            wide = pl.multiple_of(at * piece + k * depth, depth)
            part = rows[st, :, :, pl.ds(wide, depth)].reshape(tokens, depth)
            res[...] += jnp.dot(part, weights[at, pl.ds(start, depth), :], preferred_element_type=jnp.float32)
            return 0

        lax.fori_loop(0, piece // depth, body, 0)

    def project_arrived(t):
        @pl.when(i - 1 - t >= 0)
        def _():
            project(0, anchor, i - 1 - t)

        @pl.when(i + 1 + t <= n_i - 1)
        def _():
            project(0, anchor, i + 1 + t)

    events = [(2.0 * t + 2.6, "z", t) for t in range(n_i - 1)]
    events += [(2.0 * ((2 << p) - 1), "a", p) for p in range(n_bits - 1)]
    last = events[-1][0] if n_bits > 1 else 0.0
    events.append((last + 0.1, "a", n_bits - 1))
    gathered, ready = False, []
    for _, kind, at in sorted(events):
        if kind == "a":
            a_wait(at)
            if at + 1 < n_bits:
                a_start(at + 1)
            else:
                gathered = True
                project(0, anchor, i)
                for t in ready:
                    project_arrived(t)
        else:
            z_wait(at)
            if at + 1 < n_i - 1:
                z_start(at + 1)
            if gathered:
                project_arrived(at)
            else:
                ready.append(at)

    for copy in gain_in:
        copy.wait()
    gain_anchor = gains[0]
    for d in range(1, n_i):
        gain_anchor = gain_anchor + gains[d]
    gain = gain_anchor

    def fold(value):
        total = value[:, :LANES]
        for c in range(1, cols // LANES):
            total = total + value[:, c * LANES : (c + 1) * LANES]
        return jnp.sum(total.T, axis=0, keepdims=True)

    def spread(value):
        square = jnp.broadcast_to(value, (LANES, LANES)).T
        return jnp.concatenate([square] * (cols // LANES), axis=1)

    def row_stats(st, gain):
        def body(q, _):
            at = pl.ds(pl.multiple_of(q * LANES, LANES), LANES)
            r = stream[st, at, :].astype(jnp.float32) + res[at, :] * scale
            res[at, :] = r
            weighted = r * gain
            stats[st, 0, 0:1, at] = fold(r * r)
            stats[st, 0, 1:2, at] = fold(weighted * weighted)
            stats[st, 0, 2:3, at] = fold(weighted * goals[st, at, :].astype(jnp.float32))
            stats[st, 0, 3:4, at] = jnp.zeros((1, LANES), jnp.float32)
            return 0

        lax.fori_loop(0, tiles, body, 0)
        copies = [
            remote(
                stats.at[st, 0], stats.at[st, d], s_send.at[st, d], s_recv.at[st, d],
                (i, lax.rem(s + d, n_s)),
            )
            for d in range(1, n_s)
        ]
        for copy in copies:
            copy.start()
        for copy in copies:
            copy.wait()
        total = stats[st, 0]
        for d in range(1, n_s):
            total = total + stats[st, d]
        inverse = lax.rsqrt(total[0:1] * (1.0 / width) + norm_epsilon)
        slope = inverse * total[1:2] - total[2:3]
        line[0:1, :] = inverse
        line[1:2, :] = inverse * inverse * inverse * slope * (1.0 / width)

    def row_grads(st, gain):
        def body(q, total):
            at = pl.ds(pl.multiple_of(q * LANES, LANES), LANES)
            inverse, pull = spread(line[0:1, at]), spread(line[1:2, at])
            r = res[at, :]
            unit = r * inverse
            loss = unit * gain - goals[st, at, :].astype(jnp.float32)
            loss = loss.astype(jnp.bfloat16).astype(jnp.float32)
            slope_low[at, :] = (inverse * (loss * gain) - r * pull).astype(jnp.bfloat16)
            return total + jnp.sum(loss * unit, axis=0, keepdims=True)

        return lax.fori_loop(0, tiles, body, jnp.zeros((1, cols), jnp.float32))

    def weight_grad(st, wide):
        part = rows[st, :, :, pl.ds(pl.multiple_of(wide, tall), tall)].reshape(tokens, tall)
        return (
            lax.dot_general(
                part, slope_low[...], (((0,), (0,)), ((), ())), preferred_element_type=jnp.float32
            )
            * scale
        )

    row_stats(0, gain)
    gain_first = row_grads(0, gain)
    per_piece = piece // tall

    def step_one(q, _):
        o, j = q // per_piece, q % per_piece
        at = pl.ds(pl.multiple_of(j * tall, tall), tall)
        grad = weight_grad(0, q * tall)
        grads[o, at, :] = grad
        param = keep * anchor[o, at, :].astype(jnp.float32) - inner_rate * first_update(grad)
        later[o, at, :] = param.astype(jnp.bfloat16)
        return 0

    lax.fori_loop(0, n_i * per_piece, step_one, 0)
    gain_step = first_update(gain_first)
    gain = gain_anchor - inner_rate * gain_step

    res[...] = jnp.zeros_like(res)

    def project_later(at, _):
        project(1, later, at)
        return 0

    lax.fori_loop(0, n_i, project_later, 0)
    row_stats(1, gain)
    gain_second = row_grads(1, gain)
    gain_moves[0] = inner_rate * (gain_step + second_update(gain_first, gain_second))
    gain_out = to_islands(gain_moves, 1)
    for copy in gain_out:
        copy.start()

    def to_right(k):
        at = n_i - 1 - k
        return remote(later.at[at], from_left.at[k], r_send.at[0, k], r_recv.at[0, k], right)

    def to_left(k):
        return remote(later.at[k], from_right.at[k], r_send.at[1, k], r_recv.at[1, k], left)

    early = 1 - lax.div(2 * i, n_i)

    def owner_piece(q, _):
        o = q + early * (n_i - 1 - 2 * q)

        def step_two(j, _):
            at = pl.ds(pl.multiple_of(j * tall, tall), tall)
            grad = weight_grad(1, o * piece + j * tall)
            earlier = grads[o, at, :]
            moved = (1.0 - keep * keep) * anchor[o, at, :].astype(jnp.float32) + inner_rate * (
                keep * first_update(earlier) + second_update(earlier, grad)
            )
            grads[o, at, :] = moved
            later[o, at, :] = moved.astype(jnp.bfloat16)
            return 0

        lax.fori_loop(0, per_piece, step_two, 0)

        @pl.when((i == 0) & (o > 0))
        def _():
            to_right(n_i - 1 - o).start()

        @pl.when((i == n_i - 1) & (o < n_i - 1))
        def _():
            to_left(o).start()

        return 0

    lax.fori_loop(0, n_i, owner_piece, 0)

    def add(o, arrived, k):
        def body(j, _):
            at = pl.ds(pl.multiple_of(j * tall, tall), tall)
            later[o, at, :] = (grads[o, at, :] + arrived[k, at, :].astype(jnp.float32)).astype(jnp.bfloat16)
            return 0

        lax.fori_loop(0, per_piece, body, 0)

    for t in range(n_i - 1):
        k_right = t - i
        k_left = t - (n_i - 1 - i)

        @pl.when((i > 0) & (k_right >= 0) & (k_right < n_i - 1 - i))
        def _():
            to_right(k_right).wait_recv()
            add(n_i - 1 - k_right, from_left, k_right)
            to_right(k_right).start()

        @pl.when((i < n_i - 1) & (k_left >= 0) & (k_left < i))
        def _():
            to_left(k_left).wait_recv()
            add(k_left, from_right, k_left)
            to_left(k_left).start()

    for copy in gain_out:
        copy.wait()
    gain_total = gain_moves[0]
    for d in range(1, n_i):
        gain_total = gain_total + gain_moves[d]
    gain_total_ref[...] = gain_total

    total_ref[...] = grads[i]

    @pl.when(i > 0)
    def _():
        k = n_i - 1 - i
        to_right(k).wait_recv()
        total_ref[...] += from_left[k].astype(jnp.float32)

    @pl.when(i < n_i - 1)
    def _():
        to_left(i).wait_recv()
        total_ref[...] += from_right[i].astype(jnp.float32)

    for k in range(n_i - 1):

        @pl.when(k < n_i - 1 - i)
        def _(k=k):
            to_right(k).wait_send()

        @pl.when(k < i)
        def _(k=k):
            to_left(k).wait_send()

        @pl.when((i < n_i - 1) & (i - k >= 0))
        def _(k=k):
            z_copy(0, k, i - k).wait_send()

        @pl.when((i > 0) & (i + k <= n_i - 1))
        def _(k=k):
            z_copy(1, k, i + k).wait_send()

    for phase in range(n_bits):
        for st in range(steps):
            for m, at in enumerate(a_blocks(st, phase)):
                a_copy(st, phase, m, at).wait_send()


def general_device(weight_master, gain_master, weight_moment, gain_moment, attended, stream, targets):
    n_i, n_s = lax.axis_size("island"), lax.axis_size("shard")
    _, steps, block, width = attended.shape
    _, _, tokens, cols = stream.shape
    piece = weight_master.shape[0]
    own = gain_master.shape[0]
    offset = lax.axis_index("island") * own
    low = weight_master.astype(jnp.bfloat16)
    gain_low = gain_master.astype(jnp.bfloat16).astype(jnp.float32)
    gain_row = lax.dynamic_update_slice(jnp.zeros((1, cols), jnp.float32), gain_low[None], (0, offset))
    any_space = pl.BlockSpec(memory_space=pl.ANY)
    vmem = pl.BlockSpec(memory_space=pltpu.VMEM)
    f32, bf16 = jnp.float32, jnp.bfloat16
    dma = pltpu.SemaphoreType.DMA
    weight_summed, gain_summed = pl.pallas_call(
        functools.partial(general_kernel, n_i, n_s),
        out_shape=(
            jax.ShapeDtypeStruct((piece, cols), f32),
            jax.ShapeDtypeStruct((1, cols), f32),
        ),
        in_specs=[any_space, vmem, any_space, any_space, any_space],
        out_specs=(vmem, vmem),
        scratch_shapes=[
            pltpu.VMEM((steps, n_s, block, width), bf16),
            pltpu.VMEM((n_i, piece, cols), bf16),
            pltpu.VMEM((n_i, piece, cols), bf16),
            pltpu.VMEM((n_i, piece, cols), f32),
            pltpu.VMEM((tokens, cols), f32),
            pltpu.VMEM((tokens, cols), bf16),
            pltpu.VMEM((steps, tokens, cols), bf16),
            pltpu.VMEM((steps, tokens, cols), bf16),
            pltpu.VMEM((n_i - 1, piece, cols), bf16),
            pltpu.VMEM((n_i - 1, piece, cols), bf16),
            pltpu.VMEM((steps, n_s, 4, tokens), f32),
            pltpu.VMEM((2, tokens), f32),
            pltpu.VMEM((n_i, 1, cols), f32),
            pltpu.VMEM((n_i, 1, cols), f32),
            dma((3 + steps,)),
            dma((2, n_i - 1)),
            dma((2, n_i - 1)),
            dma((steps, n_s - 1)),
            dma((steps, n_s - 1)),
            dma((steps, n_s)),
            dma((steps, n_s)),
            dma((2, n_i)),
            dma((2, n_i)),
            dma((2, n_i - 1)),
            dma((2, n_i - 1)),
        ],
        compiler_params=pltpu.CompilerParams(
            collective_id=0, has_side_effects=True, vmem_limit_bytes=67043328
        ),
    )(low, gain_row, attended, stream, targets)
    weight_pseudo = weight_summed / n_i
    gain_pseudo = lax.dynamic_slice(gain_summed, (0, offset), (1, own))[0] / n_i
    weight_velocity = outer_momentum * weight_moment + weight_pseudo
    gain_velocity = outer_momentum * gain_moment + gain_pseudo
    weight_updated = weight_master - outer_rate * (weight_pseudo + outer_momentum * weight_velocity)
    gain_updated = gain_master - outer_rate * (gain_pseudo + outer_momentum * gain_velocity)
    return (weight_updated, gain_updated, weight_velocity, gain_velocity)


def outer_sum(grad_one, grad_two):
    first = (inner_rate * beta_one * (1.0 - beta_one) / (1.0 - beta_one**2)) * grad_one + (
        inner_rate * (1.0 - beta_one) / (1.0 - beta_one**2)
    ) * grad_two
    second = (beta_two * (1.0 - beta_two) / (1.0 - beta_two**2)) * (grad_one * grad_one) + (
        (1.0 - beta_two) / (1.0 - beta_two**2)
    ) * (grad_two * grad_two)
    root = second * lax.rsqrt(jnp.maximum(second, 1e-30)) + adam_epsilon
    size = jnp.abs(grad_one) + adam_epsilon
    return ((inner_rate * keep) * grad_one * root + first * size) * pl.reciprocal(root * size)


def kernel(
    n_i, n_s, master_ref, gain_ref, moment_ref, gain_moment_ref, rows_ref, stream_ref, goals_ref,
    updated_ref, gain_updated_ref, velocity_ref, gain_velocity_ref,
    master, moment, rows, rows_h, anchor, ahead_a, ahead_b, later, grads, res, slope, slope_h, stream, goals,
    outgo, from_mate, from_twin, part_out, part_in, early, stats, line, gains, gain_out, gain_in,
    local_sem, z_send, z_recv, a_send, a_recv, p_send, p_recv, ha_send, ha_recv,
    s_send, s_recv, g_send, g_recv, r_send, r_recv, e_send, e_recv, m_send, m_recv,
):
    i = lax.axis_index("island")
    s = lax.axis_index("shard")
    steps, _, block, width = rows.shape
    _, chunks, piece, _ = anchor.shape
    cols = chunks * LANES
    own = gains.shape[2]
    tokens = n_s * block
    tiles = tokens // LANES
    scale = width ** (-0.5)
    exact = math.frexp(scale)[0] == 0.5
    depth = min(1024, piece)
    tall = min(256, piece)
    span = min(512, piece)
    f32, bf16 = jnp.float32, jnp.bfloat16

    is_left = i < n_i // 2
    is_end = (i == 0) | (i == n_i - 1)
    is_inner = (i > 0) & (i < n_i - 1)
    toward = jnp.where(is_left, 1, -1)
    mate = (jnp.where(is_end, i + toward, i - toward), s)
    twin = (n_i - 1 - i, s)

    def when_inner(f):
        pl.when(is_inner)(f)

    def when_end(f):
        pl.when(is_end)(f)

    def mirrored(o):
        return jnp.where(is_left, o, n_i - 1 - o)

    near_far = jnp.where(is_left, n_i - 2, 0)
    barrier = pltpu.get_barrier_semaphore()
    for d in range(1, n_i):
        pl.semaphore_signal(barrier, inc=1, device_id=(lax.rem(i + d, n_i), s), device_id_type=MESH)
    for d in range(1, n_s):
        pl.semaphore_signal(barrier, inc=1, device_id=(i, lax.rem(s + d, n_s)), device_id_type=MESH)

    load_master = pltpu.make_async_copy(master_ref, master, local_sem.at[0])
    load_rows = [
        pltpu.make_async_copy(rows_ref.at[0, st], rows.at[st, s], local_sem.at[1 + st]) for st in range(steps)
    ]
    load_rest = [
        pltpu.make_async_copy(stream_ref.at[0], stream, local_sem.at[1 + steps]),
        pltpu.make_async_copy(goals_ref.at[0], goals, local_sem.at[2 + steps]),
        pltpu.make_async_copy(moment_ref, moment, local_sem.at[3 + steps]),
    ]
    for copy in [load_master] + load_rows + load_rest:
        copy.start()

    def remote(src, dst, send, recv, to):
        return pltpu.make_async_remote_copy(
            src_ref=src, dst_ref=dst, send_sem=send, recv_sem=recv, device_id=to, device_id_type=MESH
        )

    def z_mate(o, c):
        return remote(anchor.at[o, c], anchor.at[o, c], z_send.at[0], z_recv.at[o, c], mate)

    def z_twin(o, c):
        return remote(anchor.at[o, c], anchor.at[o, c], z_send.at[1], z_recv.at[o, c], twin)

    n_bits = n_s.bit_length() - 1
    orders = [list(range(1, n_bits)) + [0], list(range(n_bits - 1, 0, -1)) + [0]]
    half = block // 2

    def a_blocks(h, phase):
        found = []
        for m in range(1 << phase):
            at = s
            for q in range(phase):
                if (m >> q) & 1:
                    at = flip(at, orders[h][q])
            found.append(at)
        return found

    def rows_of(which, blocks, band=slice(None)):
        if which < 2:
            return rows.at[which, blocks, band]
        if which == 2:
            return rows_h.at[0, blocks, band]
        wide = pl.multiple_of((mirrored(6 - which) - near_far) * piece, LANES)
        return rows_h.at[1, blocks, band, pl.ds(wide, piece)]

    last = n_bits - 1

    def a_start(which, stage):
        phase = min(stage, last)
        count = 1 << phase
        part = range(count) if stage < last else range((stage - last) * count // 2, (stage - last + 1) * count // 2)
        for m in part:
            for h in range(2):
                block_part = rows_of(which, a_blocks(h, phase)[m], pl.ds(h * half, half))
                remote(
                    block_part, block_part, a_send.at[which], a_recv.at[which, stage],
                    (i, flip(s, orders[h][phase])),
                ).start()

    def a_wait(which, stage):
        count = (1 << stage) if stage < last else (1 << last) // 2
        blocks = rows_of(which, pl.ds(0, count))
        remote(blocks, blocks, a_send.at[which], a_recv.at[which, stage], mate).wait_recv()

    def a_sent(which):
        blocks = rows_of(which, pl.ds(0, n_s - 1))
        remote(blocks, blocks, a_send.at[which], a_recv.at[which, 0], mate).wait_send()

    def a_next(which, phase):
        a_wait(which, phase)
        if phase + 1 < last:
            a_start(which, phase + 1)
        if phase == last - 2:
            a_start(which, last)
        if phase == last - 1:
            a_start(which, last + 1)

    def a_done(which):
        a_wait(which, last)
        a_wait(which, last + 1)

    far = pl.multiple_of(jnp.where(is_left, width - 2 * piece, 0), LANES)

    def lend_rows(st):
        return remote(
            rows.at[st, s, :, pl.ds(far, 2 * piece)], rows_h.at[st, s], ha_send.at[0], ha_recv.at[st], mate
        )

    gains[i] = gain_ref[...].astype(bf16).astype(f32)
    gain_copies = [
        remote(gains.at[i], gains.at[i], g_send.at[0], g_recv.at[0], (lax.rem(i + d, n_i), s))
        for d in range(1, n_i)
    ]
    gain_wait = remote(
        gains.at[pl.ds(0, n_i - 1)], gains.at[pl.ds(0, n_i - 1)], g_send.at[0], g_recv.at[0], mate
    )

    load_master.wait()

    def lower(j, _):
        at = pl.ds(pl.multiple_of(j * tall, tall), tall)
        for c in range(chunks):
            anchor[i, c, at, :] = master[at, c * LANES : (c + 1) * LANES].astype(bf16)
        return 0

    lax.fori_loop(0, piece // tall, lower, 0)
    for copy in load_rows:
        copy.wait()
    pl.semaphore_wait(barrier, n_i - 1 + n_s - 1)
    for copy in gain_copies:
        copy.start()
    a_start(0, 0)

    @when_end
    def _():
        for c in range(chunks):
            z_mate(i, c).start()
            if c == 1:
                lend_rows(0).start()
        lend_rows(1).start()

    @when_inner
    def _():
        for c in range(chunks):
            z_mate(i, c).start()
            z_twin(i, c).start()

    res[...] = jnp.zeros_like(res)
    for copy in load_rest:
        copy.wait()

    def joined(buffer, at, ds):
        return jnp.concatenate([buffer[at, c, ds, :] for c in range(chunks)], axis=1)

    def project(o, count=chunks):
        def body(k, _):
            start = pl.multiple_of(k * depth, depth)
            wide = pl.multiple_of(o * piece + k * depth, depth)
            part = rows[0, :, :, pl.ds(wide, depth)].reshape(tokens, depth)
            weights = [anchor[o, c, pl.ds(start, depth), :] for c in range(count)]
            res[:, : count * LANES] += jnp.dot(part, jnp.concatenate(weights, axis=1), preferred_element_type=f32)
            return 0

        lax.fori_loop(0, piece // depth, body, 0)

    def arrived(o, c):
        z_mate(o, c).wait_recv()

    held = chunks - 1
    groups = 2

    def fold(value):
        return jnp.sum(value.T, axis=0, keepdims=True)

    def spread(value):
        return jnp.broadcast_to(value, (LANES, LANES)).T

    def tile_at(q):
        return pl.ds(pl.multiple_of(q * LANES, LANES), LANES)

    def lanes_of(c):
        return slice(c * LANES, (c + 1) * LANES)

    def products(st, gain, at, among):
        sums = None
        for c in among:
            r = stream[st, at, lanes_of(c)].astype(f32) + res[at, lanes_of(c)] * scale
            res[at, lanes_of(c)] = r
            weighted = r * gain[:, lanes_of(c)]
            terms = (r * r, weighted * weighted, weighted * goals[st, at, lanes_of(c)].astype(f32))
            sums = terms if sums is None else tuple(a + b for a, b in zip(sums, terms))
        return sums

    def local_stats(st, gain, among, held_sums):
        def body(q, _):
            at = tile_at(q)
            sums = products(st, gain, at, among)
            for k in range(3):
                value = sums[k] + early[k, at, :] if held_sums else sums[k]
                stats[st, 0, k : k + 1, at] = fold(value)
            stats[st, 0, 3:4, at] = jnp.zeros((1, LANES), f32)
            return 0

        lax.fori_loop(0, tiles, body, 0, unroll=True)

    def early_stats(q, _):
        at = tile_at(q)
        sums = products(0, gain_anchor, at, range(held))
        for k in range(3):
            early[k, at, :] = sums[k]
        return 0

    def part_copy():
        return remote(part_out, part_in, p_send, p_recv, mate)

    def project_for_end():
        weights = jnp.concatenate([anchor[near_far + k, held] for k in range(2)], axis=0)
        count = n_s // groups
        for g in range(groups):
            part = rows_h[0, g * count : (g + 1) * count].reshape(count * block, 2 * piece)
            part_out[g * count * block : (g + 1) * count * block, :] = jnp.dot(
                part, weights, preferred_element_type=f32
            ).astype(bf16)

    gain_wait.wait_recv()
    gain_anchor = jnp.concatenate([gains[j] for j in range(n_i)], axis=1)
    gain = gain_anchor

    @when_end
    def _():
        one, two, three = mirrored(1), mirrored(2), mirrored(3)
        a_next(0, 0)
        a_start(1, 0)
        for p in range(1, last):
            a_next(0, p)
        a_done(0)
        project(i)
        for c in range(chunks):
            arrived(one, c)
        project(one)
        a_next(1, 0)
        for c in range(held):
            arrived(two, c)
        project(two, held)
        for p in range(1, last):
            a_next(1, p)
        for c in range(held):
            arrived(three, c)
        project(three, held)
        lax.fori_loop(0, tiles, early_stats, 0, unroll=True)
        part_copy().wait_recv()
        res[:, held * LANES :] += part_in[...].astype(f32)
        local_stats(0, gain_anchor, (held,), True)

    @when_inner
    def _():
        zero, two, three = mirrored(0), mirrored(2), mirrored(3)

        def from_end(c):
            arrived(zero, c)
            z_twin(zero, c).start()

        def from_far(o, c):
            arrived(o, c)
            if c < held:
                z_mate(o, c).start()

        from_end(0)
        from_far(two, 0)
        a_next(0, 0)
        from_end(1)
        for c in range(1, chunks):
            from_far(two, c)
        from_end(2)
        for p in range(1, last):
            a_next(0, p)
        lend_rows(0).wait_recv()
        a_start(2, 0)
        from_far(three, 0)
        a_next(2, 0)
        a_start(1, 0)
        for c in range(3, chunks):
            from_end(c)
        a_done(0)
        project(i)
        from_far(three, 1)
        project(zero)
        for p in range(1, last):
            a_next(2, p)
        for c in range(2, held):
            from_far(three, c)
        project(two)
        from_far(three, held)
        a_done(2)
        project_for_end()
        part_copy().start()
        project(three)

    def row_stats(st, between=None):
        copies = [
            remote(
                stats.at[st, 0], stats.at[st, d], s_send.at[st], s_recv.at[st],
                (i, lax.rem(s + d, n_s)),
            )
            for d in range(1, n_s)
        ]
        for copy in copies:
            copy.start()
        if between is not None:
            between()
        others = stats.at[st, pl.ds(1, n_s - 1)]
        remote(others, others, s_send.at[st], s_recv.at[st], mate).wait()
        total = stats[st, 0]
        for d in range(1, n_s):
            total = total + stats[st, d]
        inverse = lax.rsqrt(total[0:1] * (1.0 / width) + norm_epsilon)
        pull = inverse * total[1:2] - total[2:3]
        line[0:1, :] = inverse
        line[1:2, :] = inverse * inverse * inverse * pull * (1.0 / width)

    def row_grads(st, gain, among):
        def body(q, totals):
            at = tile_at(q)
            inverse, pull = spread(line[0:1, at]), spread(line[1:2, at])
            found = []
            for c, total in zip(among, totals):
                r = res[at, lanes_of(c)]
                unit = r * inverse
                scaled = gain[:, lanes_of(c)]
                loss = unit * scaled - goals[st, at, lanes_of(c)].astype(f32)
                loss = loss.astype(bf16).astype(f32)
                low = inverse * (loss * scaled) - r * pull
                slope[st, c, at, :] = (low * scale if exact else low).astype(bf16)
                found.append(total + jnp.sum(loss * unit, axis=0, keepdims=True))
            return tuple(found)

        return lax.fori_loop(0, tiles, body, (jnp.zeros((1, LANES), f32),) * len(among), unroll=True)

    def product(part, against):
        grad = lax.dot_general(part, against, (((0,), (0,)), ((), ())), preferred_element_type=f32)
        return grad if exact else grad * scale

    def weight_grad(st, wide, size):
        part = rows[st, :, :, pl.ds(pl.multiple_of(wide, size), size)].reshape(tokens, size)
        return product(part, joined(slope, st, slice(None)))

    def more_rows():
        @when_inner
        def _():
            a_next(1, 0)
            lend_rows(1).wait_recv()
            a_start(3, 0)

    when_inner(lambda: local_stats(0, gain_anchor, range(chunks), False))
    row_stats(0, more_rows)
    gain_first = jnp.concatenate(row_grads(0, gain, range(chunks)), axis=1)
    res[...] = jnp.zeros_like(res)

    def lend_slope(st, c):
        return remote(slope.at[st, c], slope_h.at[st, c], r_send.at[0], r_recv.at[st, c], mate)

    @when_end
    def _():
        for c in range(held):
            lend_slope(0, c).start()

    spans = width // span
    per_piece = piece // span

    def place(q):
        return mirrored(q // per_piece), q % per_piece

    def grad_one(q):
        o, j = place(q)
        return weight_grad(0, o * piece + j * span, span)

    def step_one(q, grad, ahead):
        o, j = place(q)
        at = pl.ds(pl.multiple_of(j * span, span), span)
        grads[o, at, :] = grad
        step = (inner_rate * grad) * pl.reciprocal(jnp.abs(grad) + adam_epsilon)
        param = keep * joined(anchor, o, at).astype(f32) - step
        ahead[...] = param.astype(bf16)

    def project_later(q, ahead):
        o, j = place(q)
        wide = pl.multiple_of(o * piece + j * span, span)
        part = rows[1, :, :, pl.ds(wide, span)].reshape(tokens, span)
        res[...] += jnp.dot(part, ahead[...], preferred_element_type=f32)

    def both(t, _):
        for k in (2, 3):

            @pl.when(2 * t == k * per_piece)
            def _():
                arrived(mirrored(k), held)

        project_later(jnp.maximum(2 * t - 1, 0), ahead_b)
        even = grad_one(2 * t)
        odd = grad_one(2 * t + 1)
        step_one(2 * t, even, ahead_a)
        project_later(2 * t, ahead_a)
        step_one(2 * t + 1, odd, ahead_b)
        return 0

    def one_alone(q, _):
        step_one(q, grad_one(q), later.at[q])
        return 0

    def later_alone(q, _):
        project_later(q, later.at[q])
        return 0

    @when_end
    def _():
        a_done(1)
        ahead_b[...] = jnp.zeros_like(ahead_b)
        lax.fori_loop(0, spans // 2, both, 0)
        project_later(spans - 1, ahead_b)

    @when_inner
    def _():
        lax.fori_loop(0, spans, one_alone, 0)
        z_mate(mirrored(2), held).start()
        z_mate(mirrored(3), held).start()
        for p in range(1, last):
            a_next(1, p)
        a_next(3, 0)
        a_done(1)
        lax.fori_loop(0, spans, later_alone, 0)
        for p in range(1, last):
            a_next(3, p)

    gain_step = first_update(gain_first)
    gain = gain_anchor - inner_rate * gain_step

    local_stats(1, gain, range(chunks), False)
    row_stats(1)
    is_even = lax.rem(s, 2) == 0
    gain_second = row_grads(1, gain, (0,))

    @pl.when(is_end & is_even)
    def _():
        lend_slope(1, 0).start()

    gain_second = jnp.concatenate(gain_second + row_grads(1, gain, range(1, chunks)), axis=1)
    when_inner(lambda: a_start(4, 0))
    gain_move = inner_rate * (gain_step + second_update(gain_first, gain_second))
    for j in range(n_i):
        gain_out[j] = gain_move[:, j * own : (j + 1) * own]

    gain_moves = [
        remote(
            gain_out.at[lax.rem(i + d, n_i)], gain_in.at[d], g_send.at[1], g_recv.at[1],
            (lax.rem(i + d, n_i), s),
        )
        for d in range(1, n_i)
    ]
    for copy in gain_moves:
        copy.start()

    def move(o, first=0, until=piece // tall):
        def body(j, _):
            at = pl.ds(pl.multiple_of(j * tall, tall), tall)
            grad = weight_grad(1, o * piece + j * tall, tall)
            grads[o, at, :] = outer_sum(grads[o, at, :], grad)
            return 0

        lax.fori_loop(first, until, body, 0)

    def give(slot, c):
        return remote(outgo.at[slot, c], from_mate.at[c], e_send.at[0], e_recv.at[c], mate)

    def cross(slot, c, at=slice(None)):
        return remote(
            outgo.at[slot, c, at], from_twin.at[slot, c, at], m_send.at[0], m_recv.at[slot, c], twin
        )

    def pack(slot, c, o, *others):
        lanes = slice(c * LANES, (c + 1) * LANES)

        def body(j, _):
            at = pl.ds(pl.multiple_of(j * tall, tall), tall)
            total = grads[o, at, lanes]
            for other in others:
                total = total + other[at, :].astype(f32)
            outgo[slot, c, at, :] = total.astype(bf16)
            return 0

        lax.fori_loop(0, piece // tall, body, 0)

    def finish(c, o, *others):
        lanes = slice(c * LANES, (c + 1) * LANES)

        def body(j, _):
            at = pl.ds(pl.multiple_of(j * tall, tall), tall)
            total = grads[o, at, lanes]
            for other in others:
                total = total + other[at, :].astype(f32)
            outer = master[at, lanes]
            pseudo = total * (1.0 / n_i) + (1.0 - keep * keep) * outer.astype(bf16).astype(f32)
            velocity = outer_momentum * moment[at, lanes] + pseudo
            velocity_ref[at, lanes] = velocity
            updated_ref[at, lanes] = outer - outer_rate * (pseudo + outer_momentum * velocity)
            return 0

        lax.fori_loop(0, piece // tall, body, 0)
    @when_end
    def _():
        o = mirrored(1)
        parts = piece // tall
        wait_parts = parts - 1
        move(o, 0, wait_parts)

        @pl.when(jnp.logical_not(is_even))
        def _():
            lend_slope(1, 0).start()

        move(o, wait_parts, parts)
        for c in range(chunks):
            pack(0, c, o)
        for c in range(1, chunks):
            lend_slope(1, c).start()
            if c == held - 1:
                lend_slope(0, held).start()
        for c in range(chunks):
            give(0, c).start()
        o = mirrored(0)
        move(o)
        for c in range(chunks):
            give(0, c).wait_recv()
            finish(c, o, from_mate.at[c])

    def help_end(slot, c, o):
        base = (o - near_far) * piece
        lanes = slice(c * LANES, (c + 1) * LANES)

        def body(j, _):
            at = pl.ds(pl.multiple_of(j * tall, tall), tall)
            wide = pl.ds(pl.multiple_of(base + j * tall, tall), tall)
            pair = [
                product(rows_h[st, :, :, wide].reshape(tokens, tall), slope_h[st, c]) for st in range(steps)
            ]
            outgo[slot, c, at, :] = (grads[o, at, lanes] + outer_sum(*pair)).astype(bf16)
            cross(slot, c, at).start()
            return 0

        lax.fori_loop(0, piece // tall, body, 0)

    @when_inner
    def _():
        def help_and_cross(slot, c):
            help_end(slot, c, mirrored(3 - slot))

        def forward(c):
            cross(0, c).wait_recv()
            pack(2, c, mirrored(0), from_twin.at[0, c])
            give(2, c).start()

        move(mirrored(3))
        a_done(3)

        def far_sum(c):
            lend_slope(0, c).wait_recv()
            lend_slope(1, c).wait_recv()
            help_and_cross(0, c)

        phases = list(range(last))
        for c in range(held):
            far_sum(c)
            if c == 0:
                a_next(4, phases.pop(0))
                move(mirrored(0))
            if c == 1:
                for p in phases:
                    a_next(4, p)
                move(mirrored(2))
        forward(0)
        a_done(4)
        help_and_cross(1, 0)
        far_sum(held)
        for c in range(1, chunks):
            if c < held:
                forward(c)
            help_and_cross(1, c)
            if c == 1:
                move(mirrored(1))
        forward(held)
        for c in range(chunks):
            give(2, c).wait_recv()
            cross(1, c).wait_recv()
            finish(c, mirrored(1), from_mate.at[c], from_twin.at[1, c])

    moved_gains = gain_in.at[pl.ds(1, n_i - 1)]
    remote(moved_gains, moved_gains, g_send.at[1], g_recv.at[1], mate).wait()
    gain_total = gain_out[i]
    for d in range(1, n_i):
        gain_total = gain_total + gain_in[d]
    gain_pseudo = gain_total * (1.0 / n_i)
    gain_velocity = outer_momentum * gain_moment_ref[...] + gain_pseudo
    gain_velocity_ref[...] = gain_velocity
    gain_updated_ref[...] = gain_ref[...] - outer_rate * (gain_pseudo + outer_momentum * gain_velocity)

    def sent_pieces(way, count):
        pieces = anchor.at[pl.ds(0, count)]
        remote(pieces, pieces, z_send.at[way], z_recv.at[0, 0], mate).wait_send()

    @when_end
    def _():
        lent = rows_h.at[pl.ds(0, steps), 0]
        remote(lent, lent, ha_send.at[0], ha_recv.at[0], mate).wait_send()
        sent_pieces(0, 1)
        remote(slope, slope, r_send.at[0], r_recv.at[0, 0], mate).wait_send()
        remote(from_mate, from_mate, e_send.at[0], e_recv.at[0], mate).wait_send()

    @when_inner
    def _():
        remote(from_twin, from_twin, m_send.at[0], m_recv.at[0, 0], twin).wait_send()
        remote(from_mate, from_mate, e_send.at[0], e_recv.at[0], mate).wait_send()
        part_copy().wait_send()
        for which in (2, 3, 4):
            a_sent(which)
        sent_pieces(0, 3)
        sent_pieces(1, 2)

    gain_wait.wait_send()
    a_sent(0)
    a_sent(1)


def write_out(*refs):
    count = len(refs) // 2
    sem = refs[-1]
    copies = [pltpu.make_async_copy(refs[k], refs[count + k], sem.at[k]) for k in range(count)]
    for copy in copies:
        copy.start()
    for copy in copies:
        copy.wait()


def per_device(weight_master, gain_master, weight_moment, gain_moment, attended, stream, targets):
    n_i, n_s = lax.axis_size("island"), lax.axis_size("shard")
    _, steps, block, width = attended.shape
    _, _, tokens, cols = stream.shape
    piece = weight_master.shape[0]
    own = gain_master.shape[0]
    f32, bf16 = jnp.float32, jnp.bfloat16
    chunks = cols // LANES
    arrays = [
        ((piece, cols), f32),
        ((piece, cols), f32),
        ((steps, n_s, block, width), bf16),
        ((steps, n_s, block, 2 * piece), bf16),
        ((n_i, chunks, piece, LANES), bf16),
        ((min(512, piece), cols), bf16),
        ((min(512, piece), cols), bf16),
        ((width // min(512, piece), min(512, piece), cols), bf16),
        ((n_i, piece, cols), f32),
        ((tokens, cols), f32),
        ((steps, chunks, tokens, LANES), bf16),
        ((steps, chunks, tokens, LANES), bf16),
        ((steps, tokens, cols), bf16),
        ((steps, tokens, cols), bf16),
        ((3, chunks, piece, LANES), bf16),
        ((chunks, piece, LANES), bf16),
        ((2, chunks, piece, LANES), bf16),
        ((tokens, LANES), bf16),
        ((tokens, LANES), bf16),
        ((3, tokens, LANES), f32),
        ((steps, n_s, 4, tokens), f32),
        ((2, tokens), f32),
        ((n_i, 1, own), f32),
        ((n_i, 1, own), f32),
        ((n_i, 1, own), f32),
    ]
    held = sum(math.prod(shape) * jnp.dtype(kind).itemsize for shape, kind in arrays)
    if n_i != 4 or steps != 2 or own % LANES or chunks < 2 or block % 32 or n_s < 8 or held > 60e6:
        return general_device(weight_master, gain_master, weight_moment, gain_moment, attended, stream, targets)
    any_space = pl.BlockSpec(memory_space=pl.ANY)
    vmem = pl.BlockSpec(memory_space=pltpu.VMEM)
    dma = pltpu.SemaphoreType.DMA
    outs = ((piece, cols), (1, own), (piece, cols), (1, own))
    results = pl.pallas_call(
        functools.partial(kernel, n_i, n_s),
        out_shape=tuple(pltpu.VMEM(shape, f32) for shape in outs),
        in_specs=[any_space, vmem, any_space, vmem, any_space, any_space, any_space],
        out_specs=(vmem, vmem, vmem, vmem),
        scratch_shapes=[pltpu.VMEM(shape, kind) for shape, kind in arrays]
        + [
            dma((4 + steps,)),
            dma((2,)),
            dma((n_i, chunks)),
            dma((5,)),
            dma((5, n_s.bit_length())),
            dma(()),
            dma(()),
            dma((1,)),
            dma((steps,)),
            dma((steps,)),
            dma((steps,)),
            dma((2,)),
            dma((2,)),
            dma((1,)),
            dma((steps, chunks)),
            dma((1,)),
            dma((chunks,)),
            dma((1,)),
            dma((2, chunks)),
        ],
        compiler_params=pltpu.CompilerParams(
            collective_id=0, has_side_effects=True, vmem_limit_bytes=58 << 20
        ),
    )(weight_master, gain_master[None], weight_moment, gain_moment[None], attended, stream, targets)
    results = [pltpu.with_memory_space_constraint(x, pltpu.VMEM) for x in results]
    updated, gain_updated, velocity, gain_velocity = pl.pallas_call(
        write_out,
        out_shape=tuple(jax.ShapeDtypeStruct(shape, f32) for shape in outs),
        in_specs=[vmem] * 4,
        out_specs=(any_space,) * 4,
        scratch_shapes=[dma((4,))],
        compiler_params=pltpu.CompilerParams(vmem_limit_bytes=1 << 20),
    )(*results)
    return (updated, gain_updated[0], velocity, gain_velocity[0])


def solution(mesh):
    placed = (
        P("island", "shard"),
        P(("shard", "island")),
        P("island", "shard"),
        P(("shard", "island")),
        P("island", None, "shard", None),
        P("island", None, None, "shard"),
        P("island", None, None, "shard"),
    )
    return jax.shard_map(
        per_device,
        mesh=mesh,
        in_specs=placed,
        out_specs=(
            P("island", "shard"),
            P(("shard", "island")),
            P("island", "shard"),
            P(("shard", "island")),
        ),
        check_vma=False,
    )
```

```python
import functools
import math

import jax
import jax.numpy as jnp
from jax import lax
from jax.experimental import pallas as pl
from jax.experimental.pallas import tpu as pltpu
from jax.sharding import PartitionSpec as P

norm_epsilon = 1e-05
inner_rate = 0.05
beta_one = 0.9
beta_two = 0.95
adam_epsilon = 0.3
decay_rate = 0.1
outer_rate = 0.7
outer_momentum = 0.9

MESH = pl.DeviceIdType.MESH
LANES = 128
keep = 1.0 - inner_rate * decay_rate


def flip(index, bit):
    size = 1 << bit
    return index + size * (1 - 2 * (lax.div(index, size) % 2))


def first_update(grad):
    return grad / (jnp.abs(grad) + adam_epsilon)


def second_update(earlier, grad):
    first = (beta_one * (1.0 - beta_one)) * earlier + (1.0 - beta_one) * grad
    second = (beta_two * (1.0 - beta_two)) * earlier * earlier + (1.0 - beta_two) * grad * grad
    first_hat = first * (1.0 / (1.0 - beta_one**2))
    second_hat = second * (1.0 / (1.0 - beta_two**2))
    return first_hat / (jnp.sqrt(second_hat) + adam_epsilon)


def general_kernel(
    n_i, n_s, low_ref, gain_ref, rows_ref, stream_ref, goals_ref, total_ref, gain_total_ref,
    rows, anchor, later, grads, res, slope_low, stream, goals, from_left, from_right,
    stats, line, gains, gain_moves,
    local_sem, z_send, z_recv, a_send, a_recv, s_send, s_recv, g_send, g_recv, r_send, r_recv,
):
    i = lax.axis_index("island")
    s = lax.axis_index("shard")
    steps, _, block, width = rows.shape
    piece, cols = low_ref.shape
    tokens = n_s * block
    tiles = tokens // LANES
    scale = width ** (-0.5)
    depth = min(512, piece)
    tall = min(256, piece)

    barrier = pltpu.get_barrier_semaphore()
    for d in range(1, n_i):
        pl.semaphore_signal(barrier, inc=1, device_id=(lax.rem(i + d, n_i), s), device_id_type=MESH)
    for d in range(1, n_s):
        pl.semaphore_signal(barrier, inc=1, device_id=(i, lax.rem(s + d, n_s)), device_id_type=MESH)

    locals_ = [pltpu.make_async_copy(low_ref, anchor.at[i], local_sem.at[0])]
    for st in range(steps):
        locals_.append(pltpu.make_async_copy(rows_ref.at[0, st], rows.at[st, s], local_sem.at[1 + st]))
    locals_.append(pltpu.make_async_copy(stream_ref.at[0], stream, local_sem.at[1 + steps]))
    locals_.append(pltpu.make_async_copy(goals_ref.at[0], goals, local_sem.at[2 + steps]))
    for copy in locals_:
        copy.start()
    pl.semaphore_wait(barrier, n_i - 1 + n_s - 1)

    def remote(src, dst, send, recv, to):
        return pltpu.make_async_remote_copy(
            src_ref=src, dst_ref=dst, send_sem=send, recv_sem=recv, device_id=to, device_id_type=MESH
        )

    right, left = (lax.rem(i + 1, n_i), s), (lax.rem(i + n_i - 1, n_i), s)

    def z_copy(way, t, at):
        return remote(
            anchor.at[at], anchor.at[at], z_send.at[way, t], z_recv.at[way, t], right if way == 0 else left
        )

    def z_start(t):
        @pl.when((i < n_i - 1) & (i - t >= 0))
        def _():
            z_copy(0, t, i - t).start()

        @pl.when((i > 0) & (i + t <= n_i - 1))
        def _():
            z_copy(1, t, i + t).start()

    def z_wait(t):
        @pl.when(i - 1 - t >= 0)
        def _():
            z_copy(0, t, i - 1 - t).wait_recv()

        @pl.when(i + 1 + t <= n_i - 1)
        def _():
            z_copy(1, t, i + 1 + t).wait_recv()

    n_bits = n_s.bit_length() - 1
    orders = [list(range(1, n_bits)) + [0], list(range(n_bits - 1, 0, -1)) + [0]]

    def a_blocks(st, phase):
        order = orders[st % 2]
        found = []
        for m in range(1 << phase):
            at = s
            for q in range(phase):
                if (m >> q) & 1:
                    at = flip(at, order[q])
            found.append(at)
        return found

    def a_copy(st, phase, m, at):
        slot = (1 << phase) - 1 + m
        return remote(
            rows.at[st, at], rows.at[st, at], a_send.at[st, slot], a_recv.at[st, slot],
            (i, flip(s, orders[st % 2][phase])),
        )

    def a_start(phase):
        for st in range(steps):
            for m, at in enumerate(a_blocks(st, phase)):
                a_copy(st, phase, m, at).start()

    def a_wait(phase):
        for st in range(steps):
            for m, at in enumerate(a_blocks(st, phase)):
                a_copy(st, phase, m, flip(at, orders[st % 2][phase])).wait_recv()

    def to_islands(buffer, which):
        return [
            remote(
                buffer.at[0], buffer.at[d], g_send.at[which, d], g_recv.at[which, d],
                (lax.rem(i + d, n_i), s),
            )
            for d in range(1, n_i)
        ]

    locals_[0].wait()
    z_start(0)
    for copy in locals_[1 : 1 + steps]:
        copy.wait()
    a_start(0)
    gains[0] = gain_ref[...]
    gain_in = to_islands(gains, 0)
    for copy in gain_in:
        copy.start()
    res[...] = jnp.zeros_like(res)
    for copy in locals_[1 + steps :]:
        copy.wait()

    def project(st, weights, at):
        def body(k, _):
            start = pl.multiple_of(k * depth, depth)
            wide = pl.multiple_of(at * piece + k * depth, depth)
            part = rows[st, :, :, pl.ds(wide, depth)].reshape(tokens, depth)
            res[...] += jnp.dot(part, weights[at, pl.ds(start, depth), :], preferred_element_type=jnp.float32)
            return 0

        lax.fori_loop(0, piece // depth, body, 0)

    def project_arrived(t):
        @pl.when(i - 1 - t >= 0)
        def _():
            project(0, anchor, i - 1 - t)

        @pl.when(i + 1 + t <= n_i - 1)
        def _():
            project(0, anchor, i + 1 + t)

    events = [(2.0 * t + 2.6, "z", t) for t in range(n_i - 1)]
    events += [(2.0 * ((2 << p) - 1), "a", p) for p in range(n_bits - 1)]
    last = events[-1][0] if n_bits > 1 else 0.0
    events.append((last + 0.1, "a", n_bits - 1))
    gathered, ready = False, []
    for _, kind, at in sorted(events):
        if kind == "a":
            a_wait(at)
            if at + 1 < n_bits:
                a_start(at + 1)
            else:
                gathered = True
                project(0, anchor, i)
                for t in ready:
                    project_arrived(t)
        else:
            z_wait(at)
            if at + 1 < n_i - 1:
                z_start(at + 1)
            if gathered:
                project_arrived(at)
            else:
                ready.append(at)

    for copy in gain_in:
        copy.wait()
    gain_anchor = gains[0]
    for d in range(1, n_i):
        gain_anchor = gain_anchor + gains[d]
    gain = gain_anchor

    def fold(value):
        total = value[:, :LANES]
        for c in range(1, cols // LANES):
            total = total + value[:, c * LANES : (c + 1) * LANES]
        return jnp.sum(total.T, axis=0, keepdims=True)

    def spread(value):
        square = jnp.broadcast_to(value, (LANES, LANES)).T
        return jnp.concatenate([square] * (cols // LANES), axis=1)

    def row_stats(st, gain):
        def body(q, _):
            at = pl.ds(pl.multiple_of(q * LANES, LANES), LANES)
            r = stream[st, at, :].astype(jnp.float32) + res[at, :] * scale
            res[at, :] = r
            weighted = r * gain
            stats[st, 0, 0:1, at] = fold(r * r)
            stats[st, 0, 1:2, at] = fold(weighted * weighted)
            stats[st, 0, 2:3, at] = fold(weighted * goals[st, at, :].astype(jnp.float32))
            stats[st, 0, 3:4, at] = jnp.zeros((1, LANES), jnp.float32)
            return 0

        lax.fori_loop(0, tiles, body, 0)
        copies = [
            remote(
                stats.at[st, 0], stats.at[st, d], s_send.at[st, d], s_recv.at[st, d],
                (i, lax.rem(s + d, n_s)),
            )
            for d in range(1, n_s)
        ]
        for copy in copies:
            copy.start()
        for copy in copies:
            copy.wait()
        total = stats[st, 0]
        for d in range(1, n_s):
            total = total + stats[st, d]
        inverse = lax.rsqrt(total[0:1] * (1.0 / width) + norm_epsilon)
        slope = inverse * total[1:2] - total[2:3]
        line[0:1, :] = inverse
        line[1:2, :] = inverse * inverse * inverse * slope * (1.0 / width)

    def row_grads(st, gain):
        def body(q, total):
            at = pl.ds(pl.multiple_of(q * LANES, LANES), LANES)
            inverse, pull = spread(line[0:1, at]), spread(line[1:2, at])
            r = res[at, :]
            unit = r * inverse
            loss = unit * gain - goals[st, at, :].astype(jnp.float32)
            loss = loss.astype(jnp.bfloat16).astype(jnp.float32)
            slope_low[at, :] = (inverse * (loss * gain) - r * pull).astype(jnp.bfloat16)
            return total + jnp.sum(loss * unit, axis=0, keepdims=True)

        return lax.fori_loop(0, tiles, body, jnp.zeros((1, cols), jnp.float32))

    def weight_grad(st, wide):
        part = rows[st, :, :, pl.ds(pl.multiple_of(wide, tall), tall)].reshape(tokens, tall)
        return (
            lax.dot_general(
                part, slope_low[...], (((0,), (0,)), ((), ())), preferred_element_type=jnp.float32
            )
            * scale
        )

    row_stats(0, gain)
    gain_first = row_grads(0, gain)
    per_piece = piece // tall

    def step_one(q, _):
        o, j = q // per_piece, q % per_piece
        at = pl.ds(pl.multiple_of(j * tall, tall), tall)
        grad = weight_grad(0, q * tall)
        grads[o, at, :] = grad
        param = keep * anchor[o, at, :].astype(jnp.float32) - inner_rate * first_update(grad)
        later[o, at, :] = param.astype(jnp.bfloat16)
        return 0

    lax.fori_loop(0, n_i * per_piece, step_one, 0)
    gain_step = first_update(gain_first)
    gain = gain_anchor - inner_rate * gain_step

    res[...] = jnp.zeros_like(res)

    def project_later(at, _):
        project(1, later, at)
        return 0

    lax.fori_loop(0, n_i, project_later, 0)
    row_stats(1, gain)
    gain_second = row_grads(1, gain)
    gain_moves[0] = inner_rate * (gain_step + second_update(gain_first, gain_second))
    gain_out = to_islands(gain_moves, 1)
    for copy in gain_out:
        copy.start()

    def to_right(k):
        at = n_i - 1 - k
        return remote(later.at[at], from_left.at[k], r_send.at[0, k], r_recv.at[0, k], right)

    def to_left(k):
        return remote(later.at[k], from_right.at[k], r_send.at[1, k], r_recv.at[1, k], left)

    early = 1 - lax.div(2 * i, n_i)

    def owner_piece(q, _):
        o = q + early * (n_i - 1 - 2 * q)

        def step_two(j, _):
            at = pl.ds(pl.multiple_of(j * tall, tall), tall)
            grad = weight_grad(1, o * piece + j * tall)
            earlier = grads[o, at, :]
            moved = (1.0 - keep * keep) * anchor[o, at, :].astype(jnp.float32) + inner_rate * (
                keep * first_update(earlier) + second_update(earlier, grad)
            )
            grads[o, at, :] = moved
            later[o, at, :] = moved.astype(jnp.bfloat16)
            return 0

        lax.fori_loop(0, per_piece, step_two, 0)

        @pl.when((i == 0) & (o > 0))
        def _():
            to_right(n_i - 1 - o).start()

        @pl.when((i == n_i - 1) & (o < n_i - 1))
        def _():
            to_left(o).start()

        return 0

    lax.fori_loop(0, n_i, owner_piece, 0)

    def add(o, arrived, k):
        def body(j, _):
            at = pl.ds(pl.multiple_of(j * tall, tall), tall)
            later[o, at, :] = (grads[o, at, :] + arrived[k, at, :].astype(jnp.float32)).astype(jnp.bfloat16)
            return 0

        lax.fori_loop(0, per_piece, body, 0)

    for t in range(n_i - 1):
        k_right = t - i
        k_left = t - (n_i - 1 - i)

        @pl.when((i > 0) & (k_right >= 0) & (k_right < n_i - 1 - i))
        def _():
            to_right(k_right).wait_recv()
            add(n_i - 1 - k_right, from_left, k_right)
            to_right(k_right).start()

        @pl.when((i < n_i - 1) & (k_left >= 0) & (k_left < i))
        def _():
            to_left(k_left).wait_recv()
            add(k_left, from_right, k_left)
            to_left(k_left).start()

    for copy in gain_out:
        copy.wait()
    gain_total = gain_moves[0]
    for d in range(1, n_i):
        gain_total = gain_total + gain_moves[d]
    gain_total_ref[...] = gain_total

    total_ref[...] = grads[i]

    @pl.when(i > 0)
    def _():
        k = n_i - 1 - i
        to_right(k).wait_recv()
        total_ref[...] += from_left[k].astype(jnp.float32)

    @pl.when(i < n_i - 1)
    def _():
        to_left(i).wait_recv()
        total_ref[...] += from_right[i].astype(jnp.float32)

    for k in range(n_i - 1):

        @pl.when(k < n_i - 1 - i)
        def _(k=k):
            to_right(k).wait_send()

        @pl.when(k < i)
        def _(k=k):
            to_left(k).wait_send()

        @pl.when((i < n_i - 1) & (i - k >= 0))
        def _(k=k):
            z_copy(0, k, i - k).wait_send()

        @pl.when((i > 0) & (i + k <= n_i - 1))
        def _(k=k):
            z_copy(1, k, i + k).wait_send()

    for phase in range(n_bits):
        for st in range(steps):
            for m, at in enumerate(a_blocks(st, phase)):
                a_copy(st, phase, m, at).wait_send()


def general_device(weight_master, gain_master, weight_moment, gain_moment, attended, stream, targets):
    n_i, n_s = lax.axis_size("island"), lax.axis_size("shard")
    _, steps, block, width = attended.shape
    _, _, tokens, cols = stream.shape
    piece = weight_master.shape[0]
    own = gain_master.shape[0]
    offset = lax.axis_index("island") * own
    low = weight_master.astype(jnp.bfloat16)
    gain_low = gain_master.astype(jnp.bfloat16).astype(jnp.float32)
    gain_row = lax.dynamic_update_slice(jnp.zeros((1, cols), jnp.float32), gain_low[None], (0, offset))
    any_space = pl.BlockSpec(memory_space=pl.ANY)
    vmem = pl.BlockSpec(memory_space=pltpu.VMEM)
    f32, bf16 = jnp.float32, jnp.bfloat16
    dma = pltpu.SemaphoreType.DMA
    weight_summed, gain_summed = pl.pallas_call(
        functools.partial(general_kernel, n_i, n_s),
        out_shape=(
            jax.ShapeDtypeStruct((piece, cols), f32),
            jax.ShapeDtypeStruct((1, cols), f32),
        ),
        in_specs=[any_space, vmem, any_space, any_space, any_space],
        out_specs=(vmem, vmem),
        scratch_shapes=[
            pltpu.VMEM((steps, n_s, block, width), bf16),
            pltpu.VMEM((n_i, piece, cols), bf16),
            pltpu.VMEM((n_i, piece, cols), bf16),
            pltpu.VMEM((n_i, piece, cols), f32),
            pltpu.VMEM((tokens, cols), f32),
            pltpu.VMEM((tokens, cols), bf16),
            pltpu.VMEM((steps, tokens, cols), bf16),
            pltpu.VMEM((steps, tokens, cols), bf16),
            pltpu.VMEM((n_i - 1, piece, cols), bf16),
            pltpu.VMEM((n_i - 1, piece, cols), bf16),
            pltpu.VMEM((steps, n_s, 4, tokens), f32),
            pltpu.VMEM((2, tokens), f32),
            pltpu.VMEM((n_i, 1, cols), f32),
            pltpu.VMEM((n_i, 1, cols), f32),
            dma((3 + steps,)),
            dma((2, n_i - 1)),
            dma((2, n_i - 1)),
            dma((steps, n_s - 1)),
            dma((steps, n_s - 1)),
            dma((steps, n_s)),
            dma((steps, n_s)),
            dma((2, n_i)),
            dma((2, n_i)),
            dma((2, n_i - 1)),
            dma((2, n_i - 1)),
        ],
        compiler_params=pltpu.CompilerParams(
            collective_id=0, has_side_effects=True, vmem_limit_bytes=67043328
        ),
    )(low, gain_row, attended, stream, targets)
    weight_pseudo = weight_summed / n_i
    gain_pseudo = lax.dynamic_slice(gain_summed, (0, offset), (1, own))[0] / n_i
    weight_velocity = outer_momentum * weight_moment + weight_pseudo
    gain_velocity = outer_momentum * gain_moment + gain_pseudo
    weight_updated = weight_master - outer_rate * (weight_pseudo + outer_momentum * weight_velocity)
    gain_updated = gain_master - outer_rate * (gain_pseudo + outer_momentum * gain_velocity)
    return (weight_updated, gain_updated, weight_velocity, gain_velocity)


def outer_sum(grad_one, grad_two):
    first = (inner_rate * beta_one * (1.0 - beta_one) / (1.0 - beta_one**2)) * grad_one + (
        inner_rate * (1.0 - beta_one) / (1.0 - beta_one**2)
    ) * grad_two
    second = (beta_two * (1.0 - beta_two) / (1.0 - beta_two**2)) * (grad_one * grad_one) + (
        (1.0 - beta_two) / (1.0 - beta_two**2)
    ) * (grad_two * grad_two)
    root = second * lax.rsqrt(jnp.maximum(second, 1e-30)) + adam_epsilon
    size = jnp.abs(grad_one) + adam_epsilon
    return ((inner_rate * keep) * grad_one * root + first * size) * pl.reciprocal(root * size)


def kernel(
    n_i, n_s, master_ref, gain_ref, moment_ref, gain_moment_ref, rows_ref, stream_ref, goals_ref,
    updated_ref, gain_updated_ref, velocity_ref, gain_velocity_ref,
    master, moment, rows, rows_h, anchor, ahead_a, ahead_b, later, grads, res, slope, slope_h, stream, goals,
    outgo, from_mate, from_twin, part_out, part_in, early, stats, line, gains, gain_out, gain_in,
    round_sem, local_sem, z_send, z_recv, a_send, a_recv, p_send, p_recv, ha_send, ha_recv,
    s_send, s_recv, g_send, g_recv, r_send, r_recv, e_send, e_recv, m_send, m_recv,
):
    i = lax.axis_index("island")
    s = lax.axis_index("shard")
    steps, _, block, width = rows.shape
    _, chunks, piece, _ = anchor.shape
    cols = chunks * LANES
    own = gains.shape[2]
    tokens = n_s * block
    tiles = tokens // LANES
    scale = width ** (-0.5)
    exact = math.frexp(scale)[0] == 0.5
    depth = min(1024, piece)
    tall = min(256, piece)
    span = min(512, piece)
    f32, bf16 = jnp.float32, jnp.bfloat16

    is_left = i < n_i // 2
    is_end = (i == 0) | (i == n_i - 1)
    is_inner = (i > 0) & (i < n_i - 1)
    toward = jnp.where(is_left, 1, -1)
    mate = (jnp.where(is_end, i + toward, i - toward), s)
    twin = (n_i - 1 - i, s)

    def when_inner(f):
        pl.when(is_inner)(f)

    def when_end(f):
        pl.when(is_end)(f)

    def mirrored(o):
        return jnp.where(is_left, o, n_i - 1 - o)

    near_far = jnp.where(is_left, n_i - 2, 0)
    barrier = pltpu.get_barrier_semaphore()
    n_bits = n_s.bit_length() - 1

    def greet(semaphore):
        for b in range(n_bits):
            pl.semaphore_signal(semaphore, inc=1, device_id=(i, flip(s, b)), device_id_type=MESH)
        pl.semaphore_signal(semaphore, inc=1, device_id=mate, device_id_type=MESH)

        @pl.when(is_inner)
        def _():
            pl.semaphore_signal(semaphore, inc=1, device_id=twin, device_id_type=MESH)

    def greeted(semaphore):
        pl.semaphore_wait(semaphore, n_bits + 1 + jnp.where(is_inner, 1, 0))

    greet(barrier)
    load_master = [
        pltpu.make_async_copy(
            master_ref.at[:, c * LANES : (c + 1) * LANES], master.at[:, c * LANES : (c + 1) * LANES],
            local_sem.at[3 + steps + c],
        )
        for c in range(chunks)
    ]
    load_rows = [
        pltpu.make_async_copy(rows_ref.at[0, st], rows.at[st, s], local_sem.at[st]) for st in range(steps)
    ]
    load_rest = [
        pltpu.make_async_copy(stream_ref.at[0], stream, local_sem.at[steps]),
        pltpu.make_async_copy(goals_ref.at[0], goals, local_sem.at[1 + steps]),
        pltpu.make_async_copy(moment_ref, moment, local_sem.at[2 + steps]),
    ]
    for copy in [load_master[0], load_rows[0]] + load_master[1:] + load_rows[1:]:
        copy.start()

    def remote(src, dst, send, recv, to):
        return pltpu.make_async_remote_copy(
            src_ref=src, dst_ref=dst, send_sem=send, recv_sem=recv, device_id=to, device_id_type=MESH
        )

    def z_mate(o, c):
        return remote(anchor.at[o, c], anchor.at[o, c], z_send.at[0], z_recv.at[o, c], mate)

    def z_twin(o, c):
        return remote(anchor.at[o, c], anchor.at[o, c], z_send.at[1], z_recv.at[o, c], twin)

    orders = [list(range(1, n_bits)) + [0], list(range(n_bits - 1, 0, -1)) + [0]]
    half = block // 2

    def a_blocks(h, phase):
        found = []
        for m in range(1 << phase):
            at = s
            for q in range(phase):
                if (m >> q) & 1:
                    at = flip(at, orders[h][q])
            found.append(at)
        return found

    def rows_of(which, blocks, band=slice(None)):
        if which < 2:
            return rows.at[which, blocks, band]
        if which == 2:
            return rows_h.at[0, blocks, band]
        wide = pl.multiple_of((mirrored(6 - which) - near_far) * piece, LANES)
        return rows_h.at[1, blocks, band, pl.ds(wide, piece)]

    last = n_bits - 1

    def a_start(which, stage):
        phase = min(stage, last)
        count = 1 << phase
        part = range(count) if stage < last else range((stage - last) * count // 2, (stage - last + 1) * count // 2)
        for m in part:
            for h in range(2):
                block_part = rows_of(which, a_blocks(h, phase)[m], pl.ds(h * half, half))
                remote(
                    block_part, block_part, a_send.at[which], a_recv.at[which, stage],
                    (i, flip(s, orders[h][phase])),
                ).start()

    def a_wait(which, stage):
        count = (1 << stage) if stage < last else (1 << last) // 2
        blocks = rows_of(which, pl.ds(0, count))
        remote(blocks, blocks, a_send.at[which], a_recv.at[which, stage], mate).wait_recv()

    def a_sent(which):
        blocks = rows_of(which, pl.ds(0, n_s - 1))
        remote(blocks, blocks, a_send.at[which], a_recv.at[which, 0], mate).wait_send()

    def a_next(which, phase):
        a_wait(which, phase)
        if phase + 1 < last:
            a_start(which, phase + 1)
        if phase == last - 2:
            a_start(which, last)
        if phase == last - 1:
            a_start(which, last + 1)

    def a_done(which):
        a_wait(which, last)
        a_wait(which, last + 1)

    far = pl.multiple_of(jnp.where(is_left, width - 2 * piece, 0), LANES)

    def lend_rows(st):
        return remote(
            rows.at[st, s, :, pl.ds(far, 2 * piece)], rows_h.at[st, s], ha_send.at[0], ha_recv.at[st], mate
        )

    gains[i] = gain_ref[...].astype(bf16).astype(f32)
    gain_copies = [
        remote(gains.at[i], gains.at[i], g_send.at[0], g_recv.at[0], (lax.rem(i + d, n_i), s))
        for d in range(1, n_i)
    ]
    gain_wait = remote(
        gains.at[pl.ds(0, n_i - 1)], gains.at[pl.ds(0, n_i - 1)], g_send.at[0], g_recv.at[0], mate
    )

    def lower(c):
        def body(j, _):
            at = pl.ds(pl.multiple_of(j * tall, tall), tall)
            anchor[i, c, at, :] = master[at, c * LANES : (c + 1) * LANES].astype(bf16)
            return 0

        load_master[c].wait()
        lax.fori_loop(0, piece // tall, body, 0)

    lower(0)
    load_rows[0].wait()
    greeted(barrier)
    a_start(0, 0)
    for c in range(chunks):
        if c > 0:
            lower(c)
        if c == min(2, chunks - 1):
            pl.when(is_end)(lambda: lend_rows(0).start())
        z_mate(i, c).start()
        pl.when(is_inner)(lambda: z_twin(i, c).start())
    for copy in load_rows[1:]:
        copy.wait()
    pl.when(is_end)(lambda: lend_rows(1).start())
    for copy in load_rest:
        copy.start()
    for k in range(2):
        greet(round_sem.at[k])
        greeted(round_sem.at[k])
    for copy in gain_copies:
        copy.start()
    res[...] = jnp.zeros_like(res)
    for copy in load_rest:
        copy.wait()

    def joined(buffer, at, ds):
        return jnp.concatenate([buffer[at, c, ds, :] for c in range(chunks)], axis=1)

    def project(o, count=chunks):
        def body(k, _):
            start = pl.multiple_of(k * depth, depth)
            wide = pl.multiple_of(o * piece + k * depth, depth)
            part = rows[0, :, :, pl.ds(wide, depth)].reshape(tokens, depth)
            weights = [anchor[o, c, pl.ds(start, depth), :] for c in range(count)]
            res[:, : count * LANES] += jnp.dot(part, jnp.concatenate(weights, axis=1), preferred_element_type=f32)
            return 0

        lax.fori_loop(0, piece // depth, body, 0)

    def arrived(o, c):
        z_mate(o, c).wait_recv()

    held = chunks - 1
    groups = 2

    def fold(value):
        return jnp.sum(value.T, axis=0, keepdims=True)

    def spread(value):
        return jnp.broadcast_to(value, (LANES, LANES)).T

    def tile_at(q):
        return pl.ds(pl.multiple_of(q * LANES, LANES), LANES)

    def lanes_of(c):
        return slice(c * LANES, (c + 1) * LANES)

    def products(st, gain, at, among):
        sums = None
        for c in among:
            r = stream[st, at, lanes_of(c)].astype(f32) + res[at, lanes_of(c)] * scale
            res[at, lanes_of(c)] = r
            weighted = r * gain[:, lanes_of(c)]
            terms = (r * r, weighted * weighted, weighted * goals[st, at, lanes_of(c)].astype(f32))
            sums = terms if sums is None else tuple(a + b for a, b in zip(sums, terms))
        return sums

    def local_stats(st, gain, among, held_sums):
        def body(q, _):
            at = tile_at(q)
            sums = products(st, gain, at, among)
            for k in range(3):
                value = sums[k] + early[k, at, :] if held_sums else sums[k]
                stats[st, 0, k : k + 1, at] = fold(value)
            stats[st, 0, 3:4, at] = jnp.zeros((1, LANES), f32)
            return 0

        lax.fori_loop(0, tiles, body, 0, unroll=True)

    def early_stats(q, _):
        at = tile_at(q)
        sums = products(0, gain_read(), at, range(held))
        for k in range(3):
            early[k, at, :] = sums[k]
        return 0

    def part_copy():
        return remote(part_out, part_in, p_send, p_recv, mate)

    def project_for_end():
        weights = jnp.concatenate([anchor[near_far + k, held] for k in range(2)], axis=0)
        count = n_s // groups
        for g in range(groups):
            part = rows_h[0, g * count : (g + 1) * count].reshape(count * block, 2 * piece)
            part_out[g * count * block : (g + 1) * count * block, :] = jnp.dot(
                part, weights, preferred_element_type=f32
            ).astype(bf16)

    def gain_read():
        return jnp.concatenate([gains[j] for j in range(n_i)], axis=1)

    @when_end
    def _():
        one, two, three = mirrored(1), mirrored(2), mirrored(3)
        a_next(0, 0)
        a_start(1, 0)
        for p in range(1, last):
            a_next(0, p)
        a_done(0)
        project(i)
        for c in range(chunks):
            arrived(one, c)
        project(one)
        a_next(1, 0)
        for c in range(held):
            arrived(two, c)
        project(two, held)
        for p in range(1, last):
            a_next(1, p)
        for c in range(held):
            arrived(three, c)
        project(three, held)
        gain_wait.wait_recv()
        lax.fori_loop(0, tiles, early_stats, 0, unroll=True)
        part_copy().wait_recv()
        res[:, held * LANES :] += part_in[...].astype(f32)
        local_stats(0, gain_read(), (held,), True)

    @when_inner
    def _():
        zero, two, three = mirrored(0), mirrored(2), mirrored(3)

        def from_end(c):
            arrived(zero, c)
            z_twin(zero, c).start()

        def from_far(o, c):
            arrived(o, c)
            if c < held:
                z_mate(o, c).start()

        from_end(0)
        from_far(two, 0)
        a_next(0, 0)
        from_end(1)
        for c in range(1, chunks):
            from_far(two, c)
        from_end(2)
        for p in range(1, last):
            a_next(0, p)
        lend_rows(0).wait_recv()
        a_start(2, 0)
        from_far(three, 0)
        a_next(2, 0)
        a_start(1, 0)
        for c in range(3, chunks):
            from_end(c)
        a_done(0)
        project(i)
        from_far(three, 1)
        project(zero)
        for p in range(1, last):
            a_next(2, p)
        for c in range(2, held):
            from_far(three, c)
        project(two)
        from_far(three, held)
        a_done(2)
        project_for_end()
        part_copy().start()
        project(three)

    def row_stats(st, between=None):
        copies = [
            remote(
                stats.at[st, 0], stats.at[st, d], s_send.at[st], s_recv.at[st],
                (i, lax.rem(s + d, n_s)),
            )
            for d in range(1, n_s)
        ]
        for copy in copies:
            copy.start()
        if between is not None:
            between()
        others = stats.at[st, pl.ds(1, n_s - 1)]
        remote(others, others, s_send.at[st], s_recv.at[st], mate).wait()
        total = stats[st, 0]
        for d in range(1, n_s):
            total = total + stats[st, d]
        inverse = lax.rsqrt(total[0:1] * (1.0 / width) + norm_epsilon)
        pull = inverse * total[1:2] - total[2:3]
        line[0:1, :] = inverse
        line[1:2, :] = inverse * inverse * inverse * pull * (1.0 / width)

    def row_grads(st, gain, among):
        def body(q, totals):
            at = tile_at(q)
            inverse, pull = spread(line[0:1, at]), spread(line[1:2, at])
            found = []
            for c, total in zip(among, totals):
                r = res[at, lanes_of(c)]
                unit = r * inverse
                scaled = gain[:, lanes_of(c)]
                loss = unit * scaled - goals[st, at, lanes_of(c)].astype(f32)
                loss = loss.astype(bf16).astype(f32)
                low = inverse * (loss * scaled) - r * pull
                slope[st, c, at, :] = (low * scale if exact else low).astype(bf16)
                found.append(total + jnp.sum(loss * unit, axis=0, keepdims=True))
            return tuple(found)

        return lax.fori_loop(0, tiles, body, (jnp.zeros((1, LANES), f32),) * len(among), unroll=True)

    def product(part, against):
        grad = lax.dot_general(part, against, (((0,), (0,)), ((), ())), preferred_element_type=f32)
        return grad if exact else grad * scale

    def weight_grad(st, wide, size):
        part = rows[st, :, :, pl.ds(pl.multiple_of(wide, size), size)].reshape(tokens, size)
        return product(part, joined(slope, st, slice(None)))

    def more_rows():
        @when_inner
        def _():
            a_next(1, 0)
            lend_rows(1).wait_recv()
            a_start(3, 0)

    @when_inner
    def _():
        gain_wait.wait_recv()
        local_stats(0, gain_read(), range(chunks), False)

    gain_anchor = gain_read()
    gain = gain_anchor
    row_stats(0, more_rows)
    gain_first = jnp.concatenate(row_grads(0, gain, range(chunks)), axis=1)
    res[...] = jnp.zeros_like(res)

    def lend_slope(st, c):
        return remote(slope.at[st, c], slope_h.at[st, c], r_send.at[0], r_recv.at[st, c], mate)

    @when_end
    def _():
        for c in range(held):
            lend_slope(0, c).start()

    spans = width // span
    per_piece = piece // span

    def place(q):
        return mirrored(q // per_piece), q % per_piece

    def grad_one(q):
        o, j = place(q)
        return weight_grad(0, o * piece + j * span, span)

    def step_one(q, grad, ahead):
        o, j = place(q)
        at = pl.ds(pl.multiple_of(j * span, span), span)
        grads[o, at, :] = grad
        step = (inner_rate * grad) * pl.reciprocal(jnp.abs(grad) + adam_epsilon)
        param = keep * joined(anchor, o, at).astype(f32) - step
        ahead[...] = param.astype(bf16)

    def project_later(q, ahead):
        o, j = place(q)
        wide = pl.multiple_of(o * piece + j * span, span)
        part = rows[1, :, :, pl.ds(wide, span)].reshape(tokens, span)
        res[...] += jnp.dot(part, ahead[...], preferred_element_type=f32)

    def both(t, _):
        for k in (2, 3):

            @pl.when(2 * t == k * per_piece)
            def _():
                arrived(mirrored(k), held)

        even = grad_one(2 * t)
        odd = grad_one(2 * t + 1)
        step_one(2 * t, even, ahead_a)
        project_later(2 * t, ahead_a)
        step_one(2 * t + 1, odd, ahead_b)
        project_later(2 * t + 1, ahead_b)
        return 0

    def one_alone(q, _):
        step_one(q, grad_one(q), later.at[q])
        return 0

    group = 2 if per_piece % 2 == 0 else 1

    def later_alone(g, _):
        o, j = place(g * group)
        wide = pl.multiple_of(o * piece + j * span, span)
        part = rows[1, :, :, pl.ds(wide, group * span)].reshape(tokens, group * span)
        weights = jnp.concatenate([later[g * group + k] for k in range(group)], axis=0)
        res[...] += jnp.dot(part, weights, preferred_element_type=f32)
        return 0

    @when_end
    def _():
        a_done(1)
        lax.fori_loop(0, spans // 2, both, 0)

    @when_inner
    def _():
        lax.fori_loop(0, spans, one_alone, 0)
        z_mate(mirrored(2), held).start()
        z_mate(mirrored(3), held).start()
        for p in range(1, last):
            a_next(1, p)
        a_next(3, 0)
        a_done(1)
        lax.fori_loop(0, spans // group, later_alone, 0)
        for p in range(1, last):
            a_next(3, p)

    gain_step = first_update(gain_first)
    gain = gain_anchor - inner_rate * gain_step

    local_stats(1, gain, range(chunks), False)
    row_stats(1)
    is_even = lax.rem(s, 2) == 0
    gain_second = row_grads(1, gain, (0,))

    @pl.when(is_end & is_even)
    def _():
        lend_slope(1, 0).start()

    gain_second = jnp.concatenate(gain_second + row_grads(1, gain, range(1, chunks)), axis=1)
    when_inner(lambda: a_start(4, 0))
    gain_move = inner_rate * (gain_step + second_update(gain_first, gain_second))
    for j in range(n_i):
        gain_out[j] = gain_move[:, j * own : (j + 1) * own]

    gain_moves = [
        remote(
            gain_out.at[lax.rem(i + d, n_i)], gain_in.at[d], g_send.at[1], g_recv.at[1],
            (lax.rem(i + d, n_i), s),
        )
        for d in range(1, n_i)
    ]
    for copy in gain_moves:
        copy.start()

    def move(o, first=0, until=piece // tall):
        def body(j, _):
            at = pl.ds(pl.multiple_of(j * tall, tall), tall)
            grad = weight_grad(1, o * piece + j * tall, tall)
            grads[o, at, :] = outer_sum(grads[o, at, :], grad)
            return 0

        lax.fori_loop(first, until, body, 0)

    def give(slot, c):
        return remote(outgo.at[slot, c], from_mate.at[c], e_send.at[0], e_recv.at[c], mate)

    def cross(slot, c, at=slice(None)):
        return remote(
            outgo.at[slot, c, at], from_twin.at[slot, c, at], m_send.at[0], m_recv.at[slot, c], twin
        )

    def pack(slot, c, o, *others):
        lanes = slice(c * LANES, (c + 1) * LANES)

        def body(j, _):
            at = pl.ds(pl.multiple_of(j * tall, tall), tall)
            total = grads[o, at, lanes]
            for other in others:
                total = total + other[at, :].astype(f32)
            outgo[slot, c, at, :] = total.astype(bf16)
            return 0

        lax.fori_loop(0, piece // tall, body, 0)

    def finish(c, o, *others):
        lanes = slice(c * LANES, (c + 1) * LANES)

        def body(j, _):
            at = pl.ds(pl.multiple_of(j * tall, tall), tall)
            total = grads[o, at, lanes]
            for other in others:
                total = total + other[at, :].astype(f32)
            outer = master[at, lanes]
            pseudo = total * (1.0 / n_i) + (1.0 - keep * keep) * outer.astype(bf16).astype(f32)
            velocity = outer_momentum * moment[at, lanes] + pseudo
            velocity_ref[at, lanes] = velocity
            updated_ref[at, lanes] = outer - outer_rate * (pseudo + outer_momentum * velocity)
            return 0

        lax.fori_loop(0, piece // tall, body, 0)
    @when_end
    def _():
        o = mirrored(1)
        parts = piece // tall
        wait_parts = parts - 1
        move(o, 0, wait_parts)

        @pl.when(jnp.logical_not(is_even))
        def _():
            lend_slope(1, 0).start()

        move(o, wait_parts, parts)
        for c in range(chunks):
            pack(0, c, o)
        for c in range(1, chunks):
            lend_slope(1, c).start()
            if c == held - 1:
                lend_slope(0, held).start()
        for c in range(chunks):
            give(0, c).start()
        o = mirrored(0)
        move(o)
        for c in range(chunks):
            give(0, c).wait_recv()
            finish(c, o, from_mate.at[c])

    def help_end(slot, c, o):
        base = (o - near_far) * piece
        lanes = slice(c * LANES, (c + 1) * LANES)

        def body(j, _):
            at = pl.ds(pl.multiple_of(j * tall, tall), tall)
            wide = pl.ds(pl.multiple_of(base + j * tall, tall), tall)
            pair = [
                product(rows_h[st, :, :, wide].reshape(tokens, tall), slope_h[st, c]) for st in range(steps)
            ]
            outgo[slot, c, at, :] = (grads[o, at, lanes] + outer_sum(*pair)).astype(bf16)
            cross(slot, c, at).start()
            return 0

        lax.fori_loop(0, piece // tall, body, 0)

    @when_inner
    def _():
        def help_and_cross(slot, c):
            help_end(slot, c, mirrored(3 - slot))

        def forward(c):
            cross(0, c).wait_recv()
            pack(2, c, mirrored(0), from_twin.at[0, c])
            give(2, c).start()

        move(mirrored(3))
        a_done(3)

        def far_sum(c):
            lend_slope(0, c).wait_recv()
            lend_slope(1, c).wait_recv()
            help_and_cross(0, c)

        phases = list(range(last))
        for c in range(held):
            far_sum(c)
            if c == 0:
                a_next(4, phases.pop(0))
                move(mirrored(0))
            if c == 1:
                for p in phases:
                    a_next(4, p)
                move(mirrored(2))
        forward(0)
        a_done(4)
        help_and_cross(1, 0)
        far_sum(held)
        for c in range(1, chunks):
            if c < held:
                forward(c)
            help_and_cross(1, c)
            if c == 1:
                move(mirrored(1))
        forward(held)
        for c in range(chunks):
            give(2, c).wait_recv()
            cross(1, c).wait_recv()
            finish(c, mirrored(1), from_mate.at[c], from_twin.at[1, c])

    moved_gains = gain_in.at[pl.ds(1, n_i - 1)]
    remote(moved_gains, moved_gains, g_send.at[1], g_recv.at[1], mate).wait()
    gain_total = gain_out[i]
    for d in range(1, n_i):
        gain_total = gain_total + gain_in[d]
    gain_pseudo = gain_total * (1.0 / n_i)
    gain_velocity = outer_momentum * gain_moment_ref[...] + gain_pseudo
    gain_velocity_ref[...] = gain_velocity
    gain_updated_ref[...] = gain_ref[...] - outer_rate * (gain_pseudo + outer_momentum * gain_velocity)

    def sent_pieces(way, count):
        pieces = anchor.at[pl.ds(0, count)]
        remote(pieces, pieces, z_send.at[way], z_recv.at[0, 0], mate).wait_send()

    @when_end
    def _():
        lent = rows_h.at[pl.ds(0, steps), 0]
        remote(lent, lent, ha_send.at[0], ha_recv.at[0], mate).wait_send()
        sent_pieces(0, 1)
        remote(slope, slope, r_send.at[0], r_recv.at[0, 0], mate).wait_send()
        remote(from_mate, from_mate, e_send.at[0], e_recv.at[0], mate).wait_send()

    @when_inner
    def _():
        remote(from_twin, from_twin, m_send.at[0], m_recv.at[0, 0], twin).wait_send()
        remote(from_mate, from_mate, e_send.at[0], e_recv.at[0], mate).wait_send()
        part_copy().wait_send()
        for which in (2, 3, 4):
            a_sent(which)
        sent_pieces(0, 3)
        sent_pieces(1, 2)

    gain_wait.wait_send()
    a_sent(0)
    a_sent(1)


def write_out(*refs):
    count = len(refs) // 2
    sem = refs[-1]
    copies = [pltpu.make_async_copy(refs[k], refs[count + k], sem.at[k]) for k in range(count)]
    for copy in copies:
        copy.start()
    for copy in copies:
        copy.wait()


def per_device(weight_master, gain_master, weight_moment, gain_moment, attended, stream, targets):
    n_i, n_s = lax.axis_size("island"), lax.axis_size("shard")
    _, steps, block, width = attended.shape
    _, _, tokens, cols = stream.shape
    piece = weight_master.shape[0]
    own = gain_master.shape[0]
    f32, bf16 = jnp.float32, jnp.bfloat16
    chunks = cols // LANES
    arrays = [
        ((piece, cols), f32),
        ((piece, cols), f32),
        ((steps, n_s, block, width), bf16),
        ((steps, n_s, block, 2 * piece), bf16),
        ((n_i, chunks, piece, LANES), bf16),
        ((min(512, piece), cols), bf16),
        ((min(512, piece), cols), bf16),
        ((width // min(512, piece), min(512, piece), cols), bf16),
        ((n_i, piece, cols), f32),
        ((tokens, cols), f32),
        ((steps, chunks, tokens, LANES), bf16),
        ((steps, chunks, tokens, LANES), bf16),
        ((steps, tokens, cols), bf16),
        ((steps, tokens, cols), bf16),
        ((3, chunks, piece, LANES), bf16),
        ((chunks, piece, LANES), bf16),
        ((2, chunks, piece, LANES), bf16),
        ((tokens, LANES), bf16),
        ((tokens, LANES), bf16),
        ((3, tokens, LANES), f32),
        ((steps, n_s, 4, tokens), f32),
        ((2, tokens), f32),
        ((n_i, 1, own), f32),
        ((n_i, 1, own), f32),
        ((n_i, 1, own), f32),
    ]
    held = sum(math.prod(shape) * jnp.dtype(kind).itemsize for shape, kind in arrays)
    if n_i != 4 or steps != 2 or own % LANES or chunks < 2 or block % 32 or n_s < 8 or held > 60e6:
        return general_device(weight_master, gain_master, weight_moment, gain_moment, attended, stream, targets)
    any_space = pl.BlockSpec(memory_space=pl.ANY)
    vmem = pl.BlockSpec(memory_space=pltpu.VMEM)
    dma = pltpu.SemaphoreType.DMA
    outs = ((piece, cols), (1, own), (piece, cols), (1, own))
    results = pl.pallas_call(
        functools.partial(kernel, n_i, n_s),
        out_shape=tuple(pltpu.VMEM(shape, f32) for shape in outs),
        in_specs=[any_space, vmem, any_space, vmem, any_space, any_space, any_space],
        out_specs=(vmem, vmem, vmem, vmem),
        scratch_shapes=[pltpu.VMEM(shape, kind) for shape, kind in arrays]
        + [
            pltpu.SemaphoreType.REGULAR((2,)),
            dma((3 + steps + chunks,)),
            dma((2,)),
            dma((n_i, chunks)),
            dma((5,)),
            dma((5, n_s.bit_length())),
            dma(()),
            dma(()),
            dma((1,)),
            dma((steps,)),
            dma((steps,)),
            dma((steps,)),
            dma((2,)),
            dma((2,)),
            dma((1,)),
            dma((steps, chunks)),
            dma((1,)),
            dma((chunks,)),
            dma((1,)),
            dma((2, chunks)),
        ],
        compiler_params=pltpu.CompilerParams(
            collective_id=0, has_side_effects=True, vmem_limit_bytes=58 << 20
        ),
    )(weight_master, gain_master[None], weight_moment, gain_moment[None], attended, stream, targets)
    results = [pltpu.with_memory_space_constraint(x, pltpu.VMEM) for x in results]
    updated, gain_updated, velocity, gain_velocity = pl.pallas_call(
        write_out,
        out_shape=tuple(jax.ShapeDtypeStruct(shape, f32) for shape in outs),
        in_specs=[vmem] * 4,
        out_specs=(any_space,) * 4,
        scratch_shapes=[dma((4,))],
        compiler_params=pltpu.CompilerParams(vmem_limit_bytes=1 << 20),
    )(*results)
    return (updated, gain_updated[0], velocity, gain_velocity[0])


def solution(mesh):
    placed = (
        P("island", "shard"),
        P(("shard", "island")),
        P("island", "shard"),
        P(("shard", "island")),
        P("island", None, "shard", None),
        P("island", None, None, "shard"),
        P("island", None, None, "shard"),
    )
    return jax.shard_map(
        per_device,
        mesh=mesh,
        in_specs=placed,
        out_specs=(
            P("island", "shard"),
            P(("shard", "island")),
            P("island", "shard"),
            P(("shard", "island")),
        ),
        check_vma=False,
    )
```

```python
import functools
import math

import jax
import jax.numpy as jnp
from jax import lax
from jax.experimental import pallas as pl
from jax.experimental.pallas import tpu as pltpu
from jax.sharding import PartitionSpec as P

norm_epsilon = 1e-05
inner_rate = 0.05
beta_one = 0.9
beta_two = 0.95
adam_epsilon = 0.3
decay_rate = 0.1
outer_rate = 0.7
outer_momentum = 0.9

MESH = pl.DeviceIdType.MESH
LANES = 128
keep = 1.0 - inner_rate * decay_rate


def flip(index, bit):
    size = 1 << bit
    return index + size * (1 - 2 * (lax.div(index, size) % 2))


def first_update(grad):
    return grad / (jnp.abs(grad) + adam_epsilon)


def second_update(earlier, grad):
    first = (beta_one * (1.0 - beta_one)) * earlier + (1.0 - beta_one) * grad
    second = (beta_two * (1.0 - beta_two)) * earlier * earlier + (1.0 - beta_two) * grad * grad
    first_hat = first * (1.0 / (1.0 - beta_one**2))
    second_hat = second * (1.0 / (1.0 - beta_two**2))
    return first_hat / (jnp.sqrt(second_hat) + adam_epsilon)


def general_kernel(
    n_i, n_s, low_ref, gain_ref, rows_ref, stream_ref, goals_ref, total_ref, gain_total_ref,
    rows, anchor, later, grads, res, slope_low, stream, goals, from_left, from_right,
    stats, line, gains, gain_moves,
    local_sem, z_send, z_recv, a_send, a_recv, s_send, s_recv, g_send, g_recv, r_send, r_recv,
):
    i = lax.axis_index("island")
    s = lax.axis_index("shard")
    steps, _, block, width = rows.shape
    piece, cols = low_ref.shape
    tokens = n_s * block
    tiles = tokens // LANES
    scale = width ** (-0.5)
    depth = min(512, piece)
    tall = min(256, piece)

    barrier = pltpu.get_barrier_semaphore()
    for d in range(1, n_i):
        pl.semaphore_signal(barrier, inc=1, device_id=(lax.rem(i + d, n_i), s), device_id_type=MESH)
    for d in range(1, n_s):
        pl.semaphore_signal(barrier, inc=1, device_id=(i, lax.rem(s + d, n_s)), device_id_type=MESH)

    locals_ = [pltpu.make_async_copy(low_ref, anchor.at[i], local_sem.at[0])]
    for st in range(steps):
        locals_.append(pltpu.make_async_copy(rows_ref.at[0, st], rows.at[st, s], local_sem.at[1 + st]))
    locals_.append(pltpu.make_async_copy(stream_ref.at[0], stream, local_sem.at[1 + steps]))
    locals_.append(pltpu.make_async_copy(goals_ref.at[0], goals, local_sem.at[2 + steps]))
    for copy in locals_:
        copy.start()
    pl.semaphore_wait(barrier, n_i - 1 + n_s - 1)

    def remote(src, dst, send, recv, to):
        return pltpu.make_async_remote_copy(
            src_ref=src, dst_ref=dst, send_sem=send, recv_sem=recv, device_id=to, device_id_type=MESH
        )

    right, left = (lax.rem(i + 1, n_i), s), (lax.rem(i + n_i - 1, n_i), s)

    def z_copy(way, t, at):
        return remote(
            anchor.at[at], anchor.at[at], z_send.at[way, t], z_recv.at[way, t], right if way == 0 else left
        )

    def z_start(t):
        @pl.when((i < n_i - 1) & (i - t >= 0))
        def _():
            z_copy(0, t, i - t).start()

        @pl.when((i > 0) & (i + t <= n_i - 1))
        def _():
            z_copy(1, t, i + t).start()

    def z_wait(t):
        @pl.when(i - 1 - t >= 0)
        def _():
            z_copy(0, t, i - 1 - t).wait_recv()

        @pl.when(i + 1 + t <= n_i - 1)
        def _():
            z_copy(1, t, i + 1 + t).wait_recv()

    n_bits = n_s.bit_length() - 1
    orders = [list(range(1, n_bits)) + [0], list(range(n_bits - 1, 0, -1)) + [0]]

    def a_blocks(st, phase):
        order = orders[st % 2]
        found = []
        for m in range(1 << phase):
            at = s
            for q in range(phase):
                if (m >> q) & 1:
                    at = flip(at, order[q])
            found.append(at)
        return found

    def a_copy(st, phase, m, at):
        slot = (1 << phase) - 1 + m
        return remote(
            rows.at[st, at], rows.at[st, at], a_send.at[st, slot], a_recv.at[st, slot],
            (i, flip(s, orders[st % 2][phase])),
        )

    def a_start(phase):
        for st in range(steps):
            for m, at in enumerate(a_blocks(st, phase)):
                a_copy(st, phase, m, at).start()

    def a_wait(phase):
        for st in range(steps):
            for m, at in enumerate(a_blocks(st, phase)):
                a_copy(st, phase, m, flip(at, orders[st % 2][phase])).wait_recv()

    def to_islands(buffer, which):
        return [
            remote(
                buffer.at[0], buffer.at[d], g_send.at[which, d], g_recv.at[which, d],
                (lax.rem(i + d, n_i), s),
            )
            for d in range(1, n_i)
        ]

    locals_[0].wait()
    z_start(0)
    for copy in locals_[1 : 1 + steps]:
        copy.wait()
    a_start(0)
    gains[0] = gain_ref[...]
    gain_in = to_islands(gains, 0)
    for copy in gain_in:
        copy.start()
    res[...] = jnp.zeros_like(res)
    for copy in locals_[1 + steps :]:
        copy.wait()

    def project(st, weights, at):
        def body(k, _):
            start = pl.multiple_of(k * depth, depth)
            wide = pl.multiple_of(at * piece + k * depth, depth)
            part = rows[st, :, :, pl.ds(wide, depth)].reshape(tokens, depth)
            res[...] += jnp.dot(part, weights[at, pl.ds(start, depth), :], preferred_element_type=jnp.float32)
            return 0

        lax.fori_loop(0, piece // depth, body, 0)

    def project_arrived(t):
        @pl.when(i - 1 - t >= 0)
        def _():
            project(0, anchor, i - 1 - t)

        @pl.when(i + 1 + t <= n_i - 1)
        def _():
            project(0, anchor, i + 1 + t)

    events = [(2.0 * t + 2.6, "z", t) for t in range(n_i - 1)]
    events += [(2.0 * ((2 << p) - 1), "a", p) for p in range(n_bits - 1)]
    last = events[-1][0] if n_bits > 1 else 0.0
    events.append((last + 0.1, "a", n_bits - 1))
    gathered, ready = False, []
    for _, kind, at in sorted(events):
        if kind == "a":
            a_wait(at)
            if at + 1 < n_bits:
                a_start(at + 1)
            else:
                gathered = True
                project(0, anchor, i)
                for t in ready:
                    project_arrived(t)
        else:
            z_wait(at)
            if at + 1 < n_i - 1:
                z_start(at + 1)
            if gathered:
                project_arrived(at)
            else:
                ready.append(at)

    for copy in gain_in:
        copy.wait()
    gain_anchor = gains[0]
    for d in range(1, n_i):
        gain_anchor = gain_anchor + gains[d]
    gain = gain_anchor

    def fold(value):
        total = value[:, :LANES]
        for c in range(1, cols // LANES):
            total = total + value[:, c * LANES : (c + 1) * LANES]
        return jnp.sum(total.T, axis=0, keepdims=True)

    def spread(value):
        square = jnp.broadcast_to(value, (LANES, LANES)).T
        return jnp.concatenate([square] * (cols // LANES), axis=1)

    def row_stats(st, gain):
        def body(q, _):
            at = pl.ds(pl.multiple_of(q * LANES, LANES), LANES)
            r = stream[st, at, :].astype(jnp.float32) + res[at, :] * scale
            res[at, :] = r
            weighted = r * gain
            stats[st, 0, 0:1, at] = fold(r * r)
            stats[st, 0, 1:2, at] = fold(weighted * weighted)
            stats[st, 0, 2:3, at] = fold(weighted * goals[st, at, :].astype(jnp.float32))
            stats[st, 0, 3:4, at] = jnp.zeros((1, LANES), jnp.float32)
            return 0

        lax.fori_loop(0, tiles, body, 0)
        copies = [
            remote(
                stats.at[st, 0], stats.at[st, d], s_send.at[st, d], s_recv.at[st, d],
                (i, lax.rem(s + d, n_s)),
            )
            for d in range(1, n_s)
        ]
        for copy in copies:
            copy.start()
        for copy in copies:
            copy.wait()
        total = stats[st, 0]
        for d in range(1, n_s):
            total = total + stats[st, d]
        inverse = lax.rsqrt(total[0:1] * (1.0 / width) + norm_epsilon)
        slope = inverse * total[1:2] - total[2:3]
        line[0:1, :] = inverse
        line[1:2, :] = inverse * inverse * inverse * slope * (1.0 / width)

    def row_grads(st, gain):
        def body(q, total):
            at = pl.ds(pl.multiple_of(q * LANES, LANES), LANES)
            inverse, pull = spread(line[0:1, at]), spread(line[1:2, at])
            r = res[at, :]
            unit = r * inverse
            loss = unit * gain - goals[st, at, :].astype(jnp.float32)
            loss = loss.astype(jnp.bfloat16).astype(jnp.float32)
            slope_low[at, :] = (inverse * (loss * gain) - r * pull).astype(jnp.bfloat16)
            return total + jnp.sum(loss * unit, axis=0, keepdims=True)

        return lax.fori_loop(0, tiles, body, jnp.zeros((1, cols), jnp.float32))

    def weight_grad(st, wide):
        part = rows[st, :, :, pl.ds(pl.multiple_of(wide, tall), tall)].reshape(tokens, tall)
        return (
            lax.dot_general(
                part, slope_low[...], (((0,), (0,)), ((), ())), preferred_element_type=jnp.float32
            )
            * scale
        )

    row_stats(0, gain)
    gain_first = row_grads(0, gain)
    per_piece = piece // tall

    def step_one(q, _):
        o, j = q // per_piece, q % per_piece
        at = pl.ds(pl.multiple_of(j * tall, tall), tall)
        grad = weight_grad(0, q * tall)
        grads[o, at, :] = grad
        param = keep * anchor[o, at, :].astype(jnp.float32) - inner_rate * first_update(grad)
        later[o, at, :] = param.astype(jnp.bfloat16)
        return 0

    lax.fori_loop(0, n_i * per_piece, step_one, 0)
    gain_step = first_update(gain_first)
    gain = gain_anchor - inner_rate * gain_step

    res[...] = jnp.zeros_like(res)

    def project_later(at, _):
        project(1, later, at)
        return 0

    lax.fori_loop(0, n_i, project_later, 0)
    row_stats(1, gain)
    gain_second = row_grads(1, gain)
    gain_moves[0] = inner_rate * (gain_step + second_update(gain_first, gain_second))
    gain_out = to_islands(gain_moves, 1)
    for copy in gain_out:
        copy.start()

    def to_right(k):
        at = n_i - 1 - k
        return remote(later.at[at], from_left.at[k], r_send.at[0, k], r_recv.at[0, k], right)

    def to_left(k):
        return remote(later.at[k], from_right.at[k], r_send.at[1, k], r_recv.at[1, k], left)

    early = 1 - lax.div(2 * i, n_i)

    def owner_piece(q, _):
        o = q + early * (n_i - 1 - 2 * q)

        def step_two(j, _):
            at = pl.ds(pl.multiple_of(j * tall, tall), tall)
            grad = weight_grad(1, o * piece + j * tall)
            earlier = grads[o, at, :]
            moved = (1.0 - keep * keep) * anchor[o, at, :].astype(jnp.float32) + inner_rate * (
                keep * first_update(earlier) + second_update(earlier, grad)
            )
            grads[o, at, :] = moved
            later[o, at, :] = moved.astype(jnp.bfloat16)
            return 0

        lax.fori_loop(0, per_piece, step_two, 0)

        @pl.when((i == 0) & (o > 0))
        def _():
            to_right(n_i - 1 - o).start()

        @pl.when((i == n_i - 1) & (o < n_i - 1))
        def _():
            to_left(o).start()

        return 0

    lax.fori_loop(0, n_i, owner_piece, 0)

    def add(o, arrived, k):
        def body(j, _):
            at = pl.ds(pl.multiple_of(j * tall, tall), tall)
            later[o, at, :] = (grads[o, at, :] + arrived[k, at, :].astype(jnp.float32)).astype(jnp.bfloat16)
            return 0

        lax.fori_loop(0, per_piece, body, 0)

    for t in range(n_i - 1):
        k_right = t - i
        k_left = t - (n_i - 1 - i)

        @pl.when((i > 0) & (k_right >= 0) & (k_right < n_i - 1 - i))
        def _():
            to_right(k_right).wait_recv()
            add(n_i - 1 - k_right, from_left, k_right)
            to_right(k_right).start()

        @pl.when((i < n_i - 1) & (k_left >= 0) & (k_left < i))
        def _():
            to_left(k_left).wait_recv()
            add(k_left, from_right, k_left)
            to_left(k_left).start()

    for copy in gain_out:
        copy.wait()
    gain_total = gain_moves[0]
    for d in range(1, n_i):
        gain_total = gain_total + gain_moves[d]
    gain_total_ref[...] = gain_total

    total_ref[...] = grads[i]

    @pl.when(i > 0)
    def _():
        k = n_i - 1 - i
        to_right(k).wait_recv()
        total_ref[...] += from_left[k].astype(jnp.float32)

    @pl.when(i < n_i - 1)
    def _():
        to_left(i).wait_recv()
        total_ref[...] += from_right[i].astype(jnp.float32)

    for k in range(n_i - 1):

        @pl.when(k < n_i - 1 - i)
        def _(k=k):
            to_right(k).wait_send()

        @pl.when(k < i)
        def _(k=k):
            to_left(k).wait_send()

        @pl.when((i < n_i - 1) & (i - k >= 0))
        def _(k=k):
            z_copy(0, k, i - k).wait_send()

        @pl.when((i > 0) & (i + k <= n_i - 1))
        def _(k=k):
            z_copy(1, k, i + k).wait_send()

    for phase in range(n_bits):
        for st in range(steps):
            for m, at in enumerate(a_blocks(st, phase)):
                a_copy(st, phase, m, at).wait_send()


def general_device(weight_master, gain_master, weight_moment, gain_moment, attended, stream, targets):
    n_i, n_s = lax.axis_size("island"), lax.axis_size("shard")
    _, steps, block, width = attended.shape
    _, _, tokens, cols = stream.shape
    piece = weight_master.shape[0]
    own = gain_master.shape[0]
    offset = lax.axis_index("island") * own
    low = weight_master.astype(jnp.bfloat16)
    gain_low = gain_master.astype(jnp.bfloat16).astype(jnp.float32)
    gain_row = lax.dynamic_update_slice(jnp.zeros((1, cols), jnp.float32), gain_low[None], (0, offset))
    any_space = pl.BlockSpec(memory_space=pl.ANY)
    vmem = pl.BlockSpec(memory_space=pltpu.VMEM)
    f32, bf16 = jnp.float32, jnp.bfloat16
    dma = pltpu.SemaphoreType.DMA
    weight_summed, gain_summed = pl.pallas_call(
        functools.partial(general_kernel, n_i, n_s),
        out_shape=(
            jax.ShapeDtypeStruct((piece, cols), f32),
            jax.ShapeDtypeStruct((1, cols), f32),
        ),
        in_specs=[any_space, vmem, any_space, any_space, any_space],
        out_specs=(vmem, vmem),
        scratch_shapes=[
            pltpu.VMEM((steps, n_s, block, width), bf16),
            pltpu.VMEM((n_i, piece, cols), bf16),
            pltpu.VMEM((n_i, piece, cols), bf16),
            pltpu.VMEM((n_i, piece, cols), f32),
            pltpu.VMEM((tokens, cols), f32),
            pltpu.VMEM((tokens, cols), bf16),
            pltpu.VMEM((steps, tokens, cols), bf16),
            pltpu.VMEM((steps, tokens, cols), bf16),
            pltpu.VMEM((n_i - 1, piece, cols), bf16),
            pltpu.VMEM((n_i - 1, piece, cols), bf16),
            pltpu.VMEM((steps, n_s, 4, tokens), f32),
            pltpu.VMEM((2, tokens), f32),
            pltpu.VMEM((n_i, 1, cols), f32),
            pltpu.VMEM((n_i, 1, cols), f32),
            dma((3 + steps,)),
            dma((2, n_i - 1)),
            dma((2, n_i - 1)),
            dma((steps, n_s - 1)),
            dma((steps, n_s - 1)),
            dma((steps, n_s)),
            dma((steps, n_s)),
            dma((2, n_i)),
            dma((2, n_i)),
            dma((2, n_i - 1)),
            dma((2, n_i - 1)),
        ],
        compiler_params=pltpu.CompilerParams(
            collective_id=0, has_side_effects=True, vmem_limit_bytes=67043328
        ),
    )(low, gain_row, attended, stream, targets)
    weight_pseudo = weight_summed / n_i
    gain_pseudo = lax.dynamic_slice(gain_summed, (0, offset), (1, own))[0] / n_i
    weight_velocity = outer_momentum * weight_moment + weight_pseudo
    gain_velocity = outer_momentum * gain_moment + gain_pseudo
    weight_updated = weight_master - outer_rate * (weight_pseudo + outer_momentum * weight_velocity)
    gain_updated = gain_master - outer_rate * (gain_pseudo + outer_momentum * gain_velocity)
    return (weight_updated, gain_updated, weight_velocity, gain_velocity)


def outer_sum(grad_one, grad_two):
    first = (inner_rate * beta_one * (1.0 - beta_one) / (1.0 - beta_one**2)) * grad_one + (
        inner_rate * (1.0 - beta_one) / (1.0 - beta_one**2)
    ) * grad_two
    second = (beta_two * (1.0 - beta_two) / (1.0 - beta_two**2)) * (grad_one * grad_one) + (
        (1.0 - beta_two) / (1.0 - beta_two**2)
    ) * (grad_two * grad_two)
    root = second * lax.rsqrt(jnp.maximum(second, 1e-30)) + adam_epsilon
    size = jnp.abs(grad_one) + adam_epsilon
    return ((inner_rate * keep) * grad_one * root + first * size) * pl.reciprocal(root * size)


def kernel(
    n_i, n_s, master_ref, gain_ref, moment_ref, gain_moment_ref, rows_ref, stream_ref, goals_ref,
    updated_ref, gain_updated_ref, velocity_ref, gain_velocity_ref,
    master, moment, rows, rows_h, anchor, ahead_a, ahead_b, later, grads, res, slope, slope_h, stream, goals,
    outgo, from_mate, from_twin, part_out, part_in, early, stats, line, gains, gain_out, gain_in,
    round_sem, local_sem, z_send, z_recv, a_send, a_recv, p_send, p_recv, ha_send, ha_recv,
    s_send, s_recv, g_send, g_recv, r_send, r_recv, e_send, e_recv, m_send, m_recv,
):
    i = lax.axis_index("island")
    s = lax.axis_index("shard")
    steps, _, block, width = rows.shape
    _, chunks, piece, _ = anchor.shape
    cols = chunks * LANES
    own = gains.shape[2]
    tokens = n_s * block
    tiles = tokens // LANES
    scale = width ** (-0.5)
    exact = math.frexp(scale)[0] == 0.5
    depth = min(1024, piece)
    tall = min(256, piece)
    span = min(512, piece)
    f32, bf16 = jnp.float32, jnp.bfloat16

    is_left = i < n_i // 2
    is_end = (i == 0) | (i == n_i - 1)
    is_inner = (i > 0) & (i < n_i - 1)
    toward = jnp.where(is_left, 1, -1)
    mate = (jnp.where(is_end, i + toward, i - toward), s)
    twin = (n_i - 1 - i, s)

    def when_inner(f):
        pl.when(is_inner)(f)

    def when_end(f):
        pl.when(is_end)(f)

    def mirrored(o):
        return jnp.where(is_left, o, n_i - 1 - o)

    near_far = jnp.where(is_left, n_i - 2, 0)
    barrier = pltpu.get_barrier_semaphore()
    n_bits = n_s.bit_length() - 1

    def greet(semaphore):
        for b in range(n_bits):
            pl.semaphore_signal(semaphore, inc=1, device_id=(i, flip(s, b)), device_id_type=MESH)
        pl.semaphore_signal(semaphore, inc=1, device_id=mate, device_id_type=MESH)

        @pl.when(is_inner)
        def _():
            pl.semaphore_signal(semaphore, inc=1, device_id=twin, device_id_type=MESH)

    def greeted(semaphore):
        pl.semaphore_wait(semaphore, n_bits + 1 + jnp.where(is_inner, 1, 0))

    greet(barrier)
    load_master = [
        pltpu.make_async_copy(
            master_ref.at[:, c * LANES : (c + 1) * LANES], master.at[:, c * LANES : (c + 1) * LANES],
            local_sem.at[3 + steps + c],
        )
        for c in range(chunks)
    ]
    load_rows = [
        pltpu.make_async_copy(rows_ref.at[0, st], rows.at[st, s], local_sem.at[st]) for st in range(steps)
    ]
    load_rest = [
        pltpu.make_async_copy(stream_ref.at[0], stream, local_sem.at[steps]),
        pltpu.make_async_copy(goals_ref.at[0], goals, local_sem.at[1 + steps]),
        pltpu.make_async_copy(moment_ref, moment, local_sem.at[2 + steps]),
    ]
    for copy in [load_master[0], load_rows[0]] + load_master[1:] + load_rows[1:]:
        copy.start()

    def remote(src, dst, send, recv, to):
        return pltpu.make_async_remote_copy(
            src_ref=src, dst_ref=dst, send_sem=send, recv_sem=recv, device_id=to, device_id_type=MESH
        )

    def z_mate(o, c):
        return remote(anchor.at[o, c], anchor.at[o, c], z_send.at[0], z_recv.at[o, c], mate)

    def z_twin(o, c):
        return remote(anchor.at[o, c], anchor.at[o, c], z_send.at[1], z_recv.at[o, c], twin)

    orders = [list(range(1, n_bits)) + [0], list(range(n_bits - 1, 0, -1)) + [0]]
    half = block // 2

    def a_blocks(h, phase):
        found = []
        for m in range(1 << phase):
            at = s
            for q in range(phase):
                if (m >> q) & 1:
                    at = flip(at, orders[h][q])
            found.append(at)
        return found

    def rows_of(which, blocks, band=slice(None)):
        if which < 2:
            return rows.at[which, blocks, band]
        if which == 2:
            return rows_h.at[0, blocks, band]
        wide = pl.multiple_of((mirrored(6 - which) - near_far) * piece, LANES)
        return rows_h.at[1, blocks, band, pl.ds(wide, piece)]

    last = n_bits - 1

    def a_start(which, stage):
        phase = min(stage, last)
        count = 1 << phase
        part = range(count) if stage < last else range((stage - last) * count // 2, (stage - last + 1) * count // 2)
        for m in part:
            for h in range(2):
                block_part = rows_of(which, a_blocks(h, phase)[m], pl.ds(h * half, half))
                remote(
                    block_part, block_part, a_send.at[which], a_recv.at[which, stage],
                    (i, flip(s, orders[h][phase])),
                ).start()

    def a_wait(which, stage):
        count = (1 << stage) if stage < last else (1 << last) // 2
        blocks = rows_of(which, pl.ds(0, count))
        remote(blocks, blocks, a_send.at[which], a_recv.at[which, stage], mate).wait_recv()

    def a_sent(which):
        blocks = rows_of(which, pl.ds(0, n_s - 1))
        remote(blocks, blocks, a_send.at[which], a_recv.at[which, 0], mate).wait_send()

    def a_next(which, phase):
        a_wait(which, phase)
        if phase + 1 < last:
            a_start(which, phase + 1)
        if phase == last - 2:
            a_start(which, last)
        if phase == last - 1:
            a_start(which, last + 1)

    def a_done(which):
        a_wait(which, last)
        a_wait(which, last + 1)

    far = pl.multiple_of(jnp.where(is_left, width - 2 * piece, 0), LANES)

    def lend_rows(st):
        return remote(
            rows.at[st, s, :, pl.ds(far, 2 * piece)], rows_h.at[st, s], ha_send.at[0], ha_recv.at[st], mate
        )

    gains[i] = gain_ref[...].astype(bf16).astype(f32)
    gain_copies = [
        remote(gains.at[i], gains.at[i], g_send.at[0], g_recv.at[0], (lax.rem(i + d, n_i), s))
        for d in range(1, n_i)
    ]
    gain_wait = remote(
        gains.at[pl.ds(0, n_i - 1)], gains.at[pl.ds(0, n_i - 1)], g_send.at[0], g_recv.at[0], mate
    )

    def lower(c):
        def body(j, _):
            at = pl.ds(pl.multiple_of(j * tall, tall), tall)
            anchor[i, c, at, :] = master[at, c * LANES : (c + 1) * LANES].astype(bf16)
            return 0

        load_master[c].wait()
        lax.fori_loop(0, piece // tall, body, 0)

    lower(0)
    load_rows[0].wait()
    greeted(barrier)
    a_start(0, 0)
    for c in range(chunks):
        if c > 0:
            lower(c)
        if c == min(2, chunks - 1):
            pl.when(is_end)(lambda: lend_rows(0).start())
        z_mate(i, c).start()
        pl.when(is_inner)(lambda: z_twin(i, c).start())
    for copy in load_rows[1:]:
        copy.wait()
    pl.when(is_end)(lambda: lend_rows(1).start())
    for copy in load_rest:
        copy.start()
    for k in range(2):
        greet(round_sem.at[k])
        greeted(round_sem.at[k])
    for copy in gain_copies:
        copy.start()
    res[...] = jnp.zeros_like(res)
    for copy in load_rest:
        copy.wait()

    def joined(buffer, at, ds):
        return jnp.concatenate([buffer[at, c, ds, :] for c in range(chunks)], axis=1)

    def project(o, count=chunks):
        def body(k, _):
            start = pl.multiple_of(k * depth, depth)
            wide = pl.multiple_of(o * piece + k * depth, depth)
            part = rows[0, :, :, pl.ds(wide, depth)].reshape(tokens, depth)
            weights = [anchor[o, c, pl.ds(start, depth), :] for c in range(count)]
            res[:, : count * LANES] += jnp.dot(part, jnp.concatenate(weights, axis=1), preferred_element_type=f32)
            return 0

        lax.fori_loop(0, piece // depth, body, 0)

    def arrived(o, c):
        z_mate(o, c).wait_recv()

    held = chunks - 1
    groups = 2

    def fold(value):
        return jnp.sum(value.T, axis=0, keepdims=True)

    def spread(value):
        return jnp.broadcast_to(value, (LANES, LANES)).T

    def tile_at(q):
        return pl.ds(pl.multiple_of(q * LANES, LANES), LANES)

    def lanes_of(c):
        return slice(c * LANES, (c + 1) * LANES)

    def products(st, gain, at, among):
        sums = None
        for c in among:
            r = stream[st, at, lanes_of(c)].astype(f32) + res[at, lanes_of(c)] * scale
            res[at, lanes_of(c)] = r
            weighted = r * gain[:, lanes_of(c)]
            terms = (r * r, weighted * weighted, weighted * goals[st, at, lanes_of(c)].astype(f32))
            sums = terms if sums is None else tuple(a + b for a, b in zip(sums, terms))
        return sums

    def local_stats(st, gain, among, held_sums):
        def body(q, _):
            at = tile_at(q)
            sums = products(st, gain, at, among)
            for k in range(3):
                value = sums[k] + early[k, at, :] if held_sums else sums[k]
                stats[st, 0, k : k + 1, at] = fold(value)
            stats[st, 0, 3:4, at] = jnp.zeros((1, LANES), f32)
            return 0

        lax.fori_loop(0, tiles, body, 0, unroll=True)

    def early_stats(q, _):
        at = tile_at(q)
        sums = products(0, gain_read(), at, range(held))
        for k in range(3):
            early[k, at, :] = sums[k]
        return 0

    def part_copy():
        return remote(part_out, part_in, p_send, p_recv, mate)

    def project_for_end():
        weights = jnp.concatenate([anchor[near_far + k, held] for k in range(2)], axis=0)
        count = n_s // groups
        for g in range(groups):
            part = rows_h[0, g * count : (g + 1) * count].reshape(count * block, 2 * piece)
            part_out[g * count * block : (g + 1) * count * block, :] = jnp.dot(
                part, weights, preferred_element_type=f32
            ).astype(bf16)

    def gain_read():
        return jnp.concatenate([gains[j] for j in range(n_i)], axis=1)

    @when_end
    def _():
        one, two, three = mirrored(1), mirrored(2), mirrored(3)
        a_next(0, 0)
        a_start(1, 0)
        for p in range(1, last):
            a_next(0, p)
        a_done(0)
        project(i)
        for c in range(chunks):
            arrived(one, c)
        project(one)
        a_next(1, 0)
        for c in range(held):
            arrived(two, c)
        project(two, held)
        for p in range(1, last):
            a_next(1, p)
        for c in range(held):
            arrived(three, c)
        project(three, held)
        gain_wait.wait_recv()
        lax.fori_loop(0, tiles, early_stats, 0, unroll=True)
        part_copy().wait_recv()
        res[:, held * LANES :] += part_in[...].astype(f32)
        local_stats(0, gain_read(), (held,), True)

    @when_inner
    def _():
        zero, two, three = mirrored(0), mirrored(2), mirrored(3)

        def from_end(c):
            arrived(zero, c)
            z_twin(zero, c).start()

        def from_far(o, c):
            arrived(o, c)
            if c < held:
                z_mate(o, c).start()

        from_end(0)
        from_far(two, 0)
        a_next(0, 0)
        from_end(1)
        for c in range(1, chunks):
            from_far(two, c)
        from_end(2)
        for p in range(1, last):
            a_next(0, p)
        lend_rows(0).wait_recv()
        a_start(2, 0)
        from_far(three, 0)
        a_next(2, 0)
        a_start(1, 0)
        for c in range(3, chunks):
            from_end(c)
        a_done(0)
        project(i)
        from_far(three, 1)
        project(zero)
        for p in range(1, last):
            a_next(2, p)
        for c in range(2, held):
            from_far(three, c)
        project(two)
        from_far(three, held)
        a_done(2)
        project_for_end()
        part_copy().start()
        project(three)

    def row_stats(st, between=None):
        copies = [
            remote(
                stats.at[st, 0], stats.at[st, d], s_send.at[st], s_recv.at[st],
                (i, lax.rem(s + d, n_s)),
            )
            for d in range(1, n_s)
        ]
        for copy in copies:
            copy.start()
        if between is not None:
            between()
        others = stats.at[st, pl.ds(1, n_s - 1)]
        remote(others, others, s_send.at[st], s_recv.at[st], mate).wait()
        total = stats[st, 0]
        for d in range(1, n_s):
            total = total + stats[st, d]
        inverse = lax.rsqrt(total[0:1] * (1.0 / width) + norm_epsilon)
        pull = inverse * total[1:2] - total[2:3]
        line[0:1, :] = inverse
        line[1:2, :] = inverse * inverse * inverse * pull * (1.0 / width)

    def row_grads(st, gain, among):
        def body(q, totals):
            at = tile_at(q)
            inverse, pull = spread(line[0:1, at]), spread(line[1:2, at])
            found = []
            for c, total in zip(among, totals):
                r = res[at, lanes_of(c)]
                unit = r * inverse
                scaled = gain[:, lanes_of(c)]
                loss = unit * scaled - goals[st, at, lanes_of(c)].astype(f32)
                loss = loss.astype(bf16).astype(f32)
                low = inverse * (loss * scaled) - r * pull
                slope[st, c, at, :] = (low * scale if exact else low).astype(bf16)
                found.append(total + jnp.sum(loss * unit, axis=0, keepdims=True))
            return tuple(found)

        return lax.fori_loop(0, tiles, body, (jnp.zeros((1, LANES), f32),) * len(among), unroll=True)

    def product(part, against):
        grad = lax.dot_general(part, against, (((0,), (0,)), ((), ())), preferred_element_type=f32)
        return grad if exact else grad * scale

    def weight_grad(st, wide, size):
        part = rows[st, :, :, pl.ds(pl.multiple_of(wide, size), size)].reshape(tokens, size)
        return product(part, joined(slope, st, slice(None)))

    def more_rows():
        @when_inner
        def _():
            a_next(1, 0)
            lend_rows(1).wait_recv()
            a_start(3, 0)

    @when_inner
    def _():
        gain_wait.wait_recv()
        local_stats(0, gain_read(), range(chunks), False)

    gain_anchor = gain_read()
    gain = gain_anchor
    row_stats(0, more_rows)
    gain_first = jnp.concatenate(row_grads(0, gain, range(chunks)), axis=1)
    res[...] = jnp.zeros_like(res)

    def lend_slope(st, c):
        return remote(slope.at[st, c], slope_h.at[st, c], r_send.at[0], r_recv.at[st, c], mate)

    @when_end
    def _():
        for c in range(held):
            lend_slope(0, c).start()

    spans = width // span
    per_piece = piece // span

    def place(q):
        return mirrored(q // per_piece), q % per_piece

    def grad_one(q):
        o, j = place(q)
        return weight_grad(0, o * piece + j * span, span)

    def step_one(q, grad, ahead, keep_grad=True):
        o, j = place(q)
        at = pl.ds(pl.multiple_of(j * span, span), span)
        if keep_grad:
            grads[o, at, :] = grad
        step = (inner_rate * grad) * pl.reciprocal(jnp.abs(grad) + adam_epsilon)
        param = keep * joined(anchor, o, at).astype(f32) - step
        ahead[...] = param.astype(bf16)

    def project_later(q, ahead):
        o, j = place(q)
        wide = pl.multiple_of(o * piece + j * span, span)
        part = rows[1, :, :, pl.ds(wide, span)].reshape(tokens, span)
        res[...] += jnp.dot(part, ahead[...], preferred_element_type=f32)

    def both(t, _):
        even = grad_one(2 * t)
        odd = grad_one(2 * t + 1)
        step_one(2 * t, even, ahead_a)
        project_later(2 * t, ahead_a)
        step_one(2 * t + 1, odd, ahead_b)
        project_later(2 * t + 1, ahead_b)
        return 0

    def both_grads(t, _):
        for q in (2 * t, 2 * t + 1):
            o, j = place(q)
            grads[o, pl.ds(pl.multiple_of(j * span, span), span), :] = grad_one(q)
        return 0

    def both_rest(t, _):
        for q, ahead in ((2 * t, ahead_a), (2 * t + 1, ahead_b)):
            o, j = place(q)
            step_one(q, grads[o, pl.ds(pl.multiple_of(j * span, span), span), :], ahead, False)
        project_later(2 * t, ahead_a)
        project_later(2 * t + 1, ahead_b)
        return 0

    def one_alone(q, _):
        step_one(q, grad_one(q), later.at[q])
        return 0

    group = 2 if per_piece % 2 == 0 else 1

    def later_alone(g, _):
        o, j = place(g * group)
        wide = pl.multiple_of(o * piece + j * span, span)
        part = rows[1, :, :, pl.ds(wide, group * span)].reshape(tokens, group * span)
        weights = jnp.concatenate([later[g * group + k] for k in range(group)], axis=0)
        res[...] += jnp.dot(part, weights, preferred_element_type=f32)
        return 0

    @when_end
    def _():
        a_done(1)
        near = 2 * per_piece // 2
        lax.fori_loop(0, near, both, 0, unroll=True)
        arrived(mirrored(2), held)
        lax.fori_loop(near, near + per_piece // 2, both, 0)
        lax.fori_loop(near + per_piece // 2, spans // 2, both_grads, 0)
        arrived(mirrored(3), held)
        lax.fori_loop(near + per_piece // 2, spans // 2, both_rest, 0)

    @when_inner
    def _():
        lax.fori_loop(0, spans, one_alone, 0)
        z_mate(mirrored(2), held).start()
        z_mate(mirrored(3), held).start()
        for p in range(1, last):
            a_next(1, p)
        a_next(3, 0)
        a_done(1)
        lax.fori_loop(0, spans // group, later_alone, 0)
        for p in range(1, last):
            a_next(3, p)

    gain_step = first_update(gain_first)
    gain = gain_anchor - inner_rate * gain_step

    local_stats(1, gain, range(chunks), False)
    row_stats(1)
    is_even = lax.rem(s, 2) == 0
    gain_second = row_grads(1, gain, (0,))

    @pl.when(is_end & is_even)
    def _():
        lend_slope(1, 0).start()

    gain_second = jnp.concatenate(gain_second + row_grads(1, gain, range(1, chunks)), axis=1)
    when_inner(lambda: a_start(4, 0))
    gain_move = inner_rate * (gain_step + second_update(gain_first, gain_second))
    for j in range(n_i):
        gain_out[j] = gain_move[:, j * own : (j + 1) * own]

    gain_moves = [
        remote(
            gain_out.at[lax.rem(i + d, n_i)], gain_in.at[d], g_send.at[1], g_recv.at[1],
            (lax.rem(i + d, n_i), s),
        )
        for d in range(1, n_i)
    ]
    for copy in gain_moves:
        copy.start()

    def move(o, first=0, until=piece // span):
        def body(j, _):
            at = pl.ds(pl.multiple_of(j * span, span), span)
            grad = weight_grad(1, o * piece + j * span, span)
            grads[o, at, :] = outer_sum(grads[o, at, :], grad)
            return 0

        lax.fori_loop(first, until, body, 0)

    def give(slot, c):
        return remote(outgo.at[slot, c], from_mate.at[c], e_send.at[0], e_recv.at[c], mate)

    def cross(slot, c, at=slice(None)):
        return remote(
            outgo.at[slot, c, at], from_twin.at[slot, c, at], m_send.at[0], m_recv.at[slot, c], twin
        )

    def pack(slot, c, o, *others):
        lanes = slice(c * LANES, (c + 1) * LANES)

        def body(j, _):
            at = pl.ds(pl.multiple_of(j * tall, tall), tall)
            total = grads[o, at, lanes]
            for other in others:
                total = total + other[at, :].astype(f32)
            outgo[slot, c, at, :] = total.astype(bf16)
            return 0

        lax.fori_loop(0, piece // tall, body, 0)

    def finish(c, o, *others):
        lanes = slice(c * LANES, (c + 1) * LANES)

        def body(j, _):
            at = pl.ds(pl.multiple_of(j * tall, tall), tall)
            total = grads[o, at, lanes]
            for other in others:
                total = total + other[at, :].astype(f32)
            outer = master[at, lanes]
            pseudo = total * (1.0 / n_i) + (1.0 - keep * keep) * outer.astype(bf16).astype(f32)
            velocity = outer_momentum * moment[at, lanes] + pseudo
            velocity_ref[at, lanes] = velocity
            updated_ref[at, lanes] = outer - outer_rate * (pseudo + outer_momentum * velocity)
            return 0

        lax.fori_loop(0, piece // tall, body, 0)
    @when_end
    def _():
        o = mirrored(1)
        parts = piece // span
        wait_parts = (parts + 1) // 2
        move(o, 0, wait_parts)

        @pl.when(jnp.logical_not(is_even))
        def _():
            lend_slope(1, 0).start()

        move(o, wait_parts, parts)
        for c in range(chunks):
            pack(0, c, o)
        for c in range(1, chunks):
            lend_slope(1, c).start()
            if c == held - 1:
                lend_slope(0, held).start()
        for c in range(chunks):
            give(0, c).start()
        o = mirrored(0)
        move(o)
        for c in range(chunks):
            give(0, c).wait_recv()
            finish(c, o, from_mate.at[c])

    def help_end(slot, c, o):
        base = (o - near_far) * piece
        lanes = slice(c * LANES, (c + 1) * LANES)

        def body(j, _):
            at = pl.ds(pl.multiple_of(j * tall, tall), tall)
            wide = pl.ds(pl.multiple_of(base + j * tall, tall), tall)
            pair = [
                product(rows_h[st, :, :, wide].reshape(tokens, tall), slope_h[st, c]) for st in range(steps)
            ]
            outgo[slot, c, at, :] = (grads[o, at, lanes] + outer_sum(*pair)).astype(bf16)
            cross(slot, c, at).start()
            return 0

        lax.fori_loop(0, piece // tall, body, 0)

    @when_inner
    def _():
        def help_and_cross(slot, c):
            help_end(slot, c, mirrored(3 - slot))

        def forward(c):
            cross(0, c).wait_recv()
            pack(2, c, mirrored(0), from_twin.at[0, c])
            give(2, c).start()

        move(mirrored(3))
        a_done(3)

        def far_sum(c):
            lend_slope(0, c).wait_recv()
            lend_slope(1, c).wait_recv()
            help_and_cross(0, c)

        phases = list(range(last))
        for c in range(held):
            far_sum(c)
            if c == 0:
                a_next(4, phases.pop(0))
                move(mirrored(0))
            if c == 1:
                for p in phases:
                    a_next(4, p)
                move(mirrored(2))
        forward(0)
        a_done(4)
        help_and_cross(1, 0)
        far_sum(held)
        for c in range(1, chunks):
            if c < held:
                forward(c)
            help_and_cross(1, c)
            if c == 1:
                move(mirrored(1))
        forward(held)
        for c in range(chunks):
            give(2, c).wait_recv()
            cross(1, c).wait_recv()
            finish(c, mirrored(1), from_mate.at[c], from_twin.at[1, c])

    moved_gains = gain_in.at[pl.ds(1, n_i - 1)]
    remote(moved_gains, moved_gains, g_send.at[1], g_recv.at[1], mate).wait()
    gain_total = gain_out[i]
    for d in range(1, n_i):
        gain_total = gain_total + gain_in[d]
    gain_pseudo = gain_total * (1.0 / n_i)
    gain_velocity = outer_momentum * gain_moment_ref[...] + gain_pseudo
    gain_velocity_ref[...] = gain_velocity
    gain_updated_ref[...] = gain_ref[...] - outer_rate * (gain_pseudo + outer_momentum * gain_velocity)

    def sent_pieces(way, count):
        pieces = anchor.at[pl.ds(0, count)]
        remote(pieces, pieces, z_send.at[way], z_recv.at[0, 0], mate).wait_send()

    @when_end
    def _():
        lent = rows_h.at[pl.ds(0, steps), 0]
        remote(lent, lent, ha_send.at[0], ha_recv.at[0], mate).wait_send()
        sent_pieces(0, 1)
        remote(slope, slope, r_send.at[0], r_recv.at[0, 0], mate).wait_send()
        remote(from_mate, from_mate, e_send.at[0], e_recv.at[0], mate).wait_send()

    @when_inner
    def _():
        remote(from_twin, from_twin, m_send.at[0], m_recv.at[0, 0], twin).wait_send()
        remote(from_mate, from_mate, e_send.at[0], e_recv.at[0], mate).wait_send()
        part_copy().wait_send()
        for which in (2, 3, 4):
            a_sent(which)
        sent_pieces(0, 3)
        sent_pieces(1, 2)

    gain_wait.wait_send()
    a_sent(0)
    a_sent(1)


def write_out(*refs):
    count = len(refs) // 2
    sem = refs[-1]
    copies = [pltpu.make_async_copy(refs[k], refs[count + k], sem.at[k]) for k in range(count)]
    for copy in copies:
        copy.start()
    for copy in copies:
        copy.wait()


def per_device(weight_master, gain_master, weight_moment, gain_moment, attended, stream, targets):
    n_i, n_s = lax.axis_size("island"), lax.axis_size("shard")
    _, steps, block, width = attended.shape
    _, _, tokens, cols = stream.shape
    piece = weight_master.shape[0]
    own = gain_master.shape[0]
    f32, bf16 = jnp.float32, jnp.bfloat16
    chunks = cols // LANES
    arrays = [
        ((piece, cols), f32),
        ((piece, cols), f32),
        ((steps, n_s, block, width), bf16),
        ((steps, n_s, block, 2 * piece), bf16),
        ((n_i, chunks, piece, LANES), bf16),
        ((min(512, piece), cols), bf16),
        ((min(512, piece), cols), bf16),
        ((width // min(512, piece), min(512, piece), cols), bf16),
        ((n_i, piece, cols), f32),
        ((tokens, cols), f32),
        ((steps, chunks, tokens, LANES), bf16),
        ((steps, chunks, tokens, LANES), bf16),
        ((steps, tokens, cols), bf16),
        ((steps, tokens, cols), bf16),
        ((3, chunks, piece, LANES), bf16),
        ((chunks, piece, LANES), bf16),
        ((2, chunks, piece, LANES), bf16),
        ((tokens, LANES), bf16),
        ((tokens, LANES), bf16),
        ((3, tokens, LANES), f32),
        ((steps, n_s, 4, tokens), f32),
        ((2, tokens), f32),
        ((n_i, 1, own), f32),
        ((n_i, 1, own), f32),
        ((n_i, 1, own), f32),
    ]
    held = sum(math.prod(shape) * jnp.dtype(kind).itemsize for shape, kind in arrays)
    spans = piece // min(512, piece)
    if spans % 2 or n_i != 4 or steps != 2 or own % LANES or chunks < 2 or block % 32 or n_s < 8 or held > 60e6:
        return general_device(weight_master, gain_master, weight_moment, gain_moment, attended, stream, targets)
    any_space = pl.BlockSpec(memory_space=pl.ANY)
    vmem = pl.BlockSpec(memory_space=pltpu.VMEM)
    dma = pltpu.SemaphoreType.DMA
    outs = ((piece, cols), (1, own), (piece, cols), (1, own))
    results = pl.pallas_call(
        functools.partial(kernel, n_i, n_s),
        out_shape=tuple(pltpu.VMEM(shape, f32) for shape in outs),
        in_specs=[any_space, vmem, any_space, vmem, any_space, any_space, any_space],
        out_specs=(vmem, vmem, vmem, vmem),
        scratch_shapes=[pltpu.VMEM(shape, kind) for shape, kind in arrays]
        + [
            pltpu.SemaphoreType.REGULAR((2,)),
            dma((3 + steps + chunks,)),
            dma((2,)),
            dma((n_i, chunks)),
            dma((5,)),
            dma((5, n_s.bit_length())),
            dma(()),
            dma(()),
            dma((1,)),
            dma((steps,)),
            dma((steps,)),
            dma((steps,)),
            dma((2,)),
            dma((2,)),
            dma((1,)),
            dma((steps, chunks)),
            dma((1,)),
            dma((chunks,)),
            dma((1,)),
            dma((2, chunks)),
        ],
        compiler_params=pltpu.CompilerParams(
            collective_id=0, has_side_effects=True, vmem_limit_bytes=58 << 20
        ),
    )(weight_master, gain_master[None], weight_moment, gain_moment[None], attended, stream, targets)
    results = [pltpu.with_memory_space_constraint(x, pltpu.VMEM) for x in results]
    updated, gain_updated, velocity, gain_velocity = pl.pallas_call(
        write_out,
        out_shape=tuple(jax.ShapeDtypeStruct(shape, f32) for shape in outs),
        in_specs=[vmem] * 4,
        out_specs=(any_space,) * 4,
        scratch_shapes=[dma((4,))],
        compiler_params=pltpu.CompilerParams(vmem_limit_bytes=1 << 20),
    )(*results)
    return (updated, gain_updated[0], velocity, gain_velocity[0])


def solution(mesh):
    placed = (
        P("island", "shard"),
        P(("shard", "island")),
        P("island", "shard"),
        P(("shard", "island")),
        P("island", None, "shard", None),
        P("island", None, None, "shard"),
        P("island", None, None, "shard"),
    )
    return jax.shard_map(
        per_device,
        mesh=mesh,
        in_specs=placed,
        out_specs=(
            P("island", "shard"),
            P(("shard", "island")),
            P("island", "shard"),
            P(("shard", "island")),
        ),
        check_vma=False,
    )
```

```python
import functools
import math

import jax
import jax.numpy as jnp
from jax import lax
from jax.experimental import pallas as pl
from jax.experimental.pallas import tpu as pltpu
from jax.sharding import PartitionSpec as P

norm_epsilon = 1e-05
inner_rate = 0.05
beta_one = 0.9
beta_two = 0.95
adam_epsilon = 0.3
decay_rate = 0.1
outer_rate = 0.7
outer_momentum = 0.9

MESH = pl.DeviceIdType.MESH
LANES = 128
keep = 1.0 - inner_rate * decay_rate


def flip(index, bit):
    size = 1 << bit
    return index + size * (1 - 2 * (lax.div(index, size) % 2))


def first_update(grad):
    return grad / (jnp.abs(grad) + adam_epsilon)


def second_update(earlier, grad):
    first = (beta_one * (1.0 - beta_one)) * earlier + (1.0 - beta_one) * grad
    second = (beta_two * (1.0 - beta_two)) * earlier * earlier + (1.0 - beta_two) * grad * grad
    first_hat = first * (1.0 / (1.0 - beta_one**2))
    second_hat = second * (1.0 / (1.0 - beta_two**2))
    return first_hat / (jnp.sqrt(second_hat) + adam_epsilon)


def general_kernel(
    n_i, n_s, low_ref, gain_ref, rows_ref, stream_ref, goals_ref, total_ref, gain_total_ref,
    rows, anchor, later, grads, res, slope_low, stream, goals, from_left, from_right,
    stats, line, gains, gain_moves,
    local_sem, z_send, z_recv, a_send, a_recv, s_send, s_recv, g_send, g_recv, r_send, r_recv,
):
    i = lax.axis_index("island")
    s = lax.axis_index("shard")
    steps, _, block, width = rows.shape
    piece, cols = low_ref.shape
    tokens = n_s * block
    tiles = tokens // LANES
    scale = width ** (-0.5)
    depth = min(512, piece)
    tall = min(256, piece)

    barrier = pltpu.get_barrier_semaphore()
    for d in range(1, n_i):
        pl.semaphore_signal(barrier, inc=1, device_id=(lax.rem(i + d, n_i), s), device_id_type=MESH)
    for d in range(1, n_s):
        pl.semaphore_signal(barrier, inc=1, device_id=(i, lax.rem(s + d, n_s)), device_id_type=MESH)

    locals_ = [pltpu.make_async_copy(low_ref, anchor.at[i], local_sem.at[0])]
    for st in range(steps):
        locals_.append(pltpu.make_async_copy(rows_ref.at[0, st], rows.at[st, s], local_sem.at[1 + st]))
    locals_.append(pltpu.make_async_copy(stream_ref.at[0], stream, local_sem.at[1 + steps]))
    locals_.append(pltpu.make_async_copy(goals_ref.at[0], goals, local_sem.at[2 + steps]))
    for copy in locals_:
        copy.start()
    pl.semaphore_wait(barrier, n_i - 1 + n_s - 1)

    def remote(src, dst, send, recv, to):
        return pltpu.make_async_remote_copy(
            src_ref=src, dst_ref=dst, send_sem=send, recv_sem=recv, device_id=to, device_id_type=MESH
        )

    right, left = (lax.rem(i + 1, n_i), s), (lax.rem(i + n_i - 1, n_i), s)

    def z_copy(way, t, at):
        return remote(
            anchor.at[at], anchor.at[at], z_send.at[way, t], z_recv.at[way, t], right if way == 0 else left
        )

    def z_start(t):
        @pl.when((i < n_i - 1) & (i - t >= 0))
        def _():
            z_copy(0, t, i - t).start()

        @pl.when((i > 0) & (i + t <= n_i - 1))
        def _():
            z_copy(1, t, i + t).start()

    def z_wait(t):
        @pl.when(i - 1 - t >= 0)
        def _():
            z_copy(0, t, i - 1 - t).wait_recv()

        @pl.when(i + 1 + t <= n_i - 1)
        def _():
            z_copy(1, t, i + 1 + t).wait_recv()

    n_bits = n_s.bit_length() - 1
    orders = [list(range(1, n_bits)) + [0], list(range(n_bits - 1, 0, -1)) + [0]]

    def a_blocks(st, phase):
        order = orders[st % 2]
        found = []
        for m in range(1 << phase):
            at = s
            for q in range(phase):
                if (m >> q) & 1:
                    at = flip(at, order[q])
            found.append(at)
        return found

    def a_copy(st, phase, m, at):
        slot = (1 << phase) - 1 + m
        return remote(
            rows.at[st, at], rows.at[st, at], a_send.at[st, slot], a_recv.at[st, slot],
            (i, flip(s, orders[st % 2][phase])),
        )

    def a_start(phase):
        for st in range(steps):
            for m, at in enumerate(a_blocks(st, phase)):
                a_copy(st, phase, m, at).start()

    def a_wait(phase):
        for st in range(steps):
            for m, at in enumerate(a_blocks(st, phase)):
                a_copy(st, phase, m, flip(at, orders[st % 2][phase])).wait_recv()

    def to_islands(buffer, which):
        return [
            remote(
                buffer.at[0], buffer.at[d], g_send.at[which, d], g_recv.at[which, d],
                (lax.rem(i + d, n_i), s),
            )
            for d in range(1, n_i)
        ]

    locals_[0].wait()
    z_start(0)
    for copy in locals_[1 : 1 + steps]:
        copy.wait()
    a_start(0)
    gains[0] = gain_ref[...]
    gain_in = to_islands(gains, 0)
    for copy in gain_in:
        copy.start()
    res[...] = jnp.zeros_like(res)
    for copy in locals_[1 + steps :]:
        copy.wait()

    def project(st, weights, at):
        def body(k, _):
            start = pl.multiple_of(k * depth, depth)
            wide = pl.multiple_of(at * piece + k * depth, depth)
            part = rows[st, :, :, pl.ds(wide, depth)].reshape(tokens, depth)
            res[...] += jnp.dot(part, weights[at, pl.ds(start, depth), :], preferred_element_type=jnp.float32)
            return 0

        lax.fori_loop(0, piece // depth, body, 0)

    def project_arrived(t):
        @pl.when(i - 1 - t >= 0)
        def _():
            project(0, anchor, i - 1 - t)

        @pl.when(i + 1 + t <= n_i - 1)
        def _():
            project(0, anchor, i + 1 + t)

    events = [(2.0 * t + 2.6, "z", t) for t in range(n_i - 1)]
    events += [(2.0 * ((2 << p) - 1), "a", p) for p in range(n_bits - 1)]
    last = events[-1][0] if n_bits > 1 else 0.0
    events.append((last + 0.1, "a", n_bits - 1))
    gathered, ready = False, []
    for _, kind, at in sorted(events):
        if kind == "a":
            a_wait(at)
            if at + 1 < n_bits:
                a_start(at + 1)
            else:
                gathered = True
                project(0, anchor, i)
                for t in ready:
                    project_arrived(t)
        else:
            z_wait(at)
            if at + 1 < n_i - 1:
                z_start(at + 1)
            if gathered:
                project_arrived(at)
            else:
                ready.append(at)

    for copy in gain_in:
        copy.wait()
    gain_anchor = gains[0]
    for d in range(1, n_i):
        gain_anchor = gain_anchor + gains[d]
    gain = gain_anchor

    def fold(value):
        total = value[:, :LANES]
        for c in range(1, cols // LANES):
            total = total + value[:, c * LANES : (c + 1) * LANES]
        return jnp.sum(total.T, axis=0, keepdims=True)

    def spread(value):
        square = jnp.broadcast_to(value, (LANES, LANES)).T
        return jnp.concatenate([square] * (cols // LANES), axis=1)

    def row_stats(st, gain):
        def body(q, _):
            at = pl.ds(pl.multiple_of(q * LANES, LANES), LANES)
            r = stream[st, at, :].astype(jnp.float32) + res[at, :] * scale
            res[at, :] = r
            weighted = r * gain
            stats[st, 0, 0:1, at] = fold(r * r)
            stats[st, 0, 1:2, at] = fold(weighted * weighted)
            stats[st, 0, 2:3, at] = fold(weighted * goals[st, at, :].astype(jnp.float32))
            stats[st, 0, 3:4, at] = jnp.zeros((1, LANES), jnp.float32)
            return 0

        lax.fori_loop(0, tiles, body, 0)
        copies = [
            remote(
                stats.at[st, 0], stats.at[st, d], s_send.at[st, d], s_recv.at[st, d],
                (i, lax.rem(s + d, n_s)),
            )
            for d in range(1, n_s)
        ]
        for copy in copies:
            copy.start()
        for copy in copies:
            copy.wait()
        total = stats[st, 0]
        for d in range(1, n_s):
            total = total + stats[st, d]
        inverse = lax.rsqrt(total[0:1] * (1.0 / width) + norm_epsilon)
        slope = inverse * total[1:2] - total[2:3]
        line[0:1, :] = inverse
        line[1:2, :] = inverse * inverse * inverse * slope * (1.0 / width)

    def row_grads(st, gain):
        def body(q, total):
            at = pl.ds(pl.multiple_of(q * LANES, LANES), LANES)
            inverse, pull = spread(line[0:1, at]), spread(line[1:2, at])
            r = res[at, :]
            unit = r * inverse
            loss = unit * gain - goals[st, at, :].astype(jnp.float32)
            loss = loss.astype(jnp.bfloat16).astype(jnp.float32)
            slope_low[at, :] = (inverse * (loss * gain) - r * pull).astype(jnp.bfloat16)
            return total + jnp.sum(loss * unit, axis=0, keepdims=True)

        return lax.fori_loop(0, tiles, body, jnp.zeros((1, cols), jnp.float32))

    def weight_grad(st, wide):
        part = rows[st, :, :, pl.ds(pl.multiple_of(wide, tall), tall)].reshape(tokens, tall)
        return (
            lax.dot_general(
                part, slope_low[...], (((0,), (0,)), ((), ())), preferred_element_type=jnp.float32
            )
            * scale
        )

    row_stats(0, gain)
    gain_first = row_grads(0, gain)
    per_piece = piece // tall

    def step_one(q, _):
        o, j = q // per_piece, q % per_piece
        at = pl.ds(pl.multiple_of(j * tall, tall), tall)
        grad = weight_grad(0, q * tall)
        grads[o, at, :] = grad
        param = keep * anchor[o, at, :].astype(jnp.float32) - inner_rate * first_update(grad)
        later[o, at, :] = param.astype(jnp.bfloat16)
        return 0

    lax.fori_loop(0, n_i * per_piece, step_one, 0)
    gain_step = first_update(gain_first)
    gain = gain_anchor - inner_rate * gain_step

    res[...] = jnp.zeros_like(res)

    def project_later(at, _):
        project(1, later, at)
        return 0

    lax.fori_loop(0, n_i, project_later, 0)
    row_stats(1, gain)
    gain_second = row_grads(1, gain)
    gain_moves[0] = inner_rate * (gain_step + second_update(gain_first, gain_second))
    gain_out = to_islands(gain_moves, 1)
    for copy in gain_out:
        copy.start()

    def to_right(k):
        at = n_i - 1 - k
        return remote(later.at[at], from_left.at[k], r_send.at[0, k], r_recv.at[0, k], right)

    def to_left(k):
        return remote(later.at[k], from_right.at[k], r_send.at[1, k], r_recv.at[1, k], left)

    early = 1 - lax.div(2 * i, n_i)

    def owner_piece(q, _):
        o = q + early * (n_i - 1 - 2 * q)

        def step_two(j, _):
            at = pl.ds(pl.multiple_of(j * tall, tall), tall)
            grad = weight_grad(1, o * piece + j * tall)
            earlier = grads[o, at, :]
            moved = (1.0 - keep * keep) * anchor[o, at, :].astype(jnp.float32) + inner_rate * (
                keep * first_update(earlier) + second_update(earlier, grad)
            )
            grads[o, at, :] = moved
            later[o, at, :] = moved.astype(jnp.bfloat16)
            return 0

        lax.fori_loop(0, per_piece, step_two, 0)

        @pl.when((i == 0) & (o > 0))
        def _():
            to_right(n_i - 1 - o).start()

        @pl.when((i == n_i - 1) & (o < n_i - 1))
        def _():
            to_left(o).start()

        return 0

    lax.fori_loop(0, n_i, owner_piece, 0)

    def add(o, arrived, k):
        def body(j, _):
            at = pl.ds(pl.multiple_of(j * tall, tall), tall)
            later[o, at, :] = (grads[o, at, :] + arrived[k, at, :].astype(jnp.float32)).astype(jnp.bfloat16)
            return 0

        lax.fori_loop(0, per_piece, body, 0)

    for t in range(n_i - 1):
        k_right = t - i
        k_left = t - (n_i - 1 - i)

        @pl.when((i > 0) & (k_right >= 0) & (k_right < n_i - 1 - i))
        def _():
            to_right(k_right).wait_recv()
            add(n_i - 1 - k_right, from_left, k_right)
            to_right(k_right).start()

        @pl.when((i < n_i - 1) & (k_left >= 0) & (k_left < i))
        def _():
            to_left(k_left).wait_recv()
            add(k_left, from_right, k_left)
            to_left(k_left).start()

    for copy in gain_out:
        copy.wait()
    gain_total = gain_moves[0]
    for d in range(1, n_i):
        gain_total = gain_total + gain_moves[d]
    gain_total_ref[...] = gain_total

    total_ref[...] = grads[i]

    @pl.when(i > 0)
    def _():
        k = n_i - 1 - i
        to_right(k).wait_recv()
        total_ref[...] += from_left[k].astype(jnp.float32)

    @pl.when(i < n_i - 1)
    def _():
        to_left(i).wait_recv()
        total_ref[...] += from_right[i].astype(jnp.float32)

    for k in range(n_i - 1):

        @pl.when(k < n_i - 1 - i)
        def _(k=k):
            to_right(k).wait_send()

        @pl.when(k < i)
        def _(k=k):
            to_left(k).wait_send()

        @pl.when((i < n_i - 1) & (i - k >= 0))
        def _(k=k):
            z_copy(0, k, i - k).wait_send()

        @pl.when((i > 0) & (i + k <= n_i - 1))
        def _(k=k):
            z_copy(1, k, i + k).wait_send()

    for phase in range(n_bits):
        for st in range(steps):
            for m, at in enumerate(a_blocks(st, phase)):
                a_copy(st, phase, m, at).wait_send()


def general_device(weight_master, gain_master, weight_moment, gain_moment, attended, stream, targets):
    n_i, n_s = lax.axis_size("island"), lax.axis_size("shard")
    _, steps, block, width = attended.shape
    _, _, tokens, cols = stream.shape
    piece = weight_master.shape[0]
    own = gain_master.shape[0]
    offset = lax.axis_index("island") * own
    low = weight_master.astype(jnp.bfloat16)
    gain_low = gain_master.astype(jnp.bfloat16).astype(jnp.float32)
    gain_row = lax.dynamic_update_slice(jnp.zeros((1, cols), jnp.float32), gain_low[None], (0, offset))
    any_space = pl.BlockSpec(memory_space=pl.ANY)
    vmem = pl.BlockSpec(memory_space=pltpu.VMEM)
    f32, bf16 = jnp.float32, jnp.bfloat16
    dma = pltpu.SemaphoreType.DMA
    weight_summed, gain_summed = pl.pallas_call(
        functools.partial(general_kernel, n_i, n_s),
        out_shape=(
            jax.ShapeDtypeStruct((piece, cols), f32),
            jax.ShapeDtypeStruct((1, cols), f32),
        ),
        in_specs=[any_space, vmem, any_space, any_space, any_space],
        out_specs=(vmem, vmem),
        scratch_shapes=[
            pltpu.VMEM((steps, n_s, block, width), bf16),
            pltpu.VMEM((n_i, piece, cols), bf16),
            pltpu.VMEM((n_i, piece, cols), bf16),
            pltpu.VMEM((n_i, piece, cols), f32),
            pltpu.VMEM((tokens, cols), f32),
            pltpu.VMEM((tokens, cols), bf16),
            pltpu.VMEM((steps, tokens, cols), bf16),
            pltpu.VMEM((steps, tokens, cols), bf16),
            pltpu.VMEM((n_i - 1, piece, cols), bf16),
            pltpu.VMEM((n_i - 1, piece, cols), bf16),
            pltpu.VMEM((steps, n_s, 4, tokens), f32),
            pltpu.VMEM((2, tokens), f32),
            pltpu.VMEM((n_i, 1, cols), f32),
            pltpu.VMEM((n_i, 1, cols), f32),
            dma((3 + steps,)),
            dma((2, n_i - 1)),
            dma((2, n_i - 1)),
            dma((steps, n_s - 1)),
            dma((steps, n_s - 1)),
            dma((steps, n_s)),
            dma((steps, n_s)),
            dma((2, n_i)),
            dma((2, n_i)),
            dma((2, n_i - 1)),
            dma((2, n_i - 1)),
        ],
        compiler_params=pltpu.CompilerParams(
            collective_id=0, has_side_effects=True, vmem_limit_bytes=67043328
        ),
    )(low, gain_row, attended, stream, targets)
    weight_pseudo = weight_summed / n_i
    gain_pseudo = lax.dynamic_slice(gain_summed, (0, offset), (1, own))[0] / n_i
    weight_velocity = outer_momentum * weight_moment + weight_pseudo
    gain_velocity = outer_momentum * gain_moment + gain_pseudo
    weight_updated = weight_master - outer_rate * (weight_pseudo + outer_momentum * weight_velocity)
    gain_updated = gain_master - outer_rate * (gain_pseudo + outer_momentum * gain_velocity)
    return (weight_updated, gain_updated, weight_velocity, gain_velocity)


def outer_sum(grad_one, grad_two):
    first = (inner_rate * beta_one * (1.0 - beta_one) / (1.0 - beta_one**2)) * grad_one + (
        inner_rate * (1.0 - beta_one) / (1.0 - beta_one**2)
    ) * grad_two
    second = (beta_two * (1.0 - beta_two) / (1.0 - beta_two**2)) * (grad_one * grad_one) + (
        (1.0 - beta_two) / (1.0 - beta_two**2)
    ) * (grad_two * grad_two)
    root = second * lax.rsqrt(jnp.maximum(second, 1e-30)) + adam_epsilon
    size = jnp.abs(grad_one) + adam_epsilon
    return ((inner_rate * keep) * grad_one * root + first * size) * pl.reciprocal(root * size)


def kernel(
    n_i, n_s, master_ref, gain_ref, moment_ref, gain_moment_ref, rows_ref, stream_ref, goals_ref,
    updated_ref, gain_updated_ref, velocity_ref, gain_velocity_ref,
    master, moment, rows, rows_h, anchor, ahead_a, ahead_b, later, grads, res, slope, slope_h, stream, goals,
    outgo, from_mate, from_twin, part_out, part_in, early, stats, line, gains, gain_out, gain_in,
    round_sem, local_sem, z_send, z_recv, a_send, a_recv, p_send, p_recv, ha_send, ha_recv,
    s_send, s_recv, g_send, g_recv, r_send, r_recv, e_send, e_recv, m_send, m_recv,
):
    i = lax.axis_index("island")
    s = lax.axis_index("shard")
    steps, _, block, width = rows.shape
    _, chunks, piece, _ = anchor.shape
    cols = chunks * LANES
    own = gains.shape[2]
    tokens = n_s * block
    tiles = tokens // LANES
    scale = width ** (-0.5)
    exact = math.frexp(scale)[0] == 0.5
    depth = min(1024, piece)
    tall = min(256, piece)
    span = min(512, piece)
    f32, bf16 = jnp.float32, jnp.bfloat16

    is_left = i < n_i // 2
    is_end = (i == 0) | (i == n_i - 1)
    is_inner = (i > 0) & (i < n_i - 1)
    toward = jnp.where(is_left, 1, -1)
    mate = (jnp.where(is_end, i + toward, i - toward), s)
    twin = (n_i - 1 - i, s)

    def when_inner(f):
        pl.when(is_inner)(f)

    def when_end(f):
        pl.when(is_end)(f)

    def mirrored(o):
        return jnp.where(is_left, o, n_i - 1 - o)

    near_far = jnp.where(is_left, n_i - 2, 0)
    barrier = pltpu.get_barrier_semaphore()
    n_bits = n_s.bit_length() - 1

    def greet(semaphore):
        for b in range(n_bits):
            pl.semaphore_signal(semaphore, inc=1, device_id=(i, flip(s, b)), device_id_type=MESH)
        pl.semaphore_signal(semaphore, inc=1, device_id=mate, device_id_type=MESH)

        @pl.when(is_inner)
        def _():
            pl.semaphore_signal(semaphore, inc=1, device_id=twin, device_id_type=MESH)

    def greeted(semaphore):
        pl.semaphore_wait(semaphore, n_bits + 1 + jnp.where(is_inner, 1, 0))

    greet(barrier)
    load_master = [
        pltpu.make_async_copy(
            master_ref.at[:, c * LANES : (c + 1) * LANES], master.at[:, c * LANES : (c + 1) * LANES],
            local_sem.at[3 + steps + c],
        )
        for c in range(chunks)
    ]
    load_rows = [
        pltpu.make_async_copy(rows_ref.at[0, st], rows.at[st, s], local_sem.at[st]) for st in range(steps)
    ]
    load_rest = [
        pltpu.make_async_copy(stream_ref.at[0], stream, local_sem.at[steps]),
        pltpu.make_async_copy(goals_ref.at[0], goals, local_sem.at[1 + steps]),
        pltpu.make_async_copy(moment_ref, moment, local_sem.at[2 + steps]),
    ]
    for copy in [load_master[0], load_rows[0]] + load_master[1:] + load_rows[1:]:
        copy.start()

    def remote(src, dst, send, recv, to):
        return pltpu.make_async_remote_copy(
            src_ref=src, dst_ref=dst, send_sem=send, recv_sem=recv, device_id=to, device_id_type=MESH
        )

    def z_mate(o, c):
        return remote(anchor.at[o, c], anchor.at[o, c], z_send.at[0], z_recv.at[o, c], mate)

    def z_twin(o, c):
        return remote(anchor.at[o, c], anchor.at[o, c], z_send.at[1], z_recv.at[o, c], twin)

    orders = [list(range(1, n_bits)) + [0], list(range(n_bits - 1, 0, -1)) + [0]]
    half = block // 2

    def a_blocks(h, phase):
        found = []
        for m in range(1 << phase):
            at = s
            for q in range(phase):
                if (m >> q) & 1:
                    at = flip(at, orders[h][q])
            found.append(at)
        return found

    def rows_of(which, blocks, band=slice(None)):
        if which < 2:
            return rows.at[which, blocks, band]
        if which == 2:
            return rows_h.at[0, blocks, band]
        wide = pl.multiple_of((mirrored(6 - which) - near_far) * piece, LANES)
        return rows_h.at[1, blocks, band, pl.ds(wide, piece)]

    last = n_bits - 1

    def a_start(which, stage):
        phase = min(stage, last)
        count = 1 << phase
        part = range(count) if stage < last else range((stage - last) * count // 2, (stage - last + 1) * count // 2)
        for m in part:
            for h in range(2):
                block_part = rows_of(which, a_blocks(h, phase)[m], pl.ds(h * half, half))
                remote(
                    block_part, block_part, a_send.at[which], a_recv.at[which, stage],
                    (i, flip(s, orders[h][phase])),
                ).start()

    def a_wait(which, stage):
        count = (1 << stage) if stage < last else (1 << last) // 2
        blocks = rows_of(which, pl.ds(0, count))
        remote(blocks, blocks, a_send.at[which], a_recv.at[which, stage], mate).wait_recv()

    def a_sent(which):
        blocks = rows_of(which, pl.ds(0, n_s - 1))
        remote(blocks, blocks, a_send.at[which], a_recv.at[which, 0], mate).wait_send()

    def a_next(which, phase):
        a_wait(which, phase)
        if phase + 1 < last:
            a_start(which, phase + 1)
        if phase == last - 2:
            a_start(which, last)
        if phase == last - 1:
            a_start(which, last + 1)

    def a_done(which):
        a_wait(which, last)
        a_wait(which, last + 1)

    far = pl.multiple_of(jnp.where(is_left, width - 2 * piece, 0), LANES)

    def lend_rows(st):
        return remote(
            rows.at[st, s, :, pl.ds(far, 2 * piece)], rows_h.at[st, s], ha_send.at[0], ha_recv.at[st], mate
        )

    gains[i] = gain_ref[...].astype(bf16).astype(f32)
    gain_copies = [
        remote(gains.at[i], gains.at[i], g_send.at[0], g_recv.at[0], (lax.rem(i + d, n_i), s))
        for d in range(1, n_i)
    ]
    gain_wait = remote(
        gains.at[pl.ds(0, n_i - 1)], gains.at[pl.ds(0, n_i - 1)], g_send.at[0], g_recv.at[0], mate
    )

    def lower(c):
        def body(j, _):
            at = pl.ds(pl.multiple_of(j * tall, tall), tall)
            anchor[i, c, at, :] = master[at, c * LANES : (c + 1) * LANES].astype(bf16)
            return 0

        load_master[c].wait()
        lax.fori_loop(0, piece // tall, body, 0)

    lower(0)
    load_rows[0].wait()
    greeted(barrier)
    a_start(0, 0)
    for c in range(chunks):
        if c > 0:
            lower(c)
        if c == min(2, chunks - 1):
            pl.when(is_end)(lambda: lend_rows(0).start())
        z_mate(i, c).start()
        pl.when(is_inner)(lambda: z_twin(i, c).start())
    for copy in load_rows[1:]:
        copy.wait()
    pl.when(is_end)(lambda: lend_rows(1).start())
    for copy in load_rest:
        copy.start()
    for k in range(2):
        greet(round_sem.at[k])
        greeted(round_sem.at[k])
    for copy in gain_copies:
        copy.start()
    res[...] = jnp.zeros_like(res)
    for copy in load_rest:
        copy.wait()

    def joined(buffer, at, ds):
        return jnp.concatenate([buffer[at, c, ds, :] for c in range(chunks)], axis=1)

    def project(o, count=chunks):
        def body(k, _):
            start = pl.multiple_of(k * depth, depth)
            wide = pl.multiple_of(o * piece + k * depth, depth)
            part = rows[0, :, :, pl.ds(wide, depth)].reshape(tokens, depth)
            weights = [anchor[o, c, pl.ds(start, depth), :] for c in range(count)]
            res[:, : count * LANES] += jnp.dot(part, jnp.concatenate(weights, axis=1), preferred_element_type=f32)
            return 0

        lax.fori_loop(0, piece // depth, body, 0)

    def arrived(o, c):
        z_mate(o, c).wait_recv()

    held = chunks - 1
    groups = 2

    def fold(value):
        return jnp.sum(value.T, axis=0, keepdims=True)

    def spread(value):
        return jnp.broadcast_to(value, (LANES, LANES)).T

    def tile_at(q):
        return pl.ds(pl.multiple_of(q * LANES, LANES), LANES)

    def lanes_of(c):
        return slice(c * LANES, (c + 1) * LANES)

    def products(st, gain, at, among):
        sums = None
        for c in among:
            r = stream[st, at, lanes_of(c)].astype(f32) + res[at, lanes_of(c)] * scale
            res[at, lanes_of(c)] = r
            weighted = r * gain[:, lanes_of(c)]
            terms = (r * r, weighted * weighted, weighted * goals[st, at, lanes_of(c)].astype(f32))
            sums = terms if sums is None else tuple(a + b for a, b in zip(sums, terms))
        return sums

    def local_stats(st, gain, among, held_sums):
        def body(q, _):
            at = tile_at(q)
            sums = products(st, gain, at, among)
            for k in range(3):
                value = sums[k] + early[k, at, :] if held_sums else sums[k]
                stats[st, 0, k : k + 1, at] = fold(value)
            stats[st, 0, 3:4, at] = jnp.zeros((1, LANES), f32)
            return 0

        lax.fori_loop(0, tiles, body, 0, unroll=True)

    def early_stats(q, _):
        at = tile_at(q)
        sums = products(0, gain_read(), at, range(held))
        for k in range(3):
            early[k, at, :] = sums[k]
        return 0

    def part_copy():
        return remote(part_out, part_in, p_send, p_recv, mate)

    def project_for_end():
        weights = jnp.concatenate([anchor[near_far + k, held] for k in range(2)], axis=0)
        count = n_s // groups
        for g in range(groups):
            part = rows_h[0, g * count : (g + 1) * count].reshape(count * block, 2 * piece)
            part_out[g * count * block : (g + 1) * count * block, :] = jnp.dot(
                part, weights, preferred_element_type=f32
            ).astype(bf16)

    def gain_read():
        return jnp.concatenate([gains[j] for j in range(n_i)], axis=1)

    @when_end
    def _():
        one, two, three = mirrored(1), mirrored(2), mirrored(3)
        a_next(0, 0)
        a_start(1, 0)
        for p in range(1, last):
            a_next(0, p)
        a_done(0)
        project(i)
        for c in range(chunks):
            arrived(one, c)
        project(one)
        a_next(1, 0)
        for c in range(held):
            arrived(two, c)
        project(two, held)
        for p in range(1, last):
            a_next(1, p)
        for c in range(held):
            arrived(three, c)
        project(three, held)
        gain_wait.wait_recv()
        lax.fori_loop(0, tiles, early_stats, 0, unroll=True)
        part_copy().wait_recv()
        res[:, held * LANES :] += part_in[...].astype(f32)
        local_stats(0, gain_read(), (held,), True)

    @when_inner
    def _():
        zero, two, three = mirrored(0), mirrored(2), mirrored(3)

        def from_end(c):
            arrived(zero, c)
            z_twin(zero, c).start()

        def from_far(o, c):
            arrived(o, c)
            if c < held:
                z_mate(o, c).start()

        from_end(0)
        from_far(two, 0)
        a_next(0, 0)
        from_end(1)
        for c in range(1, chunks):
            from_far(two, c)
        from_end(2)
        for p in range(1, last):
            a_next(0, p)
        lend_rows(0).wait_recv()
        a_start(2, 0)
        from_far(three, 0)
        a_next(2, 0)
        a_start(1, 0)
        for c in range(3, chunks):
            from_end(c)
        a_done(0)
        project(i)
        from_far(three, 1)
        project(zero)
        for p in range(1, last):
            a_next(2, p)
        for c in range(2, held):
            from_far(three, c)
        project(two)
        from_far(three, held)
        a_done(2)
        project_for_end()
        part_copy().start()
        project(three)

    def row_stats(st, between=None):
        copies = [
            remote(
                stats.at[st, 0], stats.at[st, d], s_send.at[st], s_recv.at[st],
                (i, lax.rem(s + d, n_s)),
            )
            for d in range(1, n_s)
        ]
        for copy in copies:
            copy.start()
        if between is not None:
            between()
        others = stats.at[st, pl.ds(1, n_s - 1)]
        remote(others, others, s_send.at[st], s_recv.at[st], mate).wait()
        total = stats[st, 0]
        for d in range(1, n_s):
            total = total + stats[st, d]
        inverse = lax.rsqrt(total[0:1] * (1.0 / width) + norm_epsilon)
        pull = inverse * total[1:2] - total[2:3]
        line[0:1, :] = inverse
        line[1:2, :] = inverse * inverse * inverse * pull * (1.0 / width)

    def row_grads(st, gain, among):
        def body(q, totals):
            at = tile_at(q)
            inverse, pull = spread(line[0:1, at]), spread(line[1:2, at])
            found = []
            for c, total in zip(among, totals):
                r = res[at, lanes_of(c)]
                if st == 0:
                    res[at, lanes_of(c)] = jnp.zeros_like(r)
                unit = r * inverse
                scaled = gain[:, lanes_of(c)]
                loss = unit * scaled - goals[st, at, lanes_of(c)].astype(f32)
                loss = loss.astype(bf16).astype(f32)
                low = inverse * (loss * scaled) - r * pull
                slope[st, c, at, :] = (low * scale if exact else low).astype(bf16)
                found.append(total + jnp.sum(loss * unit, axis=0, keepdims=True))
            return tuple(found)

        return lax.fori_loop(0, tiles, body, (jnp.zeros((1, LANES), f32),) * len(among), unroll=True)

    def product(part, against):
        grad = lax.dot_general(part, against, (((0,), (0,)), ((), ())), preferred_element_type=f32)
        return grad if exact else grad * scale

    def weight_grad(st, wide, size):
        part = rows[st, :, :, pl.ds(pl.multiple_of(wide, size), size)].reshape(tokens, size)
        return product(part, joined(slope, st, slice(None)))

    def more_rows():
        @when_inner
        def _():
            a_next(1, 0)
            lend_rows(1).wait_recv()
            a_start(3, 0)

    @when_inner
    def _():
        gain_wait.wait_recv()
        local_stats(0, gain_read(), range(chunks), False)

    gain_anchor = gain_read()
    gain = gain_anchor
    row_stats(0, more_rows)
    gain_first = jnp.concatenate(row_grads(0, gain, range(chunks)), axis=1)

    def lend_slope(st, c):
        return remote(slope.at[st, c], slope_h.at[st, c], r_send.at[0], r_recv.at[c], mate)

    @when_end
    def _():
        for c in range(held):
            lend_slope(0, c).start()

    spans = width // span
    per_piece = piece // span

    def place(q):
        return mirrored(q // per_piece), q % per_piece

    def grad_one(q):
        o, j = place(q)
        return weight_grad(0, o * piece + j * span, span)

    def step_one(q, grad, ahead, keep_grad=True):
        o, j = place(q)
        at = pl.ds(pl.multiple_of(j * span, span), span)
        if keep_grad:
            grads[o, at, :] = grad
        step = (inner_rate * grad) * pl.reciprocal(jnp.abs(grad) + adam_epsilon)
        param = keep * joined(anchor, o, at).astype(f32) - step
        ahead[...] = param.astype(bf16)

    def project_later(q, ahead):
        o, j = place(q)
        wide = pl.multiple_of(o * piece + j * span, span)
        part = rows[1, :, :, pl.ds(wide, span)].reshape(tokens, span)
        res[...] += jnp.dot(part, ahead[...], preferred_element_type=f32)

    def both(t, _):
        even = grad_one(2 * t)
        odd = grad_one(2 * t + 1)
        step_one(2 * t, even, ahead_a)
        project_later(2 * t, ahead_a)
        step_one(2 * t + 1, odd, ahead_b)
        project_later(2 * t + 1, ahead_b)
        return 0

    def both_grads(t, _):
        for q in (2 * t, 2 * t + 1):
            o, j = place(q)
            grads[o, pl.ds(pl.multiple_of(j * span, span), span), :] = grad_one(q)
        return 0

    def both_rest(t, _):
        for q, ahead in ((2 * t, ahead_a), (2 * t + 1, ahead_b)):
            o, j = place(q)
            step_one(q, grads[o, pl.ds(pl.multiple_of(j * span, span), span), :], ahead, False)
        project_later(2 * t, ahead_a)
        project_later(2 * t + 1, ahead_b)
        return 0

    def one_alone(q, _):
        step_one(q, grad_one(q), later.at[q])
        return 0

    group = 2 if per_piece % 2 == 0 else 1

    def later_alone(g, _):
        o, j = place(g * group)
        wide = pl.multiple_of(o * piece + j * span, span)
        part = rows[1, :, :, pl.ds(wide, group * span)].reshape(tokens, group * span)
        weights = jnp.concatenate([later[g * group + k] for k in range(group)], axis=0)
        res[...] += jnp.dot(part, weights, preferred_element_type=f32)
        return 0

    @when_end
    def _():
        a_done(1)
        near = 2 * per_piece // 2
        lax.fori_loop(0, near, both, 0, unroll=True)
        arrived(mirrored(2), held)
        lax.fori_loop(near, near + per_piece // 2, both, 0)
        lax.fori_loop(near + per_piece // 2, spans // 2, both_grads, 0)
        arrived(mirrored(3), held)
        lax.fori_loop(near + per_piece // 2, spans // 2, both_rest, 0)

    @when_inner
    def _():
        lax.fori_loop(0, spans, one_alone, 0)
        z_mate(mirrored(2), held).start()
        z_mate(mirrored(3), held).start()
        for p in range(1, last):
            a_next(1, p)
        a_next(3, 0)
        a_done(1)
        lax.fori_loop(0, spans // group, later_alone, 0)
        for p in range(1, last):
            a_next(3, p)

    gain_step = first_update(gain_first)
    gain = gain_anchor - inner_rate * gain_step

    local_stats(1, gain, range(chunks), False)
    row_stats(1)
    is_even = lax.rem(s, 2) == 0
    gain_second = row_grads(1, gain, (0,))

    @when_end
    def _():
        lend_slope(1, 0).start()

    gain_second = jnp.concatenate(gain_second + row_grads(1, gain, range(1, chunks)), axis=1)
    when_inner(lambda: a_start(4, 0))
    gain_move = inner_rate * (gain_step + second_update(gain_first, gain_second))
    for j in range(n_i):
        gain_out[j] = gain_move[:, j * own : (j + 1) * own]

    gain_moves = [
        remote(
            gain_out.at[lax.rem(i + d, n_i)], gain_in.at[d], g_send.at[1], g_recv.at[1],
            (lax.rem(i + d, n_i), s),
        )
        for d in range(1, n_i)
    ]
    for copy in gain_moves:
        copy.start()

    def move(o, first=0, until=piece // span):
        def body(j, _):
            at = pl.ds(pl.multiple_of(j * span, span), span)
            grad = weight_grad(1, o * piece + j * span, span)
            grads[o, at, :] = outer_sum(grads[o, at, :], grad)
            return 0

        lax.fori_loop(first, until, body, 0)

    def give(slot, c):
        return remote(outgo.at[slot, c], from_mate.at[c], e_send.at[0], e_recv.at[c], mate)

    def cross(slot, c, at=slice(None)):
        return remote(
            outgo.at[slot, c, at], from_twin.at[slot, c, at], m_send.at[0], m_recv.at[slot, c], twin
        )

    def pack(slot, c, o, *others):
        lanes = slice(c * LANES, (c + 1) * LANES)

        def body(j, _):
            at = pl.ds(pl.multiple_of(j * tall, tall), tall)
            total = grads[o, at, lanes]
            for other in others:
                total = total + other[at, :].astype(f32)
            outgo[slot, c, at, :] = total.astype(bf16)
            return 0

        lax.fori_loop(0, piece // tall, body, 0)

    def finish(c, o, *others):
        lanes = slice(c * LANES, (c + 1) * LANES)

        def body(j, _):
            at = pl.ds(pl.multiple_of(j * tall, tall), tall)
            total = grads[o, at, lanes]
            for other in others:
                total = total + other[at, :].astype(f32)
            outer = master[at, lanes]
            pseudo = total * (1.0 / n_i) + (1.0 - keep * keep) * outer.astype(bf16).astype(f32)
            velocity = outer_momentum * moment[at, lanes] + pseudo
            velocity_ref[at, lanes] = velocity
            updated_ref[at, lanes] = outer - outer_rate * (pseudo + outer_momentum * velocity)
            return 0

        lax.fori_loop(0, piece // tall, body, 0)
    @when_end
    def _():
        o = mirrored(1)
        for c in range(1, chunks):
            lend_slope(1, c).start()
            if c == held - 1:
                lend_slope(0, held).start()
        move(o)
        for c in range(chunks):
            pack(0, c, o)
        for c in range(chunks):
            give(0, c).start()
        o = mirrored(0)
        move(o)
        for c in range(chunks):
            give(0, c).wait_recv()
            finish(c, o, from_mate.at[c])

    def help_end(slot, c, o):
        base = (o - near_far) * piece
        lanes = slice(c * LANES, (c + 1) * LANES)

        def body(j, _):
            at = pl.ds(pl.multiple_of(j * tall, tall), tall)
            wide = pl.ds(pl.multiple_of(base + j * tall, tall), tall)
            pair = [
                product(rows_h[st, :, :, wide].reshape(tokens, tall), slope_h[st, c]) for st in range(steps)
            ]
            outgo[slot, c, at, :] = (grads[o, at, lanes] + outer_sum(*pair)).astype(bf16)
            cross(slot, c, at).start()
            return 0

        lax.fori_loop(0, piece // tall, body, 0)

    @when_inner
    def _():
        def help_and_cross(slot, c):
            help_end(slot, c, mirrored(3 - slot))

        def forward(c):
            cross(0, c).wait_recv()
            pack(2, c, mirrored(0), from_twin.at[0, c])
            give(2, c).start()

        move(mirrored(3))
        a_done(3)

        def far_sum(c):
            both_steps = slope_h.at[:, c]
            remote(both_steps, both_steps, r_send.at[0], r_recv.at[c], mate).wait_recv()
            help_and_cross(0, c)

        phases = list(range(last))
        for c in range(held):
            far_sum(c)
            if c == 0:
                a_next(4, phases.pop(0))
                move(mirrored(0))
            if c == 1:
                for p in phases:
                    a_next(4, p)
                move(mirrored(2))
        forward(0)
        a_done(4)
        help_and_cross(1, 0)
        far_sum(held)
        for c in range(1, chunks):
            if c < held:
                forward(c)
            help_and_cross(1, c)
            if c == 1:
                move(mirrored(1))
        forward(held)
        for c in range(chunks):
            give(2, c).wait_recv()
            cross(1, c).wait_recv()
            finish(c, mirrored(1), from_mate.at[c], from_twin.at[1, c])

    moved_gains = gain_in.at[pl.ds(1, n_i - 1)]
    remote(moved_gains, moved_gains, g_send.at[1], g_recv.at[1], mate).wait()
    gain_total = gain_out[i]
    for d in range(1, n_i):
        gain_total = gain_total + gain_in[d]
    gain_pseudo = gain_total * (1.0 / n_i)
    gain_velocity = outer_momentum * gain_moment_ref[...] + gain_pseudo
    gain_velocity_ref[...] = gain_velocity
    gain_updated_ref[...] = gain_ref[...] - outer_rate * (gain_pseudo + outer_momentum * gain_velocity)

    def sent_pieces(way, count):
        pieces = anchor.at[pl.ds(0, count)]
        remote(pieces, pieces, z_send.at[way], z_recv.at[0, 0], mate).wait_send()

    @when_end
    def _():
        lent = rows_h.at[pl.ds(0, steps), 0]
        remote(lent, lent, ha_send.at[0], ha_recv.at[0], mate).wait_send()
        sent_pieces(0, 1)
        remote(slope, slope, r_send.at[0], r_recv.at[0], mate).wait_send()
        remote(from_mate, from_mate, e_send.at[0], e_recv.at[0], mate).wait_send()

    @when_inner
    def _():
        remote(from_twin, from_twin, m_send.at[0], m_recv.at[0, 0], twin).wait_send()
        remote(from_mate, from_mate, e_send.at[0], e_recv.at[0], mate).wait_send()
        part_copy().wait_send()
        for which in (2, 3, 4):
            a_sent(which)
        sent_pieces(0, 3)
        sent_pieces(1, 2)

    gain_wait.wait_send()
    a_sent(0)
    a_sent(1)


def write_out(*refs):
    count = len(refs) // 2
    sem = refs[-1]
    copies = [pltpu.make_async_copy(refs[k], refs[count + k], sem.at[k]) for k in range(count)]
    for copy in copies:
        copy.start()
    for copy in copies:
        copy.wait()


def per_device(weight_master, gain_master, weight_moment, gain_moment, attended, stream, targets):
    n_i, n_s = lax.axis_size("island"), lax.axis_size("shard")
    _, steps, block, width = attended.shape
    _, _, tokens, cols = stream.shape
    piece = weight_master.shape[0]
    own = gain_master.shape[0]
    f32, bf16 = jnp.float32, jnp.bfloat16
    chunks = cols // LANES
    arrays = [
        ((piece, cols), f32),
        ((piece, cols), f32),
        ((steps, n_s, block, width), bf16),
        ((steps, n_s, block, 2 * piece), bf16),
        ((n_i, chunks, piece, LANES), bf16),
        ((min(512, piece), cols), bf16),
        ((min(512, piece), cols), bf16),
        ((width // min(512, piece), min(512, piece), cols), bf16),
        ((n_i, piece, cols), f32),
        ((tokens, cols), f32),
        ((steps, chunks, tokens, LANES), bf16),
        ((steps, chunks, tokens, LANES), bf16),
        ((steps, tokens, cols), bf16),
        ((steps, tokens, cols), bf16),
        ((3, chunks, piece, LANES), bf16),
        ((chunks, piece, LANES), bf16),
        ((2, chunks, piece, LANES), bf16),
        ((tokens, LANES), bf16),
        ((tokens, LANES), bf16),
        ((3, tokens, LANES), f32),
        ((steps, n_s, 4, tokens), f32),
        ((2, tokens), f32),
        ((n_i, 1, own), f32),
        ((n_i, 1, own), f32),
        ((n_i, 1, own), f32),
    ]
    held = sum(math.prod(shape) * jnp.dtype(kind).itemsize for shape, kind in arrays)
    spans = piece // min(512, piece)
    if spans % 2 or n_i != 4 or steps != 2 or own % LANES or chunks < 2 or block % 32 or n_s < 8 or held > 60e6:
        return general_device(weight_master, gain_master, weight_moment, gain_moment, attended, stream, targets)
    any_space = pl.BlockSpec(memory_space=pl.ANY)
    vmem = pl.BlockSpec(memory_space=pltpu.VMEM)
    dma = pltpu.SemaphoreType.DMA
    outs = ((piece, cols), (1, own), (piece, cols), (1, own))
    results = pl.pallas_call(
        functools.partial(kernel, n_i, n_s),
        out_shape=tuple(pltpu.VMEM(shape, f32) for shape in outs),
        in_specs=[any_space, vmem, any_space, vmem, any_space, any_space, any_space],
        out_specs=(vmem, vmem, vmem, vmem),
        scratch_shapes=[pltpu.VMEM(shape, kind) for shape, kind in arrays]
        + [
            pltpu.SemaphoreType.REGULAR((2,)),
            dma((3 + steps + chunks,)),
            dma((2,)),
            dma((n_i, chunks)),
            dma((5,)),
            dma((5, n_s.bit_length())),
            dma(()),
            dma(()),
            dma((1,)),
            dma((steps,)),
            dma((steps,)),
            dma((steps,)),
            dma((2,)),
            dma((2,)),
            dma((1,)),
            dma((chunks,)),
            dma((1,)),
            dma((chunks,)),
            dma((1,)),
            dma((2, chunks)),
        ],
        compiler_params=pltpu.CompilerParams(
            collective_id=0, has_side_effects=True, vmem_limit_bytes=58 << 20
        ),
    )(weight_master, gain_master[None], weight_moment, gain_moment[None], attended, stream, targets)
    results = [pltpu.with_memory_space_constraint(x, pltpu.VMEM) for x in results]
    updated, gain_updated, velocity, gain_velocity = pl.pallas_call(
        write_out,
        out_shape=tuple(jax.ShapeDtypeStruct(shape, f32) for shape in outs),
        in_specs=[vmem] * 4,
        out_specs=(any_space,) * 4,
        scratch_shapes=[dma((4,))],
        compiler_params=pltpu.CompilerParams(vmem_limit_bytes=1 << 20),
    )(*results)
    return (updated, gain_updated[0], velocity, gain_velocity[0])


def solution(mesh):
    placed = (
        P("island", "shard"),
        P(("shard", "island")),
        P("island", "shard"),
        P(("shard", "island")),
        P("island", None, "shard", None),
        P("island", None, None, "shard"),
        P("island", None, None, "shard"),
    )
    return jax.shard_map(
        per_device,
        mesh=mesh,
        in_specs=placed,
        out_specs=(
            P("island", "shard"),
            P(("shard", "island")),
            P("island", "shard"),
            P(("shard", "island")),
        ),
        check_vma=False,
    )
```
